512 devices in a mesh: group: 2 (over y), plane: 16 (over z), planey: 8 (over x), ens: 2 (over core).
Axes of the slice: x: 8, y: 2, z: 16, core: 2. Of those that a mesh axis runs over, the one named last changes fastest.
The devices are a block of a 8x8x16 slice.
Arguments:
- u_prior: float32 [8, 2, 10, 256, 1024], P(('group', 'ens'), None, None, 'plane', 'planey'), parts along dimension 0, may hold values from -6 to 6
- friction_rows: int32 [8], P(('group', 'ens')), parts along dimension 0, may hold values from 0 to 15
- friction_table: float32 [32, 256, 1024], P('group', 'plane', 'planey'), parts along dimension 0, may hold values from 0.3 to 3
- bed_fixed: int32 [256, 1024], P('plane', 'planey'), may hold values from -536870912 to 536870911
- ice_mask: int32 [256, 1024], P('plane', 'planey'), may hold values 0 or 1
Outputs:
- mean_velocity: float32 [4, 10, 256, 1024], P('group', None, 'plane', 'planey'), parts along dimension 0
The draws below stay inside these ranges and needn't reach their ends.
There are 2 independent parts, one for each index of `group`. The reference program is written for one: setup_inputs(seed, part) draws one part's arguments, and reference() takes and returns one part's arrays. A program takes and returns all parts, laid end to end along the dimension named above; an argument that names none is the same for every part. Nothing has to cross between parts.
Inputs may be any that keep to these rules, and one draw needn't show every extreme that they name: `friction_rows`: each sample names one row of the friction table.
All inputs are finite; a program needn't handle non-finite values. No bound on the sum of `ice_mask` on one device may be relied on, other than what follows from the above.
Results may differ from the reference program's by a relative error of at most 0.0003.
Values sent between devices are 32-bit elements; how exact they have to be, the bound alone decides.
No kernel may reach another device: no remote copies, remote signals or barrier semaphores. Data moves between devices by JAX's collectives and lax.ppermute only.
A program may use at most 64 MiB of HBM per device.

```python
import math
import jax
import jax.numpy as jnp
from jax import lax

NZ = 10
ITERS = 2
LEVELS = 16
SAMPLES = 4
NX = 256
NY = 1024


def with_ends(drawn, rng, least, largest):
    spot = [jax.random.randint(jax.random.fold_in(rng, axis), (), 0, length) for axis, length in enumerate(drawn.shape)]
    main_axis = drawn.shape.index(max(drawn.shape))
    next_to = spot[:main_axis] + [(spot[main_axis] + 1) % drawn.shape[main_axis]] + spot[main_axis + 1:]
    return drawn.at[tuple(spot)].set(least).at[tuple(next_to)].set(largest)


def shard_levels(stream_key, dims, shards, smallest, top_value):
    factor_of, own = 1.0, jax.random.fold_in(stream_key, 6)
    for axis_at, blocks in shards:
        draws = jnp.exp(jax.random.uniform(jax.random.fold_in(own, axis_at), (blocks,), jnp.float32, smallest / len(shards), top_value / len(shards)))
        factor_of = factor_of * jnp.repeat(draws, dims[axis_at] // blocks).reshape([-1 if axis == axis_at else 1 for axis in range(len(dims))])
    return factor_of


def scatter_about(stream_key, shape, width, bound, split=(), kind=jnp.bfloat16):
    values = jax.random.normal(stream_key, shape, jnp.float32) * width
    if len(split) > 0:
        values = shard_levels(stream_key, shape, split, -0.22, 0.18) * values
    return jnp.clip(values, min=-bound, max=bound).astype(kind)


def setup_inputs(seed: int = 0, part: int = 0) -> dict:
    keys = jax.random.split(jax.random.key(seed), 6)
    own_keys = jax.random.split(jax.random.fold_in(keys[5], part), 6)
    return {
        "u_prior": scatter_about(own_keys[0], (SAMPLES, 2, NZ, NX, NY), 1.0, 6.0, ((0, 2), (3, 16), (4, 8)), jnp.float32),
        "friction_rows": with_ends(jax.random.randint(own_keys[1], (SAMPLES,), 0, LEVELS), jax.random.fold_in(own_keys[1], 1), 0, LEVELS - 1).astype(jnp.int32),
        "friction_table": jnp.clip(jnp.exp(math.log(3.0) - 2.3025851 * jax.random.uniform(own_keys[2], (LEVELS, NX, NY), jnp.float32) ** shard_levels(own_keys[2], (LEVELS, NX, NY), ((1, 16), (2, 8)), -0.2, 0.2)), 0.3, 3.0),
        "bed_fixed": with_ends(jax.random.randint(keys[3], (NX, NY), -536870912, 536870912), jax.random.fold_in(keys[3], 1), -536870912, 536870911).astype(jnp.int32),
        "ice_mask": with_ends((jax.random.randint(keys[4], (NX, NY), 0, 8) < 7).astype(jnp.int32), jax.random.fold_in(keys[4], 1), 0, 1),
    }


bed_unit = 2.0 ** -29
factor_u = (2.0, 1.0, 0.5)
factor_v = (2.0, 0.5, 1.0)


def coefficient(offset):
    nonzero = len([entry for entry in offset if entry != 0])
    weight_u = 0.25 ** (nonzero - 1)
    weight_v = weight_u
    for dimension in range(3):
        if offset[dimension] != 0:
            weight_u = weight_u * factor_u[dimension]
            weight_v = weight_v * factor_v[dimension]
    return jnp.array([weight_u, weight_v], jnp.float32).reshape(2, 1, 1, 1)


def neighbour_sum(padded):
    layers = padded.shape[-3] - 2
    span_x = padded.shape[-2] - 2
    span_y = padded.shape[-1] - 2
    summed = None
    for step_z in (-1, 0, 1):
        for step_x in (-1, 0, 1):
            for step_y in (-1, 0, 1):
                if step_z == 0 and step_x == 0 and step_y == 0:
                    continue
                window = padded[..., 1 + step_z:1 + step_z + layers, 1 + step_x:1 + step_x + span_x, 1 + step_y:1 + step_y + span_y]
                addend = coefficient((step_z, step_x, step_y)) * window
                summed = addend if summed is None else summed + addend
    return summed


def strain_roots(extended):
    padded = jnp.pad(extended, [(0, 0)] * (extended.ndim - 3) + [(1, 1), (0, 0), (0, 0)])
    along_x = (padded[..., 1:-1, 2:, 1:-1] - padded[..., 1:-1, :-2, 1:-1]) * 0.5
    along_y = (padded[..., 1:-1, 1:-1, 2:] - padded[..., 1:-1, 1:-1, :-2]) * 0.5
    along_z = (padded[..., 2:, 1:-1, 1:-1] - padded[..., :-2, 1:-1, 1:-1]) * 0.5
    stretch_x = along_x[..., 0, :, :, :]
    stretch_y = along_y[..., 1, :, :, :]
    shear_one = along_y[..., 0, :, :, :]
    shear_two = along_x[..., 1, :, :, :]
    vertical_u = along_z[..., 0, :, :, :]
    vertical_v = along_z[..., 1, :, :, :]
    shear = shear_one + shear_two
    strain = stretch_x * stretch_x + stretch_y * stretch_y + stretch_x * stretch_y + 0.25 * shear * shear + 0.25 * (vertical_u * vertical_u + vertical_v * vertical_v)
    return jnp.power(strain + 0.1, -1.0 / 6.0)[..., None, :, :, :]


def reference(u_prior, friction_rows, friction_table, bed_fixed, ice_mask):
    cover = ice_mask.astype(jnp.float32)
    bed = bed_fixed.astype(jnp.float32) * bed_unit
    bed_pad = jnp.pad(bed, 1)
    slope_x = (bed_pad[2:, 1:-1] - bed_pad[:-2, 1:-1]) * 0.5
    slope_y = (bed_pad[1:-1, 2:] - bed_pad[1:-1, :-2]) * 0.5
    thickness = 1.0 + 2.0 * jnp.arange(NX, dtype=jnp.float32)[:, None] / (NX - 1)
    force = jnp.stack([-(cover * thickness * slope_x), -(cover * thickness * slope_y)])[:, None, :, :]
    bottom = (jnp.arange(NZ, dtype=jnp.int32) == 0).astype(jnp.float32)[:, None, None]
    levels = jnp.arange(LEVELS, dtype=jnp.int32)

    def solve(summed, inputs):
        prior, table_row = inputs
        extended = jnp.pad(prior, ((0, 0), (0, 0), (1, 1), (1, 1)))
        roots = cover * strain_roots(extended)
        across = neighbour_sum(jnp.pad(roots, ((0, 0), (1, 1), (1, 1), (1, 1))))
        chosen = (levels == table_row).astype(jnp.float32)
        friction = jnp.sum(chosen[:, None, None] * friction_table, axis=0)
        diag = cover * friction * bottom + (1.0 - cover)

        def operate(field):
            product = roots * field
            nearby = neighbour_sum(jnp.pad(product, ((0, 0), (1, 1), (1, 1), (1, 1))))
            return roots * (across * field - nearby) + diag * field

        solution = prior * cover
        residual = force - operate(solution)
        direction = residual
        norm_now = jnp.sum(residual * residual)
        for step in range(ITERS):
            image = operate(direction)
            alpha = norm_now / jnp.sum(direction * image)
            solution = solution + alpha * direction
            if step + 1 < ITERS:
                residual = residual - alpha * image
                norm_next = jnp.sum(residual * residual)
                direction = residual + (norm_next / norm_now) * direction
                norm_now = norm_next
        return summed + solution, None

    start = jnp.zeros((2, NZ, NX, NY), jnp.float32)
    summed = lax.scan(solve, start, (u_prior, friction_rows))[0]
    return summed / SAMPLES
```

```python
import jax
import jax.numpy as jnp
from jax import lax
from jax.experimental import pallas as pl
from jax.experimental.pallas import tpu as pltpu
from jax.sharding import PartitionSpec as P

bed_unit = 2.0 ** (-29)
HALO = 4
STRIP = 24
GROUPED = STRIP // HALO
MAIN_I = (0.25, 0.125)
MAIN_J = (0.125, 0.25)


VMEM = pl.BlockSpec(memory_space=pltpu.VMEM)
SMEM = pl.BlockSpec(memory_space=pltpu.SMEM)


def roll(x, shift, axis):
    return pltpu.roll(x, shift % x.shape[axis], axis)


def lanes(shape):
    return lax.broadcasted_iota(jnp.int32, shape, len(shape) - 1)


def rows(shape):
    return lax.broadcasted_iota(jnp.int32, shape, len(shape) - 2)


def pack_rows(rows_ref, u_ref, table_ref, bed_ref, mask_ref, up_ref, down_ref, geo_ref, sems):
    layers = u_ref.shape[2]
    copies = [
        pltpu.make_async_copy(table_ref.at[rows_ref[s]], geo_ref.at[2 + s], sems.at[s])
        for s in range(2)
    ]
    for copy in copies:
        copy.start()
    geo_ref[0] = mask_ref[...].astype(jnp.float32)
    geo_ref[1] = bed_ref[...].astype(jnp.float32) * bed_unit
    low = rows((8, 128)) < HALO
    for layer in range(layers + 1):
        if layer == layers:
            for copy in copies:
                copy.wait()
        for pair in range(2):
            tiles = [
                u_ref[s, pair, layer] if layer < layers else geo_ref[2 * pair + s] for s in range(2)
            ]
            top = [tile[0:8] for tile in tiles]
            end = [tile[8:16] for tile in tiles]
            up_ref[layer, pair] = jnp.where(low, roll(end[0], HALO, 0), end[1])
            down_ref[layer, pair] = jnp.where(low, top[0], roll(top[1], HALO, 0))


def pack_columns(u_ref, geo_ref, below_ref, above_ref, outer_ref, strip_ref, right_ref, left_ref):
    layers = u_ref.shape[2]
    low = rows((8, 128)) < HALO
    lane = lanes((8, 128))
    used = lane < 4 * STRIP
    place = lane % STRIP
    slot = place // HALO
    zero = jnp.zeros((8, 128), jnp.float32)
    sent_right = [[zero] * 3 for _ in range(2)]
    sent_left = [[zero] * 3 for _ in range(2)]
    for layer in range(layers + 1):
        outer = []
        for pair in range(2):
            below = below_ref[layer, pair]
            above = above_ref[layer, pair]
            outer.append(jnp.where(low, above, roll(below, HALO, 0)))
            outer.append(jnp.where(low, roll(above, HALO, 0), below))
        for k in range(4):
            outer_ref[layer, k] = outer[k]
        for t in range(3):
            strip = zero
            for k in range(4):
                if t == 2:
                    tile = outer[k]
                elif layer < layers:
                    tile = u_ref[k % 2, k // 2, layer, 8 * t : 8 * t + 8]
                else:
                    tile = geo_ref[k, 8 * t : 8 * t + 8]
                at = lane - STRIP * k
                strip = jnp.where((at >= 4) & (at < 12), roll(tile, STRIP * k + 4, 1), strip)
                strip = jnp.where((at >= 12) & (at < 20), roll(tile, STRIP * k + 12 - 120, 1), strip)
            strip_ref[layer, 8 * t : 8 * t + 8] = strip
            group, index = layer // GROUPED, layer % GROUPED
            here = used & (slot == index)
            sent_right[group][t] = jnp.where(
                here, roll(strip, HALO * index - 16, 1), sent_right[group][t]
            )
            sent_left[group][t] = jnp.where(
                here, roll(strip, HALO * index - 4, 1), sent_left[group][t]
            )
    for group in range(2):
        for t in range(3):
            right_ref[group, 8 * t : 8 * t + 8] = sent_right[group][t]
            left_ref[group, 8 * t : 8 * t + 8] = sent_left[group][t]


def operator(
    plane_ref, u_ref, geo_ref, outer_ref, strip_ref, from_left_ref, from_right_ref,
    residual_ref, image_ref, start_ref, gram_ref,
    wide_ref, roots_ref, scale_ref, field_ref, next_ref, *, total_x,
):
    layers = u_ref.shape[2]
    shape = (24, 128)
    lane = lanes(shape)
    row = rows(shape)
    used = lane < 4 * STRIP
    place = lane % STRIP
    number = lane // STRIP

    def around_i(x):
        return roll(x, 1, 0) + roll(x, -1, 0)

    def around_j(x):
        return roll(x, 1, 1) + roll(x, -1, 1)

    geo_strip = None
    for layer in range(layers + 1):
        group, index = layer // GROUPED, layer % GROUPED
        strip = strip_ref[layer]
        strip = jnp.where(used & (place < 4), roll(from_left_ref[group], -HALO * index, 1), strip)
        strip = jnp.where(used & (place >= 20), roll(from_right_ref[group], 20 - HALO * index, 1), strip)
        if layer < layers:
            wide_ref[layer] = strip
        else:
            geo_strip = strip

    def spread_strip(source, to):
        result = jnp.zeros(shape, jnp.float32)
        for k in range(4):
            result = jnp.where(number == k, roll(source, STRIP * (k - to), 1), result)
        return result

    def main_geo(k):
        return jnp.concatenate([geo_ref[k], outer_ref[layers, k]], axis=0)

    def main(k, layer):
        return jnp.concatenate([u_ref[k % 2, k // 2, layer], outer_ref[layer, k]], axis=0)

    mask = main_geo(0)
    bed = main_geo(1)
    strip_mask = spread_strip(geo_strip, 0)
    strip_bed = spread_strip(geo_strip, 1)
    strip_friction = jnp.where(lane < 2 * STRIP, roll(geo_strip, -2 * STRIP, 1), geo_strip)
    position = jnp.where(row < 20, row, row - 24).astype(jnp.float32) + plane_ref[0]
    thickness = 1.0 + 2.0 * position / (total_x - 1)

    def forces(cover, ground):
        slope_x = (roll(ground, -1, 0) - roll(ground, 1, 0)) * 0.5
        slope_y = (roll(ground, -1, 1) - roll(ground, 1, 1)) * 0.5
        return -(cover * thickness * slope_x), -(cover * thickness * slope_y)

    main_force = forces(mask, bed)
    strip_x, strip_y = forces(strip_mask, strip_bed)
    strip_force = jnp.where(lane < 2 * STRIP, strip_x, strip_y)
    bare = 1.0 - mask
    strip_bare = 1.0 - strip_mask

    def viscosity(u, v, below_u, below_v, above_u, above_v, cover):
        stretch_x = roll(u, -1, 0) - roll(u, 1, 0)
        stretch_y = roll(v, -1, 1) - roll(v, 1, 1)
        shear = (roll(u, -1, 1) - roll(u, 1, 1)) + (roll(v, -1, 0) - roll(v, 1, 0))
        rise_u = above_u - below_u
        rise_v = above_v - below_v
        strain = stretch_x * stretch_x + stretch_y * (stretch_y + stretch_x)
        strain = strain + 0.25 * (shear * shear + (rise_u * rise_u + rise_v * rise_v))
        return cover * jnp.exp(jnp.log(0.25 * strain + 0.1) * (-1.0 / 6.0))

    zero = jnp.zeros(shape, jnp.float32)

    def column(get, z):
        return get(z) if 0 <= z < layers else zero

    for s in range(2):
        for z in range(layers):
            get_u, get_v = (lambda y, s=s: main(s, y)), (lambda y, s=s: main(2 + s, y))
            roots_ref[s, z] = viscosity(
                get_u(z), get_v(z), column(get_u, z - 1), column(get_v, z - 1),
                column(get_u, z + 1), column(get_v, z + 1), mask,
            )
    for z in range(layers):
        get_u = lambda y: wide_ref[y]

        def get_v(y):
            return roll(wide_ref[y], -2 * STRIP, 1)

        found = viscosity(
            get_u(z), get_v(z), column(get_u, z - 1), column(get_v, z - 1),
            column(get_u, z + 1), column(get_v, z + 1), strip_mask,
        )
        roots_ref[2, z] = jnp.where(lane < 2 * STRIP, found, roll(found, 2 * STRIP, 1))

    side_i = jnp.where(lane < 2 * STRIP, MAIN_I[0], MAIN_I[1])
    side_j = jnp.where(lane < 2 * STRIP, MAIN_J[0], MAIN_J[1])
    for s in range(3):
        for z in range(layers):
            centre = roots_ref[s, z]
            if z > 0 and z + 1 < layers:
                centre = centre + 0.5 * (roots_ref[s, z - 1] + roots_ref[s, z + 1])
            elif z > 0:
                centre = centre + 0.5 * roots_ref[s, z - 1]
            else:
                centre = centre + 0.5 * roots_ref[s, z + 1]
            along_i = around_i(centre)
            along_j = around_j(centre)
            both = centre + 0.03125 * around_j(along_i)
            if s < 2:
                for c in range(2):
                    scale_ref[2 * c + s, z] = both + MAIN_I[c] * along_i + MAIN_J[c] * along_j
            else:
                scale_ref[4, z] = both + side_i * along_i + side_j * along_j

    def apply(k, get, put):
        if k < 4:
            weight_i, weight_j = MAIN_I[k // 2], MAIN_J[k // 2]
            friction = mask * main_geo(2 + k % 2) + bare
            empty, roots = bare, k % 2
        else:
            weight_i, weight_j = side_i, side_j
            friction = strip_mask * strip_friction + strip_bare
            empty, roots = strip_bare, 2

        def filtered(z):
            product = roots_ref[roots, z] * get(z)
            product = product + weight_i * around_i(product)
            return product + weight_j * around_j(product)

        before, now = None, filtered(0)
        for z in range(layers):
            after = filtered(z + 1) if z + 1 < layers else None
            if before is None:
                total = now + 0.5 * after
            elif after is None:
                total = now + 0.5 * before
            else:
                total = now + 0.5 * (before + after)
            field = get(z)
            result = 4.0 * roots_ref[roots, z] * (scale_ref[k, z] * field - total)
            put(z, result + (friction if z == 0 else empty) * field)
            before, now = now, after

    sums = []
    for k in range(5):
        cover = mask if k < 4 else strip_mask
        force = main_force[k // 2] if k < 4 else strip_force

        def start(z, k=k, cover=cover):
            return cover * (main(k, z) if k < 4 else wide_ref[z])

        def put_residual(z, value, k=k, force=force):
            residual = force - value
            field_ref[z] = residual
            residual_ref[k, z] = residual[0:16]

        def put_image(z, value, k=k):
            next_ref[z] = value
            image_ref[k, z] = value[0:16]

        totals = [jnp.zeros((8, 128), jnp.float32)] * 4

        def put_second(z, value):
            for t in range(2):
                at = slice(8 * t, 8 * t + 8)
                r, a, b = field_ref[z, at], next_ref[z, at], value[at]
                totals[0] = totals[0] + r * r
                totals[1] = totals[1] + r * a
                totals[2] = totals[2] + a * a
                totals[3] = totals[3] + a * b

        apply(k, start, put_residual)
        apply(k, lambda z: field_ref[z], put_image)
        apply(k, lambda z: next_ref[z], put_second)
        sums.append(totals)

    for c in range(2):
        for z in range(layers):
            start_ref[c, z] = mask[0:16] * u_ref[0, c, z] + mask[0:16] * u_ref[1, c, z]

    lane8 = lanes((8, 128))
    inside = (lane8 >= HALO) & (lane8 < 128 - HALO)
    spot = lane8 % STRIP
    edge = (lane8 < 4 * STRIP) & (((spot >= 4) & (spot < 8)) | ((spot >= 16) & (spot < 20)))
    row8 = rows((8, 128))
    table = jnp.zeros((8, 128), jnp.float32)
    for g in range(4):
        for s in range(2):
            value = jnp.where(inside, sums[s][g] + sums[2 + s][g], 0.0)
            value = value + jnp.where(edge & ((lane8 // STRIP) % 2 == s), sums[4][g], 0.0)
            value = jnp.sum(value, axis=0, keepdims=True)
            table = jnp.where(row8 == 2 * g + s, value, table)
    table = jnp.sum(table, axis=1, keepdims=True)
    line = jnp.sum(jnp.where(lane8 == row8, table, 0.0), axis=0, keepdims=True)
    gram_ref[...] = jnp.broadcast_to(line, gram_ref.shape)


def combine(gram_ref, residual_ref, image_ref, start_ref, out_ref):
    layers = start_ref.shape[1]
    shape = (8, 128)
    lane = lanes(shape)
    total = jnp.broadcast_to(jnp.sum(gram_ref[...], axis=0, keepdims=True), shape)
    rr = total
    ra = roll(total, -2, 1)
    aa = roll(total, -4, 1)
    ab = roll(total, -6, 1)
    first = rr / ra
    norm_next = rr - 2.0 * first * ra + first * first * aa
    growth = 1.0 + norm_next / rr
    curve = growth * growth * ra - 2.0 * growth * first * aa + first * first * ab
    second = norm_next / curve
    residual_part = first + second * growth
    image_part = second * first
    ks = [jnp.broadcast_to(residual_part[:, s : s + 1], shape) for s in range(2)]
    ms = [jnp.broadcast_to(image_part[:, s : s + 1], shape) for s in range(2)]
    odd = (lane // STRIP) % 2 == 1
    k_side = jnp.where(odd, ks[1], ks[0])
    m_side = jnp.where(odd, ms[1], ms[0])
    for z in range(layers):
        for t in range(2):
            at = slice(8 * t, 8 * t + 8)
            side = k_side * residual_ref[4, z, at] - m_side * image_ref[4, z, at]
            side = side + roll(side, -STRIP, 1)
            for c in range(2):
                step = ks[0] * residual_ref[2 * c, z, at] - ms[0] * image_ref[2 * c, z, at]
                step = step + ks[1] * residual_ref[2 * c + 1, z, at]
                step = step - ms[1] * image_ref[2 * c + 1, z, at]
                base = 2 * STRIP * c
                step = jnp.where(lane < HALO, roll(side, -(base + 4), 1), step)
                step = jnp.where(lane >= 128 - HALO, roll(side, 124 - base - 16, 1), step)
                out_ref[c, z, at] = start_ref[c, z, at] + step


def f32(*shape):
    return jax.ShapeDtypeStruct(shape, jnp.float32)


def call(kernel, outs, ins, name, scratch=(), in_specs=None):
    return pl.pallas_call(
        kernel,
        in_specs=in_specs or [VMEM] * len(ins),
        out_specs=[VMEM] * len(outs),
        out_shape=list(outs),
        scratch_shapes=list(scratch),
        name=name,
    )(*ins)


def swap_sides(forward, backward, axis):
    count = lax.axis_size(axis)
    up = [(i, i + 1) for i in range(count - 1)]
    down = [(i + 1, i) for i in range(count - 1)]
    return lax.ppermute(forward, axis, up), lax.ppermute(backward, axis, down)


def body(u_prior, friction_rows, friction_table, bed_fixed, ice_mask):
    members, parts, layers, rows_x, rows_y = u_prior.shape
    total_x = rows_x * lax.axis_size("plane")
    up, down, geo = call(
        pack_rows,
        [f32(layers + 1, 2, 8, rows_y), f32(layers + 1, 2, 8, rows_y), f32(4, rows_x, rows_y)],
        [friction_rows, u_prior, friction_table, bed_fixed, ice_mask],
        "pack_rows",
        scratch=[pltpu.SemaphoreType.DMA((2,))],
        in_specs=[SMEM, VMEM, pl.BlockSpec(memory_space=pl.ANY), VMEM, VMEM],
    )
    below, above = swap_sides(up, down, "plane")
    outer, strip, right, left = call(
        pack_columns,
        [f32(layers + 1, 4, 8, rows_y), f32(layers + 1, 24, 128), f32(2, 24, 128), f32(2, 24, 128)],
        [u_prior, geo, below, above],
        "pack_columns",
    )
    from_left, from_right = swap_sides(right, left, "planey")
    plane_start = (lax.axis_index("plane") * rows_x).astype(jnp.float32).reshape(1)
    devices = lax.axis_size("plane") * lax.axis_size("planey")
    ins = [u_prior, geo, outer, strip, from_left, from_right]
    residual, image, start, gram = call(
        lambda *refs: operator(*refs, total_x=total_x),
        [
            f32(5, layers, rows_x, 128),
            f32(5, layers, rows_x, 128),
            f32(2, layers, rows_x, 128),
            f32(devices, 128),
        ],
        [plane_start] + ins,
        "operator",
        scratch=[
            pltpu.VMEM((layers, 24, 128), jnp.float32),
            pltpu.VMEM((3, layers, 24, 128), jnp.float32),
            pltpu.VMEM((5, layers, 24, 128), jnp.float32),
            pltpu.VMEM((layers, 24, 128), jnp.float32),
            pltpu.VMEM((layers, 24, 128), jnp.float32),
        ],
        in_specs=[SMEM] + [VMEM] * len(ins),
    )
    gathered = lax.all_to_all(gram, ("plane", "planey"), 0, 0, tiled=True)
    (local_sum,) = call(
        combine, [f32(2, layers, rows_x, 128)], [gathered, residual, image, start], "combine"
    )
    summed = lax.all_gather(local_sum, "ens").sum(axis=0)
    return summed / (members * lax.axis_size("ens"))


def solution(mesh):
    in_specs = (
        P(("group", "ens"), None, None, "plane", "planey"),
        P(("group", "ens")),
        P("group", "plane", "planey"),
        P("plane", "planey"),
        P("plane", "planey"),
    )
    out_specs = P("group", None, "plane", "planey")
    return jax.shard_map(body, mesh=mesh, in_specs=in_specs, out_specs=out_specs, check_vma=False)
```

```python
import jax
import jax.numpy as jnp
from jax import lax
from jax.experimental import pallas as pl
from jax.experimental.pallas import tpu as pltpu
from jax.sharding import PartitionSpec as P

bed_unit = 2.0 ** (-29)
HALO = 4
STRIP = 24
GROUPED = STRIP // HALO
MAIN_I = (0.25, 0.125)
MAIN_J = (0.125, 0.25)


VMEM = pl.BlockSpec(memory_space=pltpu.VMEM)
SMEM = pl.BlockSpec(memory_space=pltpu.SMEM)
ANY = pl.BlockSpec(memory_space=pl.ANY)


def roll(x, shift, axis):
    return pltpu.roll(x, shift % x.shape[axis], axis)


def lanes(shape):
    return lax.broadcasted_iota(jnp.int32, shape, len(shape) - 1)


def rows(shape):
    return lax.broadcasted_iota(jnp.int32, shape, len(shape) - 2)


def pack_rows(
    rows_ref, u_hbm, table_hbm, bed_hbm, mask_hbm, up_ref, down_ref, geo_ref, u_ref, ints_ref, sems
):
    layers = u_ref.shape[2]
    moves = [
        (u_hbm, u_ref),
        (mask_hbm, ints_ref.at[0]),
        (bed_hbm, ints_ref.at[1]),
        (table_hbm.at[rows_ref[0]], geo_ref.at[2]),
        (table_hbm.at[rows_ref[1]], geo_ref.at[3]),
    ]
    copies = [pltpu.make_async_copy(*move, sems.at[i]) for i, move in enumerate(moves)]
    for copy in copies:
        copy.start()
    for copy in copies[1:]:
        copy.wait()
    geo_ref[0] = ints_ref[0].astype(jnp.float32)
    geo_ref[1] = ints_ref[1].astype(jnp.float32) * bed_unit
    copies[0].wait()
    low = rows((8, 128)) < HALO
    for layer in range(layers + 1):
        for pair in range(2):
            tiles = [
                u_ref[s, pair, layer] if layer < layers else geo_ref[2 * pair + s] for s in range(2)
            ]
            top = [tile[0:8] for tile in tiles]
            end = [tile[8:16] for tile in tiles]
            up_ref[layer, pair] = jnp.where(low, roll(end[0], HALO, 0), end[1])
            down_ref[layer, pair] = jnp.where(low, top[0], roll(top[1], HALO, 0))


def pack_columns(u_ref, geo_ref, below_ref, above_ref, outer_ref, strip_ref, right_ref, left_ref):
    layers = u_ref.shape[2]
    low = rows((8, 128)) < HALO
    lane = lanes((8, 128))
    used = lane < 4 * STRIP
    place = lane % STRIP
    slot = place // HALO
    zero = jnp.zeros((8, 128), jnp.float32)
    sent_right = [[zero] * 3 for _ in range(2)]
    sent_left = [[zero] * 3 for _ in range(2)]
    for layer in range(layers + 1):
        outer = []
        for pair in range(2):
            below = below_ref[layer, pair]
            above = above_ref[layer, pair]
            outer.append(jnp.where(low, above, roll(below, HALO, 0)))
            outer.append(jnp.where(low, roll(above, HALO, 0), below))
        for k in range(4):
            outer_ref[layer, k] = outer[k]
        for t in range(3):
            strip = zero
            for k in range(4):
                if t == 2:
                    tile = outer[k]
                elif layer < layers:
                    tile = u_ref[k % 2, k // 2, layer, 8 * t : 8 * t + 8]
                else:
                    tile = geo_ref[k, 8 * t : 8 * t + 8]
                at = lane - STRIP * k
                strip = jnp.where((at >= 4) & (at < 12), roll(tile, STRIP * k + 4, 1), strip)
                strip = jnp.where((at >= 12) & (at < 20), roll(tile, STRIP * k + 12 - 120, 1), strip)
            strip_ref[layer, 8 * t : 8 * t + 8] = strip
            group, index = layer // GROUPED, layer % GROUPED
            here = used & (slot == index)
            sent_right[group][t] = jnp.where(
                here, roll(strip, HALO * index - 16, 1), sent_right[group][t]
            )
            sent_left[group][t] = jnp.where(
                here, roll(strip, HALO * index - 4, 1), sent_left[group][t]
            )
    for group in range(2):
        for t in range(3):
            right_ref[group, 8 * t : 8 * t + 8] = sent_right[group][t]
            left_ref[group, 8 * t : 8 * t + 8] = sent_left[group][t]


def operator(
    plane_ref, u_ref, geo_ref, outer_ref, strip_ref, from_left_ref, from_right_ref,
    residual_ref, image_ref, start_ref, gram_ref,
    wide_ref, roots_ref, scale_ref, field_ref, next_ref, *, total_x,
):
    layers = u_ref.shape[2]
    shape = (24, 128)
    lane = lanes(shape)
    row = rows(shape)
    used = lane < 4 * STRIP
    place = lane % STRIP
    number = lane // STRIP

    def around_i(x):
        return roll(x, 1, 0) + roll(x, -1, 0)

    def around_j(x):
        return roll(x, 1, 1) + roll(x, -1, 1)

    geo_strip = None
    for layer in range(layers + 1):
        group, index = layer // GROUPED, layer % GROUPED
        strip = strip_ref[layer]
        strip = jnp.where(used & (place < 4), roll(from_left_ref[group], -HALO * index, 1), strip)
        strip = jnp.where(used & (place >= 20), roll(from_right_ref[group], 20 - HALO * index, 1), strip)
        if layer < layers:
            wide_ref[layer] = strip
        else:
            geo_strip = strip

    def spread_strip(source, to):
        result = jnp.zeros(shape, jnp.float32)
        for k in range(4):
            result = jnp.where(number == k, roll(source, STRIP * (k - to), 1), result)
        return result

    def main_geo(k):
        return jnp.concatenate([geo_ref[k], outer_ref[layers, k]], axis=0)

    def main(k, layer):
        return jnp.concatenate([u_ref[k % 2, k // 2, layer], outer_ref[layer, k]], axis=0)

    mask = main_geo(0)
    bed = main_geo(1)
    strip_mask = spread_strip(geo_strip, 0)
    strip_bed = spread_strip(geo_strip, 1)
    strip_friction = jnp.where(lane < 2 * STRIP, roll(geo_strip, -2 * STRIP, 1), geo_strip)
    position = jnp.where(row < 20, row, row - 24).astype(jnp.float32) + plane_ref[0]
    thickness = 1.0 + 2.0 * position / (total_x - 1)

    def forces(cover, ground):
        slope_x = (roll(ground, -1, 0) - roll(ground, 1, 0)) * 0.5
        slope_y = (roll(ground, -1, 1) - roll(ground, 1, 1)) * 0.5
        return -(cover * thickness * slope_x), -(cover * thickness * slope_y)

    main_force = forces(mask, bed)
    strip_x, strip_y = forces(strip_mask, strip_bed)
    strip_force = jnp.where(lane < 2 * STRIP, strip_x, strip_y)
    bare = 1.0 - mask
    strip_bare = 1.0 - strip_mask

    def viscosity(u, v, below_u, below_v, above_u, above_v, cover):
        stretch_x = roll(u, -1, 0) - roll(u, 1, 0)
        stretch_y = roll(v, -1, 1) - roll(v, 1, 1)
        shear = (roll(u, -1, 1) - roll(u, 1, 1)) + (roll(v, -1, 0) - roll(v, 1, 0))
        rise_u = above_u - below_u
        rise_v = above_v - below_v
        strain = stretch_x * stretch_x + stretch_y * (stretch_y + stretch_x)
        strain = strain + 0.25 * (shear * shear + (rise_u * rise_u + rise_v * rise_v))
        return cover * jnp.exp(jnp.log(0.25 * strain + 0.1) * (-1.0 / 6.0))

    zero = jnp.zeros(shape, jnp.float32)

    def column(get, z):
        return get(z) if 0 <= z < layers else zero

    for s in range(2):
        for z in range(layers):
            get_u, get_v = (lambda y, s=s: main(s, y)), (lambda y, s=s: main(2 + s, y))
            roots_ref[s, z] = viscosity(
                get_u(z), get_v(z), column(get_u, z - 1), column(get_v, z - 1),
                column(get_u, z + 1), column(get_v, z + 1), mask,
            )
    for z in range(layers):
        get_u = lambda y: wide_ref[y]

        def get_v(y):
            return roll(wide_ref[y], -2 * STRIP, 1)

        found = viscosity(
            get_u(z), get_v(z), column(get_u, z - 1), column(get_v, z - 1),
            column(get_u, z + 1), column(get_v, z + 1), strip_mask,
        )
        roots_ref[2, z] = jnp.where(lane < 2 * STRIP, found, roll(found, 2 * STRIP, 1))

    side_i = jnp.where(lane < 2 * STRIP, MAIN_I[0], MAIN_I[1])
    side_j = jnp.where(lane < 2 * STRIP, MAIN_J[0], MAIN_J[1])
    for s in range(3):
        for z in range(layers):
            centre = roots_ref[s, z]
            if z > 0 and z + 1 < layers:
                centre = centre + 0.5 * (roots_ref[s, z - 1] + roots_ref[s, z + 1])
            elif z > 0:
                centre = centre + 0.5 * roots_ref[s, z - 1]
            else:
                centre = centre + 0.5 * roots_ref[s, z + 1]
            along_i = around_i(centre)
            along_j = around_j(centre)
            both = centre + 0.03125 * around_j(along_i)
            if s < 2:
                for c in range(2):
                    scale_ref[2 * c + s, z] = both + MAIN_I[c] * along_i + MAIN_J[c] * along_j
            else:
                scale_ref[4, z] = both + side_i * along_i + side_j * along_j

    def apply(k, get, put):
        if k < 4:
            weight_i, weight_j = MAIN_I[k // 2], MAIN_J[k // 2]
            friction = mask * main_geo(2 + k % 2) + bare
            empty, roots = bare, k % 2
        else:
            weight_i, weight_j = side_i, side_j
            friction = strip_mask * strip_friction + strip_bare
            empty, roots = strip_bare, 2

        def filtered(z):
            product = roots_ref[roots, z] * get(z)
            product = product + weight_i * around_i(product)
            return product + weight_j * around_j(product)

        before, now = None, filtered(0)
        for z in range(layers):
            after = filtered(z + 1) if z + 1 < layers else None
            if before is None:
                total = now + 0.5 * after
            elif after is None:
                total = now + 0.5 * before
            else:
                total = now + 0.5 * (before + after)
            field = get(z)
            result = 4.0 * roots_ref[roots, z] * (scale_ref[k, z] * field - total)
            put(z, result + (friction if z == 0 else empty) * field)
            before, now = now, after

    sums = []
    for k in range(5):
        cover = mask if k < 4 else strip_mask
        force = main_force[k // 2] if k < 4 else strip_force

        def start(z, k=k, cover=cover):
            return cover * (main(k, z) if k < 4 else wide_ref[z])

        def put_residual(z, value, k=k, force=force):
            residual = force - value
            field_ref[z] = residual
            residual_ref[k, z] = residual[0:16]

        def put_image(z, value, k=k):
            next_ref[z] = value
            image_ref[k, z] = value[0:16]

        totals = [jnp.zeros((8, 128), jnp.float32)] * 4

        def put_second(z, value):
            for t in range(2):
                at = slice(8 * t, 8 * t + 8)
                r, a, b = field_ref[z, at], next_ref[z, at], value[at]
                totals[0] = totals[0] + r * r
                totals[1] = totals[1] + r * a
                totals[2] = totals[2] + a * a
                totals[3] = totals[3] + a * b

        apply(k, start, put_residual)
        apply(k, lambda z: field_ref[z], put_image)
        apply(k, lambda z: next_ref[z], put_second)
        sums.append(totals)

    for c in range(2):
        for z in range(layers):
            start_ref[c, z] = mask[0:16] * u_ref[0, c, z] + mask[0:16] * u_ref[1, c, z]

    lane8 = lanes((8, 128))
    inside = (lane8 >= HALO) & (lane8 < 128 - HALO)
    spot = lane8 % STRIP
    edge = (lane8 < 4 * STRIP) & (((spot >= 4) & (spot < 8)) | ((spot >= 16) & (spot < 20)))
    row8 = rows((8, 128))
    table = jnp.zeros((8, 128), jnp.float32)
    for g in range(4):
        for s in range(2):
            value = jnp.where(inside, sums[s][g] + sums[2 + s][g], 0.0)
            value = value + jnp.where(edge & ((lane8 // STRIP) % 2 == s), sums[4][g], 0.0)
            value = jnp.sum(value, axis=0, keepdims=True)
            table = jnp.where(row8 == 2 * g + s, value, table)
    table = jnp.sum(table, axis=1, keepdims=True)
    line = jnp.sum(jnp.where(lane8 == row8, table, 0.0), axis=0, keepdims=True)
    gram_ref[...] = jnp.broadcast_to(line, gram_ref.shape)


def combine(gram_ref, residual_ref, image_ref, start_ref, out_ref):
    layers = start_ref.shape[1]
    shape = (8, 128)
    lane = lanes(shape)
    total = jnp.broadcast_to(jnp.sum(gram_ref[...], axis=0, keepdims=True), shape)
    rr = total
    ra = roll(total, -2, 1)
    aa = roll(total, -4, 1)
    ab = roll(total, -6, 1)
    first = rr / ra
    norm_next = rr - 2.0 * first * ra + first * first * aa
    growth = 1.0 + norm_next / rr
    curve = growth * growth * ra - 2.0 * growth * first * aa + first * first * ab
    second = norm_next / curve
    residual_part = first + second * growth
    image_part = second * first
    ks = [jnp.broadcast_to(residual_part[:, s : s + 1], shape) for s in range(2)]
    ms = [jnp.broadcast_to(image_part[:, s : s + 1], shape) for s in range(2)]
    odd = (lane // STRIP) % 2 == 1
    k_side = jnp.where(odd, ks[1], ks[0])
    m_side = jnp.where(odd, ms[1], ms[0])
    for z in range(layers):
        for t in range(2):
            at = slice(8 * t, 8 * t + 8)
            side = k_side * residual_ref[4, z, at] - m_side * image_ref[4, z, at]
            side = side + roll(side, -STRIP, 1)
            for c in range(2):
                step = ks[0] * residual_ref[2 * c, z, at] - ms[0] * image_ref[2 * c, z, at]
                step = step + ks[1] * residual_ref[2 * c + 1, z, at]
                step = step - ms[1] * image_ref[2 * c + 1, z, at]
                base = 2 * STRIP * c
                step = jnp.where(lane < HALO, roll(side, -(base + 4), 1), step)
                step = jnp.where(lane >= 128 - HALO, roll(side, 124 - base - 16, 1), step)
                out_ref[c, z, at] = start_ref[c, z, at] + step


def f32(*shape):
    return pltpu.VMEM(shape, jnp.float32)


def call(kernel, outs, ins, name, scratch=(), in_specs=None):
    specs = in_specs or [VMEM] * len(ins)
    ins = [
        pltpu.with_memory_space_constraint(x, pltpu.VMEM) if spec is VMEM else x
        for x, spec in zip(ins, specs)
    ]
    return pl.pallas_call(
        kernel,
        in_specs=specs,
        out_specs=[VMEM] * len(outs),
        out_shape=list(outs),
        scratch_shapes=list(scratch),
        name=name,
    )(*ins)


def swap_sides(forward, backward, axis):
    count = lax.axis_size(axis)
    up = [(i, i + 1) for i in range(count - 1)]
    down = [(i + 1, i) for i in range(count - 1)]
    return lax.ppermute(forward, axis, up), lax.ppermute(backward, axis, down)


def copies_of_all(copies, axis):
    return lax.all_to_all(copies, axis, 0, 0, tiled=True)


def body(u_prior, friction_rows, friction_table, bed_fixed, ice_mask):
    members, parts, layers, rows_x, rows_y = u_prior.shape
    total_x = rows_x * lax.axis_size("plane")
    up, down, geo, u_near = call(
        pack_rows,
        [
            f32(layers + 1, 2, 8, rows_y),
            f32(layers + 1, 2, 8, rows_y),
            f32(4, rows_x, rows_y),
            f32(*u_prior.shape),
        ],
        [friction_rows, u_prior, friction_table, bed_fixed, ice_mask],
        "pack_rows",
        scratch=[pltpu.VMEM((2, rows_x, rows_y), jnp.int32), pltpu.SemaphoreType.DMA((5,))],
        in_specs=[SMEM, ANY, ANY, ANY, ANY],
    )
    below, above = swap_sides(up, down, "plane")
    outer, strip, right, left = call(
        pack_columns,
        [f32(layers + 1, 4, 8, rows_y), f32(layers + 1, 24, 128), f32(2, 24, 128), f32(2, 24, 128)],
        [u_near, geo, below, above],
        "pack_columns",
    )
    from_left, from_right = swap_sides(right, left, "planey")
    plane_start = (lax.axis_index("plane") * rows_x).astype(jnp.float32).reshape(1)
    ins = [u_near, geo, outer, strip, from_left, from_right]
    residual, image, start, gram = call(
        lambda *refs: operator(*refs, total_x=total_x),
        [
            f32(5, layers, rows_x, 128),
            f32(5, layers, rows_x, 128),
            f32(2, layers, rows_x, 128),
            f32(lax.axis_size("plane"), 128),
        ],
        [plane_start] + ins,
        "operator",
        scratch=[
            pltpu.VMEM((layers, 24, 128), jnp.float32),
            pltpu.VMEM((3, layers, 24, 128), jnp.float32),
            pltpu.VMEM((5, layers, 24, 128), jnp.float32),
            pltpu.VMEM((layers, 24, 128), jnp.float32),
            pltpu.VMEM((layers, 24, 128), jnp.float32),
        ],
        in_specs=[SMEM] + [VMEM] * len(ins),
    )
    gathered = copies_of_all(gram, "plane")
    line = jnp.sum(gathered, axis=0, keepdims=True)
    gathered = copies_of_all(jnp.broadcast_to(line, (lax.axis_size("planey"), 128)), "planey")
    (local_sum,) = call(
        combine, [f32(2, layers, rows_x, 128)], [gathered, residual, image, start], "combine"
    )
    summed = lax.all_gather(local_sum, "ens").sum(axis=0)
    return summed / (members * lax.axis_size("ens"))


def solution(mesh):
    in_specs = (
        P(("group", "ens"), None, None, "plane", "planey"),
        P(("group", "ens")),
        P("group", "plane", "planey"),
        P("plane", "planey"),
        P("plane", "planey"),
    )
    out_specs = P("group", None, "plane", "planey")
    return jax.shard_map(body, mesh=mesh, in_specs=in_specs, out_specs=out_specs, check_vma=False)
```

```python
import jax
import jax.numpy as jnp
from jax import lax
from jax.experimental import pallas as pl
from jax.experimental.pallas import tpu as pltpu
from jax.sharding import PartitionSpec as P

bed_unit = 2.0 ** (-29)
HALO = 4
STRIP = 24
GROUPED = STRIP // HALO
MAIN_I = (0.25, 0.125)
MAIN_J = (0.125, 0.25)


VMEM = pl.BlockSpec(memory_space=pltpu.VMEM)
SMEM = pl.BlockSpec(memory_space=pltpu.SMEM)
ANY = pl.BlockSpec(memory_space=pl.ANY)


def roll(x, shift, axis):
    return pltpu.roll(x, shift % x.shape[axis], axis)


def lanes(shape):
    return lax.broadcasted_iota(jnp.int32, shape, len(shape) - 1)


def rows(shape):
    return lax.broadcasted_iota(jnp.int32, shape, len(shape) - 2)


def pack_rows(
    rows_ref, place_ref, u_hbm, table_hbm, bed_hbm, mask_hbm,
    odd_ref, even_ref, geo_ref, u_ref, ints_ref, sems,
):
    layers = u_ref.shape[2]
    moves = [
        (u_hbm, u_ref),
        (mask_hbm, ints_ref.at[0]),
        (bed_hbm, ints_ref.at[1]),
        (table_hbm.at[rows_ref[0]], geo_ref.at[2]),
        (table_hbm.at[rows_ref[1]], geo_ref.at[3]),
    ]
    copies = [pltpu.make_async_copy(*move, sems.at[i]) for i, move in enumerate(moves)]
    for copy in copies:
        copy.start()
    for copy in copies[1:]:
        copy.wait()
    geo_ref[0] = ints_ref[0].astype(jnp.float32)
    geo_ref[1] = ints_ref[1].astype(jnp.float32) * bed_unit
    copies[0].wait()
    low = rows((8, 128)) < HALO
    odd = place_ref[0] % 2 == 1
    for layer in range(layers + 1):
        for pair in range(2):
            tiles = [
                u_ref[s, pair, layer] if layer < layers else geo_ref[2 * pair + s] for s in range(2)
            ]
            top = [tile[0:8] for tile in tiles]
            end = [tile[8:16] for tile in tiles]
            up = jnp.where(low, roll(end[0], HALO, 0), end[1])
            down = jnp.where(low, top[0], roll(top[1], HALO, 0))
            odd_ref[layer, pair] = jnp.where(odd, up, down)
            even_ref[layer, pair] = jnp.where(odd, down, up)


def pack_columns(
    row_place_ref, column_place_ref, u_ref, geo_ref, by_odd_ref, by_even_ref,
    outer_ref, strip_ref, odd_ref, even_ref,
):
    layers = u_ref.shape[2]
    low = rows((8, 128)) < HALO
    lane = lanes((8, 128))
    used = lane < 4 * STRIP
    slot = (lane % STRIP) // HALO
    zero = jnp.zeros((8, 128), jnp.float32)
    odd = row_place_ref[0] % 2 == 1
    for layer in range(layers + 1):
        outer = []
        for pair in range(2):
            by_odd = by_odd_ref[layer, pair]
            by_even = by_even_ref[layer, pair]
            below = jnp.where(odd, by_even, by_odd)
            above = jnp.where(odd, by_odd, by_even)
            outer.append(jnp.where(low, above, roll(below, HALO, 0)))
            outer.append(jnp.where(low, roll(above, HALO, 0), below))
        for k in range(4):
            outer_ref[layer, k] = outer[k]
        for t in range(3):
            strip = zero
            for k in range(4):
                if t == 2:
                    tile = outer[k]
                elif layer < layers:
                    tile = u_ref[k % 2, k // 2, layer, 8 * t : 8 * t + 8]
                else:
                    tile = geo_ref[k, 8 * t : 8 * t + 8]
                at = lane - STRIP * k
                strip = jnp.where((at >= 4) & (at < 12), roll(tile, STRIP * k + 4, 1), strip)
                strip = jnp.where((at >= 12) & (at < 20), roll(tile, STRIP * k + 12 - 120, 1), strip)
            strip_ref[layer, 8 * t : 8 * t + 8] = strip

    def send(t, carry):
        at = pl.ds(pl.multiple_of(8 * t, 8), 8)
        swapped = column_place_ref[0] % 2 == 1
        for group in range(2):
            right, left = zero, zero
            for index in range(min(GROUPED, layers + 1 - GROUPED * group)):
                strip = strip_ref[GROUPED * group + index, at]
                here = used & (slot == index)
                right = jnp.where(here, roll(strip, HALO * index - 16, 1), right)
                left = jnp.where(here, roll(strip, HALO * index - 4, 1), left)
            odd_ref[group, at] = jnp.where(swapped, right, left)
            even_ref[group, at] = jnp.where(swapped, left, right)
        return carry

    lax.fori_loop(0, 3, send, 0)


def operator(
    row_place_ref, column_place_ref, u_ref, geo_ref, outer_ref, strip_ref, by_odd_ref, by_even_ref,
    residual_ref, image_ref, start_ref, gram_ref,
    wide_ref, roots_ref, scale_ref, field_ref, next_ref, *, total_x,
):
    layers = u_ref.shape[2]
    shape = (24, 128)
    lane = lanes(shape)
    row = rows(shape)
    used = lane < 4 * STRIP
    place = lane % STRIP
    number = lane // STRIP

    def around_i(x):
        return roll(x, 1, 0) + roll(x, -1, 0)

    def around_j(x):
        return roll(x, 1, 1) + roll(x, -1, 1)

    geo_strip = None
    odd = column_place_ref[0] % 2 == 1
    from_left = [jnp.where(odd, by_even_ref[g], by_odd_ref[g]) for g in range(2)]
    from_right = [jnp.where(odd, by_odd_ref[g], by_even_ref[g]) for g in range(2)]
    for layer in range(layers + 1):
        group, index = layer // GROUPED, layer % GROUPED
        strip = strip_ref[layer]
        strip = jnp.where(used & (place < 4), roll(from_left[group], -HALO * index, 1), strip)
        strip = jnp.where(used & (place >= 20), roll(from_right[group], 20 - HALO * index, 1), strip)
        if layer < layers:
            wide_ref[layer] = strip
        else:
            geo_strip = strip

    def spread_strip(source, to):
        result = jnp.zeros(shape, jnp.float32)
        for k in range(4):
            result = jnp.where(number == k, roll(source, STRIP * (k - to), 1), result)
        return result

    def main_geo(k):
        return jnp.concatenate([geo_ref[k], outer_ref[layers, k]], axis=0)

    def main(k, layer):
        return jnp.concatenate([u_ref[k % 2, k // 2, layer], outer_ref[layer, k]], axis=0)

    mask = main_geo(0)
    bed = main_geo(1)
    strip_mask = spread_strip(geo_strip, 0)
    strip_bed = spread_strip(geo_strip, 1)
    strip_friction = jnp.where(lane < 2 * STRIP, roll(geo_strip, -2 * STRIP, 1), geo_strip)
    position = jnp.where(row < 20, row, row - 24) + row_place_ref[0] * 16
    position = position.astype(jnp.float32)
    thickness = 1.0 + 2.0 * position / (total_x - 1)

    def forces(cover, ground):
        slope_x = (roll(ground, -1, 0) - roll(ground, 1, 0)) * 0.5
        slope_y = (roll(ground, -1, 1) - roll(ground, 1, 1)) * 0.5
        return -(cover * thickness * slope_x), -(cover * thickness * slope_y)

    main_force = forces(mask, bed)
    strip_x, strip_y = forces(strip_mask, strip_bed)
    strip_force = jnp.where(lane < 2 * STRIP, strip_x, strip_y)
    bare = 1.0 - mask
    strip_bare = 1.0 - strip_mask

    def viscosity(u, v, below_u, below_v, above_u, above_v, cover):
        stretch_x = roll(u, -1, 0) - roll(u, 1, 0)
        stretch_y = roll(v, -1, 1) - roll(v, 1, 1)
        shear = (roll(u, -1, 1) - roll(u, 1, 1)) + (roll(v, -1, 0) - roll(v, 1, 0))
        rise_u = above_u - below_u
        rise_v = above_v - below_v
        strain = stretch_x * stretch_x + stretch_y * (stretch_y + stretch_x)
        strain = strain + 0.25 * (shear * shear + (rise_u * rise_u + rise_v * rise_v))
        return cover * jnp.exp(jnp.log(0.25 * strain + 0.1) * (-1.0 / 6.0))

    zero = jnp.zeros(shape, jnp.float32)

    def column(get, z):
        return get(z) if 0 <= z < layers else zero

    for s in range(2):
        for z in range(layers):
            get_u, get_v = (lambda y, s=s: main(s, y)), (lambda y, s=s: main(2 + s, y))
            roots_ref[s, z] = viscosity(
                get_u(z), get_v(z), column(get_u, z - 1), column(get_v, z - 1),
                column(get_u, z + 1), column(get_v, z + 1), mask,
            )
    for z in range(layers):
        get_u = lambda y: wide_ref[y]

        def get_v(y):
            return roll(wide_ref[y], -2 * STRIP, 1)

        found = viscosity(
            get_u(z), get_v(z), column(get_u, z - 1), column(get_v, z - 1),
            column(get_u, z + 1), column(get_v, z + 1), strip_mask,
        )
        roots_ref[2, z] = jnp.where(lane < 2 * STRIP, found, roll(found, 2 * STRIP, 1))

    side_i = jnp.where(lane < 2 * STRIP, MAIN_I[0], MAIN_I[1])
    side_j = jnp.where(lane < 2 * STRIP, MAIN_J[0], MAIN_J[1])
    for s in range(3):
        for z in range(layers):
            centre = roots_ref[s, z]
            if z > 0 and z + 1 < layers:
                centre = centre + 0.5 * (roots_ref[s, z - 1] + roots_ref[s, z + 1])
            elif z > 0:
                centre = centre + 0.5 * roots_ref[s, z - 1]
            else:
                centre = centre + 0.5 * roots_ref[s, z + 1]
            along_i = around_i(centre)
            along_j = around_j(centre)
            both = centre + 0.03125 * around_j(along_i)
            if s < 2:
                for c in range(2):
                    scale_ref[2 * c + s, z] = both + MAIN_I[c] * along_i + MAIN_J[c] * along_j
            else:
                scale_ref[4, z] = both + side_i * along_i + side_j * along_j

    def apply(k, get, put):
        if k < 4:
            weight_i, weight_j = MAIN_I[k // 2], MAIN_J[k // 2]
            friction = mask * main_geo(2 + k % 2) + bare
            empty, roots = bare, k % 2
        else:
            weight_i, weight_j = side_i, side_j
            friction = strip_mask * strip_friction + strip_bare
            empty, roots = strip_bare, 2

        def filtered(z):
            product = roots_ref[roots, z] * get(z)
            product = product + weight_i * around_i(product)
            return product + weight_j * around_j(product)

        before, now = None, filtered(0)
        for z in range(layers):
            after = filtered(z + 1) if z + 1 < layers else None
            if before is None:
                total = now + 0.5 * after
            elif after is None:
                total = now + 0.5 * before
            else:
                total = now + 0.5 * (before + after)
            field = get(z)
            result = 4.0 * roots_ref[roots, z] * (scale_ref[k, z] * field - total)
            put(z, result + (friction if z == 0 else empty) * field)
            before, now = now, after

    sums = []
    for k in range(5):
        cover = mask if k < 4 else strip_mask
        force = main_force[k // 2] if k < 4 else strip_force

        def start(z, k=k, cover=cover):
            return cover * (main(k, z) if k < 4 else wide_ref[z])

        def put_residual(z, value, k=k, force=force):
            residual = force - value
            field_ref[z] = residual
            residual_ref[k, z] = residual[0:16]

        def put_image(z, value, k=k):
            next_ref[z] = value
            image_ref[k, z] = value[0:16]

        totals = [jnp.zeros((8, 128), jnp.float32)] * 4

        def put_second(z, value):
            for t in range(2):
                at = slice(8 * t, 8 * t + 8)
                r, a, b = field_ref[z, at], next_ref[z, at], value[at]
                totals[0] = totals[0] + r * r
                totals[1] = totals[1] + r * a
                totals[2] = totals[2] + a * a
                totals[3] = totals[3] + a * b

        apply(k, start, put_residual)
        apply(k, lambda z: field_ref[z], put_image)
        apply(k, lambda z: next_ref[z], put_second)
        sums.append(totals)

    for c in range(2):
        for z in range(layers):
            start_ref[c, z] = mask[0:16] * u_ref[0, c, z] + mask[0:16] * u_ref[1, c, z]

    lane8 = lanes((8, 128))
    inside = (lane8 >= HALO) & (lane8 < 128 - HALO)
    spot = lane8 % STRIP
    edge = (lane8 < 4 * STRIP) & (((spot >= 4) & (spot < 8)) | ((spot >= 16) & (spot < 20)))
    row8 = rows((8, 128))
    table = jnp.zeros((8, 128), jnp.float32)
    for g in range(4):
        for s in range(2):
            value = jnp.where(inside, sums[s][g] + sums[2 + s][g], 0.0)
            value = value + jnp.where(edge & ((lane8 // STRIP) % 2 == s), sums[4][g], 0.0)
            value = jnp.sum(value, axis=0, keepdims=True)
            table = jnp.where(row8 == 2 * g + s, value, table)
    table = jnp.sum(table, axis=1, keepdims=True)
    line = jnp.sum(jnp.where(lane8 == row8, table, 0.0), axis=0, keepdims=True)
    gram_ref[...] = jnp.broadcast_to(line, gram_ref.shape)


def combine(gram_ref, residual_ref, image_ref, start_ref, out_ref):
    layers = start_ref.shape[1]
    shape = (8, 128)
    lane = lanes(shape)
    total = jnp.broadcast_to(jnp.sum(gram_ref[...], axis=0, keepdims=True), shape)
    rr = total
    ra = roll(total, -2, 1)
    aa = roll(total, -4, 1)
    ab = roll(total, -6, 1)
    first = rr / ra
    norm_next = rr - 2.0 * first * ra + first * first * aa
    growth = 1.0 + norm_next / rr
    curve = growth * growth * ra - 2.0 * growth * first * aa + first * first * ab
    second = norm_next / curve
    residual_part = first + second * growth
    image_part = second * first
    ks = [jnp.broadcast_to(residual_part[:, s : s + 1], shape) for s in range(2)]
    ms = [jnp.broadcast_to(image_part[:, s : s + 1], shape) for s in range(2)]
    odd = (lane // STRIP) % 2 == 1
    k_side = jnp.where(odd, ks[1], ks[0])
    m_side = jnp.where(odd, ms[1], ms[0])
    for z in range(layers):
        for t in range(2):
            at = slice(8 * t, 8 * t + 8)
            side = k_side * residual_ref[4, z, at] - m_side * image_ref[4, z, at]
            side = side + roll(side, -STRIP, 1)
            for c in range(2):
                step = ks[0] * residual_ref[2 * c, z, at] - ms[0] * image_ref[2 * c, z, at]
                step = step + ks[1] * residual_ref[2 * c + 1, z, at]
                step = step - ms[1] * image_ref[2 * c + 1, z, at]
                base = 2 * STRIP * c
                step = jnp.where(lane < HALO, roll(side, -(base + 4), 1), step)
                step = jnp.where(lane >= 128 - HALO, roll(side, 124 - base - 16, 1), step)
                out_ref[c, z, at] = start_ref[c, z, at] + step


def f32(*shape):
    return pltpu.VMEM(shape, jnp.float32)


def call(kernel, outs, ins, name, scratch=(), in_specs=None):
    specs = in_specs or [VMEM] * len(ins)
    ins = [
        pltpu.with_memory_space_constraint(x, pltpu.VMEM) if spec is VMEM else x
        for x, spec in zip(ins, specs)
    ]
    return pl.pallas_call(
        kernel,
        in_specs=specs,
        out_specs=[VMEM] * len(outs),
        out_shape=list(outs),
        scratch_shapes=list(scratch),
        name=name,
    )(*ins)


def swap_sides(by_odd, by_even, axis):
    count = lax.axis_size(axis)

    def swap(message, first):
        pairs = [(i, i + 1) for i in range(first, count - 1, 2)]
        return lax.ppermute(message, axis, pairs + [(j, i) for i, j in pairs])

    return swap(by_odd, 1), swap(by_even, 0)


def copies_of_all(copies, axis):
    return lax.all_to_all(copies, axis, 0, 0, tiled=True)


def body(u_prior, friction_rows, friction_table, bed_fixed, ice_mask):
    members, parts, layers, rows_x, rows_y = u_prior.shape
    total_x = rows_x * lax.axis_size("plane")
    row_place = lax.axis_index("plane").reshape(1)
    column_place = lax.axis_index("planey").reshape(1)
    by_odd, by_even, geo, u_near = call(
        pack_rows,
        [
            f32(layers + 1, 2, 8, rows_y),
            f32(layers + 1, 2, 8, rows_y),
            f32(4, rows_x, rows_y),
            f32(*u_prior.shape),
        ],
        [friction_rows, row_place, u_prior, friction_table, bed_fixed, ice_mask],
        "pack_rows",
        scratch=[pltpu.VMEM((2, rows_x, rows_y), jnp.int32), pltpu.SemaphoreType.DMA((5,))],
        in_specs=[SMEM, SMEM, ANY, ANY, ANY, ANY],
    )
    by_odd, by_even = swap_sides(by_odd, by_even, "plane")
    outer, strip, side_odd, side_even = call(
        pack_columns,
        [f32(layers + 1, 4, 8, rows_y), f32(layers + 1, 24, 128), f32(2, 24, 128), f32(2, 24, 128)],
        [row_place, column_place, u_near, geo, by_odd, by_even],
        "pack_columns",
        in_specs=[SMEM, SMEM] + [VMEM] * 4,
    )
    side_odd, side_even = swap_sides(side_odd, side_even, "planey")
    ins = [u_near, geo, outer, strip, side_odd, side_even]
    residual, image, start, gram = call(
        lambda *refs: operator(*refs, total_x=total_x),
        [
            f32(5, layers, rows_x, 128),
            f32(5, layers, rows_x, 128),
            f32(2, layers, rows_x, 128),
            f32(lax.axis_size("plane"), 128),
        ],
        [row_place, column_place] + ins,
        "operator",
        scratch=[
            pltpu.VMEM((layers, 24, 128), jnp.float32),
            pltpu.VMEM((3, layers, 24, 128), jnp.float32),
            pltpu.VMEM((5, layers, 24, 128), jnp.float32),
            pltpu.VMEM((layers, 24, 128), jnp.float32),
            pltpu.VMEM((layers, 24, 128), jnp.float32),
        ],
        in_specs=[SMEM, SMEM] + [VMEM] * len(ins),
    )
    gathered = copies_of_all(gram, "plane")
    line = jnp.sum(gathered, axis=0, keepdims=True)
    gathered = copies_of_all(jnp.broadcast_to(line, (lax.axis_size("planey"), 128)), "planey")
    (local_sum,) = call(
        combine, [f32(2, layers, rows_x, 128)], [gathered, residual, image, start], "combine"
    )
    summed = lax.all_gather(local_sum, "ens").sum(axis=0)
    return summed / (members * lax.axis_size("ens"))


def solution(mesh):
    in_specs = (
        P(("group", "ens"), None, None, "plane", "planey"),
        P(("group", "ens")),
        P("group", "plane", "planey"),
        P("plane", "planey"),
        P("plane", "planey"),
    )
    out_specs = P("group", None, "plane", "planey")
    return jax.shard_map(body, mesh=mesh, in_specs=in_specs, out_specs=out_specs, check_vma=False)
```

```python
import jax
import jax.numpy as jnp
from jax import lax
from jax.experimental import pallas as pl
from jax.experimental.pallas import tpu as pltpu
from jax.sharding import PartitionSpec as P

bed_unit = 2.0 ** (-29)
HALO = 4
STRIP = 24
GROUPED = STRIP // HALO
MAIN_I = (0.25, 0.125)
MAIN_J = (0.125, 0.25)


VMEM = pl.BlockSpec(memory_space=pltpu.VMEM)
SMEM = pl.BlockSpec(memory_space=pltpu.SMEM)
ANY = pl.BlockSpec(memory_space=pl.ANY)


def roll(x, shift, axis):
    return pltpu.roll(x, shift % x.shape[axis], axis)


def lanes(shape):
    return lax.broadcasted_iota(jnp.int32, shape, len(shape) - 1)


def rows(shape):
    return lax.broadcasted_iota(jnp.int32, shape, len(shape) - 2)


def pack_rows(
    place_ref, rows_hbm, u_hbm, table_hbm, bed_hbm, mask_hbm,
    odd_ref, even_ref, geo_ref, u_ref, rows_ref, table_ref, ints_ref, sems,
):
    layers = u_ref.shape[2]
    moves = [
        (u_hbm, u_ref),
        (rows_hbm, rows_ref),
        (table_hbm, table_ref),
        (mask_hbm, ints_ref.at[0]),
        (bed_hbm, ints_ref.at[1]),
    ]
    copies = [pltpu.make_async_copy(*move, sems.at[i]) for i, move in enumerate(moves)]
    for copy in copies:
        copy.start()
    for copy in copies:
        copy.wait()
    geo_ref[0] = ints_ref[0].astype(jnp.float32)
    geo_ref[1] = ints_ref[1].astype(jnp.float32) * bed_unit
    for s in range(2):
        geo_ref[2 + s] = table_ref[rows_ref[s]]
    low = rows((8, 128)) < HALO
    odd = place_ref[0] % 2 == 1
    for layer in range(layers + 1):
        for pair in range(2):
            tiles = [
                u_ref[s, pair, layer] if layer < layers else geo_ref[2 * pair + s] for s in range(2)
            ]
            top = [tile[0:8] for tile in tiles]
            end = [tile[8:16] for tile in tiles]
            up = jnp.where(low, roll(end[0], HALO, 0), end[1])
            down = jnp.where(low, top[0], roll(top[1], HALO, 0))
            odd_ref[layer, pair] = jnp.where(odd, up, down)
            even_ref[layer, pair] = jnp.where(odd, down, up)


def pack_columns(
    row_place_ref, column_place_ref, u_ref, geo_ref, by_odd_ref, by_even_ref,
    outer_ref, strip_ref, odd_ref, even_ref,
):
    layers = u_ref.shape[2]
    low = rows((8, 128)) < HALO
    lane = lanes((8, 128))
    used = lane < 4 * STRIP
    slot = (lane % STRIP) // HALO
    zero = jnp.zeros((8, 128), jnp.float32)
    odd = row_place_ref[0] % 2 == 1
    for layer in range(layers + 1):
        outer = []
        for pair in range(2):
            by_odd = by_odd_ref[layer, pair]
            by_even = by_even_ref[layer, pair]
            below = jnp.where(odd, by_even, by_odd)
            above = jnp.where(odd, by_odd, by_even)
            outer.append(jnp.where(low, above, roll(below, HALO, 0)))
            outer.append(jnp.where(low, roll(above, HALO, 0), below))
        for k in range(4):
            outer_ref[layer, k] = outer[k]
        for t in range(3):
            strip = zero
            for k in range(4):
                if t == 2:
                    tile = outer[k]
                elif layer < layers:
                    tile = u_ref[k % 2, k // 2, layer, 8 * t : 8 * t + 8]
                else:
                    tile = geo_ref[k, 8 * t : 8 * t + 8]
                at = lane - STRIP * k
                strip = jnp.where((at >= 4) & (at < 12), roll(tile, STRIP * k + 4, 1), strip)
                strip = jnp.where((at >= 12) & (at < 20), roll(tile, STRIP * k + 12 - 120, 1), strip)
            strip_ref[layer, 8 * t : 8 * t + 8] = strip

    def send(t, carry):
        at = pl.ds(pl.multiple_of(8 * t, 8), 8)
        swapped = column_place_ref[0] % 2 == 1
        for group in range(2):
            right, left = zero, zero
            for index in range(min(GROUPED, layers + 1 - GROUPED * group)):
                strip = strip_ref[GROUPED * group + index, at]
                here = used & (slot == index)
                right = jnp.where(here, roll(strip, HALO * index - 16, 1), right)
                left = jnp.where(here, roll(strip, HALO * index - 4, 1), left)
            odd_ref[group, at] = jnp.where(swapped, right, left)
            even_ref[group, at] = jnp.where(swapped, left, right)
        return carry

    lax.fori_loop(0, 3, send, 0)


def around_i(x):
    return roll(x, 1, 0) + roll(x, -1, 0)


def around_j(x):
    return roll(x, 1, 1) + roll(x, -1, 1)


def forces(cover, ground, row_start, total_x):
    row = rows(cover.shape)
    position = (jnp.where(row < 20, row, row - 24) + row_start).astype(jnp.float32)
    thickness = 1.0 + 2.0 * position / (total_x - 1)
    slope_x = (roll(ground, -1, 0) - roll(ground, 1, 0)) * 0.5
    slope_y = (roll(ground, -1, 1) - roll(ground, 1, 1)) * 0.5
    return -(cover * thickness * slope_x), -(cover * thickness * slope_y)


def difference(get, z, layers):
    if z == 0:
        return get(1)
    if z + 1 == layers:
        return -get(z - 1)
    return get(z + 1) - get(z - 1)


def viscosity(get_u, get_v, z, layers, cover):
    u, v = get_u(z), get_v(z)
    stretch_x = roll(u, -1, 0) - roll(u, 1, 0)
    stretch_y = roll(v, -1, 1) - roll(v, 1, 1)
    shear = (roll(u, -1, 1) - roll(u, 1, 1)) + (roll(v, -1, 0) - roll(v, 1, 0))
    rise_u = difference(get_u, z, layers)
    rise_v = difference(get_v, z, layers)
    strain = stretch_x * stretch_x + stretch_y * (stretch_y + stretch_x)
    strain = strain + 0.25 * (shear * shear + (rise_u * rise_u + rise_v * rise_v))
    return cover * jnp.exp(jnp.log(0.25 * strain + 0.1) * (-1.0 / 6.0))


def with_neighbours(get, z, layers):
    if z == 0:
        return get(0) + 0.5 * get(1)
    if z + 1 == layers:
        return get(z) + 0.5 * get(z - 1)
    return get(z) + 0.5 * (get(z - 1) + get(z + 1))


def apply(get, put, roots, scale, weight_i, weight_j, friction, empty, layers, kept=24):
    def kept_rows(x):
        return x[0:kept] if x.ndim else x

    def filtered(z):
        product = roots(z) * get(z)
        product = (product + weight_i * around_i(product))[0:kept]
        return product + kept_rows(weight_j) * around_j(product)

    done = {}
    for z in range(layers + 1):
        if z < layers:
            done[z] = filtered(z)
        if z > 0:
            at = z - 1
            total = with_neighbours(lambda y: done[y], at, layers)
            field = get(at)[0:kept]
            result = 4.0 * roots(at)[0:kept] * (scale(at)[0:kept] * field - total)
            put(at, result + (friction if at == 0 else empty)[0:kept] * field)


def products(field, image, second, layers, totals):
    totals = list(totals)
    for z in range(layers):
        for t in range(2):
            at = slice(8 * t, 8 * t + 8)
            r, a, b = field(z)[at], image(z)[at], second(z)[at]
            for i, (x, y) in enumerate(((r, r), (r, a), (a, a), (a, b))):
                totals[i] = totals[i] + x * y
    return totals


def main_part(
    row_place_ref, u_ref, geo_ref, outer_ref,
    residual_ref, image_ref, start_ref, table_ref,
    wide_ref, roots_ref, scale_ref, field_ref, next_ref, second_ref, *, total_x,
):
    layers = u_ref.shape[2]
    row_start = row_place_ref[0] * 16

    def geo(k):
        return jnp.concatenate([geo_ref[k], outer_ref[layers, k]], axis=0)

    mask = geo(0)
    bare = 1.0 - mask
    force = forces(mask, geo(1), row_start, total_x)
    lane8 = lanes((8, 128))
    inside = (lane8 >= HALO) & (lane8 < 128 - HALO)
    row8 = rows((8, 128))
    table_ref[...] = jnp.zeros((8, 128), jnp.float32)

    def sample(s, carry):
        friction = mask * jnp.concatenate([geo_ref[2 + s], outer_ref[layers, 2 + s]], axis=0) + bare
        for c in range(2):
            for z in range(layers):
                wide_ref[c, z, 0:16] = u_ref[s, c, z]
                wide_ref[c, z, 16:24] = outer_ref[z, 2 * c + s]
        for z in range(layers):
            roots_ref[z] = viscosity(
                lambda y: wide_ref[0, y], lambda y: wide_ref[1, y], z, layers, mask
            )
        for z in range(layers):
            centre = with_neighbours(lambda y: roots_ref[y], z, layers)
            along_i = around_i(centre)
            along_j = around_j(centre)
            both = centre + 0.03125 * around_j(along_i)
            for c in range(2):
                scale_ref[c, z] = both + MAIN_I[c] * along_i + MAIN_J[c] * along_j

        def component(c, carry):
            first = c == 0
            weight_i = jnp.where(first, MAIN_I[0], MAIN_I[1])
            weight_j = jnp.where(first, MAIN_J[0], MAIN_J[1])
            pull = jnp.where(first, force[0], force[1])
            shared = (
                lambda z: roots_ref[z], lambda z: scale_ref[c, z],
                weight_i, weight_j, friction, bare, layers,
            )

            def put_residual(z, value):
                residual = pull - value
                field_ref[z] = residual
                residual_ref[2 * c + s, z] = residual[0:16]

            def put_image(z, value):
                next_ref[z] = value
                image_ref[2 * c + s, z] = value[0:16]

            def put_second(z, value):
                second_ref[z] = value

            apply(lambda z: mask * wide_ref[c, z], put_residual, *shared)
            apply(lambda z: field_ref[z], put_image, *shared)
            apply(lambda z: next_ref[z], put_second, *shared, kept=16)
            totals = products(
                lambda z: field_ref[z], lambda z: next_ref[z], lambda z: second_ref[z], layers,
                [jnp.zeros((8, 128), jnp.float32)] * 4,
            )
            for g in range(4):
                line = jnp.sum(jnp.where(inside, totals[g], 0.0), axis=0, keepdims=True)
                table_ref[...] += jnp.where(row8 == 2 * g + s, line, 0.0)
            return carry

        return lax.fori_loop(0, 2, component, carry)

    lax.fori_loop(0, 2, sample, 0)
    for c in range(2):
        for z in range(layers):
            start_ref[c, z] = mask[0:16] * u_ref[0, c, z] + mask[0:16] * u_ref[1, c, z]


def strip_part(
    row_place_ref, column_place_ref, strip_ref, by_odd_ref, by_even_ref, table_ref,
    residual_ref, image_ref, gram_ref,
    wide_ref, roots_ref, scale_ref, field_ref, next_ref, second_ref, *, total_x,
):
    layers = strip_ref.shape[0] - 1
    shape = (24, 128)
    lane = lanes(shape)
    used = lane < 4 * STRIP
    place = lane % STRIP
    number = lane // STRIP
    low = lane < 2 * STRIP

    geo = None
    odd = column_place_ref[0] % 2 == 1
    from_left = [jnp.where(odd, by_even_ref[g], by_odd_ref[g]) for g in range(2)]
    from_right = [jnp.where(odd, by_odd_ref[g], by_even_ref[g]) for g in range(2)]
    for layer in range(layers + 1):
        group, index = layer // GROUPED, layer % GROUPED
        strip = strip_ref[layer]
        strip = jnp.where(used & (place < 4), roll(from_left[group], -HALO * index, 1), strip)
        strip = jnp.where(used & (place >= 20), roll(from_right[group], 20 - HALO * index, 1), strip)
        if layer < layers:
            wide_ref[layer] = strip
        else:
            geo = strip

    def spread(to):
        result = jnp.zeros(shape, jnp.float32)
        for k in range(4):
            result = jnp.where(number == k, roll(geo, STRIP * (k - to), 1), result)
        return result

    mask = spread(0)
    bare = 1.0 - mask
    friction = mask * jnp.where(low, roll(geo, -2 * STRIP, 1), geo) + bare
    force_x, force_y = forces(mask, spread(1), row_place_ref[0] * 16, total_x)
    force = jnp.where(low, force_x, force_y)
    weight_i = jnp.where(low, MAIN_I[0], MAIN_I[1])
    weight_j = jnp.where(low, MAIN_J[0], MAIN_J[1])

    for z in range(layers):
        found = viscosity(
            lambda y: wide_ref[y], lambda y: roll(wide_ref[y], -2 * STRIP, 1), z, layers, mask
        )
        roots_ref[z] = jnp.where(low, found, roll(found, 2 * STRIP, 1))
    for z in range(layers):
        centre = with_neighbours(lambda y: roots_ref[y], z, layers)
        centre = centre + weight_i * around_i(centre)
        scale_ref[z] = centre + weight_j * around_j(centre)

    def put_residual(z, value):
        residual = force - value
        field_ref[z] = residual
        residual_ref[z] = residual[0:16]

    def put_image(z, value):
        next_ref[z] = value
        image_ref[z] = value[0:16]

    def put_second(z, value):
        second_ref[z] = value

    shared = (
        lambda z: roots_ref[z], lambda z: scale_ref[z], weight_i, weight_j, friction, bare, layers,
    )
    apply(lambda z: mask * wide_ref[z], put_residual, *shared)
    apply(lambda z: field_ref[z], put_image, *shared)
    apply(lambda z: next_ref[z], put_second, *shared, kept=16)
    totals = products(
        lambda z: field_ref[z], lambda z: next_ref[z], lambda z: second_ref[z], layers,
        [jnp.zeros((8, 128), jnp.float32)] * 4,
    )

    lane8 = lanes((8, 128))
    row8 = rows((8, 128))
    spot = lane8 % STRIP
    edge = (lane8 < 4 * STRIP) & (((spot >= 4) & (spot < 8)) | ((spot >= 16) & (spot < 20)))
    table = table_ref[...]
    for g in range(4):
        line = jnp.broadcast_to(jnp.sum(totals[g], axis=0, keepdims=True), (8, 128))
        for s in range(2):
            here = edge & ((lane8 // STRIP) % 2 == s) & (row8 == 2 * g + s)
            table = table + jnp.where(here, line, 0.0)
    table = jnp.sum(table, axis=1, keepdims=True)
    line = jnp.sum(jnp.where(lane8 == row8, table, 0.0), axis=0, keepdims=True)
    gram_ref[...] = jnp.broadcast_to(line, gram_ref.shape)


def combine(
    gram_ref, residual_ref, image_ref, start_ref, side_residual_ref, side_image_ref, out_ref
):
    layers = start_ref.shape[1]
    shape = (8, 128)
    lane = lanes(shape)
    total = jnp.broadcast_to(jnp.sum(gram_ref[...], axis=0, keepdims=True), shape)
    rr = total
    ra = roll(total, -2, 1)
    aa = roll(total, -4, 1)
    ab = roll(total, -6, 1)
    first = rr / ra
    norm_next = rr - 2.0 * first * ra + first * first * aa
    growth = 1.0 + norm_next / rr
    curve = growth * growth * ra - 2.0 * growth * first * aa + first * first * ab
    second = norm_next / curve
    residual_part = first + second * growth
    image_part = second * first
    ks = [jnp.broadcast_to(residual_part[:, s : s + 1], shape) for s in range(2)]
    ms = [jnp.broadcast_to(image_part[:, s : s + 1], shape) for s in range(2)]
    odd = (lane // STRIP) % 2 == 1
    k_side = jnp.where(odd, ks[1], ks[0])
    m_side = jnp.where(odd, ms[1], ms[0])
    for z in range(layers):
        for t in range(2):
            at = slice(8 * t, 8 * t + 8)
            side = k_side * side_residual_ref[z, at] - m_side * side_image_ref[z, at]
            side = side + roll(side, -STRIP, 1)
            for c in range(2):
                step = ks[0] * residual_ref[2 * c, z, at] - ms[0] * image_ref[2 * c, z, at]
                step = step + ks[1] * residual_ref[2 * c + 1, z, at]
                step = step - ms[1] * image_ref[2 * c + 1, z, at]
                base = 2 * STRIP * c
                step = jnp.where(lane < HALO, roll(side, -(base + 4), 1), step)
                step = jnp.where(lane >= 128 - HALO, roll(side, 124 - base - 16, 1), step)
                out_ref[c, z, at] = start_ref[c, z, at] + step


def f32(*shape):
    return pltpu.VMEM(shape, jnp.float32)


def call(kernel, outs, ins, name, scratch=(), in_specs=None):
    specs = in_specs or [VMEM] * len(ins)
    ins = [
        pltpu.with_memory_space_constraint(x, pltpu.VMEM) if spec is VMEM else x
        for x, spec in zip(ins, specs)
    ]
    return pl.pallas_call(
        kernel,
        in_specs=specs,
        out_specs=[VMEM] * len(outs),
        out_shape=list(outs),
        scratch_shapes=list(scratch),
        name=name,
    )(*ins)


def swap_sides(by_odd, by_even, axis):
    count = lax.axis_size(axis)

    def swap(message, first):
        pairs = [(i, i + 1) for i in range(first, count - 1, 2)]
        return lax.ppermute(message, axis, pairs + [(j, i) for i, j in pairs])

    return swap(by_odd, 1), swap(by_even, 0)


def copies_of_all(copies, axis):
    return lax.all_to_all(copies, axis, 0, 0, tiled=True)


def body(u_prior, friction_rows, friction_table, bed_fixed, ice_mask):
    members, parts, layers, rows_x, rows_y = u_prior.shape
    total_x = rows_x * lax.axis_size("plane")
    row_place = lax.axis_index("plane").reshape(1)
    column_place = lax.axis_index("planey").reshape(1)
    by_odd, by_even, geo, u_near = call(
        pack_rows,
        [
            f32(layers + 1, 2, 8, rows_y),
            f32(layers + 1, 2, 8, rows_y),
            f32(4, rows_x, rows_y),
            f32(*u_prior.shape),
        ],
        [row_place, friction_rows, u_prior, friction_table, bed_fixed, ice_mask],
        "pack_rows",
        scratch=[
            pltpu.SMEM(friction_rows.shape, jnp.int32),
            pltpu.VMEM(friction_table.shape, jnp.float32),
            pltpu.VMEM((2, rows_x, rows_y), jnp.int32),
            pltpu.SemaphoreType.DMA((5,)),
        ],
        in_specs=[SMEM] + [ANY] * 5,
    )
    by_odd, by_even = swap_sides(by_odd, by_even, "plane")
    outer, strip, side_odd, side_even = call(
        pack_columns,
        [f32(layers + 1, 4, 8, rows_y), f32(layers + 1, 24, 128), f32(2, 24, 128), f32(2, 24, 128)],
        [row_place, column_place, u_near, geo, by_odd, by_even],
        "pack_columns",
        in_specs=[SMEM, SMEM] + [VMEM] * 4,
    )
    side_odd, side_even = swap_sides(side_odd, side_even, "planey")
    residual, image, start, table = call(
        lambda *refs: main_part(*refs, total_x=total_x),
        [
            f32(4, layers, rows_x, 128),
            f32(4, layers, rows_x, 128),
            f32(2, layers, rows_x, 128),
            f32(8, 128),
        ],
        [row_place, u_near, geo, outer],
        "main_part",
        scratch=[
            pltpu.VMEM((2, layers, 24, 128), jnp.float32),
            pltpu.VMEM((layers, 24, 128), jnp.float32),
            pltpu.VMEM((2, layers, 24, 128), jnp.float32),
            pltpu.VMEM((layers, 24, 128), jnp.float32),
            pltpu.VMEM((layers, 24, 128), jnp.float32),
            pltpu.VMEM((layers, 16, 128), jnp.float32),
        ],
        in_specs=[SMEM] + [VMEM] * 3,
    )
    side_residual, side_image, gram = call(
        lambda *refs: strip_part(*refs, total_x=total_x),
        [
            f32(layers, rows_x, 128),
            f32(layers, rows_x, 128),
            f32(lax.axis_size("plane"), 128),
        ],
        [row_place, column_place, strip, side_odd, side_even, table],
        "strip_part",
        scratch=[pltpu.VMEM((layers, 24, 128), jnp.float32)] * 5
        + [pltpu.VMEM((layers, 16, 128), jnp.float32)],
        in_specs=[SMEM, SMEM] + [VMEM] * 4,
    )
    gathered = copies_of_all(gram, "plane")
    line = jnp.sum(gathered, axis=0, keepdims=True)
    gathered = copies_of_all(jnp.broadcast_to(line, (lax.axis_size("planey"), 128)), "planey")
    (local_sum,) = call(
        combine, [f32(2, layers, rows_x, 128)], [gathered, residual, image, start, side_residual, side_image],
        "combine",

    )
    summed = lax.all_gather(local_sum, "ens").sum(axis=0)
    return summed / (members * lax.axis_size("ens"))


def solution(mesh):
    in_specs = (
        P(("group", "ens"), None, None, "plane", "planey"),
        P(("group", "ens")),
        P("group", "plane", "planey"),
        P("plane", "planey"),
        P("plane", "planey"),
    )
    out_specs = P("group", None, "plane", "planey")
    return jax.shard_map(body, mesh=mesh, in_specs=in_specs, out_specs=out_specs, check_vma=False)
```

```python
import jax
import jax.numpy as jnp
from jax import lax
from jax.experimental import pallas as pl
from jax.experimental.pallas import tpu as pltpu
from jax.sharding import PartitionSpec as P


bed_unit = 2.0 ** (-29)
HALO = 4
STRIP = 24
GROUPED = STRIP // HALO
MAIN_I = (0.25, 0.125)
MAIN_J = (0.125, 0.25)


VMEM = pl.BlockSpec(memory_space=pltpu.VMEM)
SMEM = pl.BlockSpec(memory_space=pltpu.SMEM)
ANY = pl.BlockSpec(memory_space=pl.ANY)


def roll(x, shift, axis):
    return pltpu.roll(x, shift % x.shape[axis], axis)


def lanes(shape):
    return lax.broadcasted_iota(jnp.int32, shape, len(shape) - 1)


def rows(shape):
    return lax.broadcasted_iota(jnp.int32, shape, len(shape) - 2)


def pack_rows(
    place_ref, rows_hbm, u_hbm, table_hbm, bed_hbm, mask_hbm,
    odd_ref, even_ref, side_odd_ref, side_even_ref, geo_ref, u_ref, strip_ref,
    rows_ref, table_ref, ints_ref, sems,
):
    layers = u_ref.shape[2]
    moves = [
        (u_hbm, u_ref),
        (rows_hbm, rows_ref),
        (table_hbm, table_ref),
        (mask_hbm, ints_ref.at[0]),
        (bed_hbm, ints_ref.at[1]),
    ]
    copies = [pltpu.make_async_copy(*move, sems.at[i]) for i, move in enumerate(moves)]
    for copy in copies:
        copy.start()
    for copy in copies:
        copy.wait()
    geo_ref[0] = ints_ref[0].astype(jnp.float32)
    geo_ref[1] = ints_ref[1].astype(jnp.float32) * bed_unit
    for s in range(2):
        geo_ref[2 + s] = table_ref[rows_ref[s]]
    low = rows((8, 128)) < HALO
    lane = lanes((8, 128))
    zero = jnp.zeros((8, 128), jnp.float32)
    odd = place_ref[0] % 2 == 1

    def send(by_odd, by_even, at, top, end):
        up = jnp.where(low, roll(end[0], HALO, 0), end[1])
        down = jnp.where(low, top[0], roll(top[1], HALO, 0))
        by_odd[at] = jnp.where(odd, up, down)
        by_even[at] = jnp.where(odd, down, up)

    strips = []
    for layer in range(layers + 1):
        tiles = [
            u_ref[k % 2, k // 2, layer] if layer < layers else geo_ref[k] for k in range(4)
        ]
        halves = []
        for t in range(2):
            strip = zero
            for k in range(4):
                tile = tiles[k][8 * t : 8 * t + 8]
                at = lane - STRIP * k
                strip = jnp.where((at >= 4) & (at < 12), roll(tile, STRIP * k + 4, 1), strip)
                strip = jnp.where((at >= 12) & (at < 20), roll(tile, STRIP * k + 12 - 120, 1), strip)
            strip_ref[layer, 8 * t : 8 * t + 8] = strip
            halves.append(strip)
        strips.append(halves)
        for pair in range(2):
            both = tiles[2 * pair : 2 * pair + 2]
            send(
                odd_ref, even_ref, (layer, pair),
                [tile[0:8] for tile in both], [tile[8:16] for tile in both],
            )
    strips.append([zero, zero])
    for at in range(len(strips) // 2):
        both = strips[2 * at : 2 * at + 2]
        send(
            side_odd_ref, side_even_ref, at,
            [halves[0] for halves in both], [halves[1] for halves in both],
        )


def outer_rows(odd, by_odd, by_even):
    low = rows((8, 128)) < HALO
    below = jnp.where(odd, by_even, by_odd)
    above = jnp.where(odd, by_odd, by_even)
    return (
        jnp.where(low, above, roll(below, HALO, 0)),
        jnp.where(low, roll(above, HALO, 0), below),
    )


def pack_columns(
    row_place_ref, column_place_ref, own_ref, by_odd_ref, by_even_ref,
    strip_ref, odd_ref, even_ref,
):
    layers = own_ref.shape[0] - 1
    lane = lanes((8, 128))
    used = lane < 4 * STRIP
    slot = (lane % STRIP) // HALO
    odd = row_place_ref[0] % 2 == 1
    swapped = column_place_ref[0] % 2 == 1
    outer = []
    for at in range(by_odd_ref.shape[0]):
        outer.extend(outer_rows(odd, by_odd_ref[at], by_even_ref[at]))
    for t in range(3):
        place = slice(8 * t, 8 * t + 8)
        for group in range(2):
            right = jnp.zeros((8, 128), jnp.float32)
            left = right
            for index in range(min(GROUPED, layers + 1 - GROUPED * group)):
                layer = GROUPED * group + index
                strip = own_ref[layer, place] if t < 2 else outer[layer]
                strip_ref[layer, place] = strip
                here = used & (slot == index)
                right = jnp.where(here, roll(strip, HALO * index - 16, 1), right)
                left = jnp.where(here, roll(strip, HALO * index - 4, 1), left)
            odd_ref[group, place] = jnp.where(swapped, right, left)
            even_ref[group, place] = jnp.where(swapped, left, right)


def around_i(x):
    return roll(x, 1, 0) + roll(x, -1, 0)


def around_j(x):
    return roll(x, 1, 1) + roll(x, -1, 1)


def forces(cover, ground, row_start, total_x):
    row = rows(cover.shape)
    position = (jnp.where(row < 20, row, row - 24) + row_start).astype(jnp.float32)
    thickness = 1.0 + 2.0 * position / (total_x - 1)
    slope_x = (roll(ground, -1, 0) - roll(ground, 1, 0)) * 0.5
    slope_y = (roll(ground, -1, 1) - roll(ground, 1, 1)) * 0.5
    return -(cover * thickness * slope_x), -(cover * thickness * slope_y)


def difference(get, z, layers):
    if z == 0:
        return get(1)
    if z + 1 == layers:
        return -get(z - 1)
    return get(z + 1) - get(z - 1)


def viscosity(get_u, get_v, z, layers, cover):
    u, v = get_u(z), get_v(z)
    stretch_x = roll(u, -1, 0) - roll(u, 1, 0)
    stretch_y = roll(v, -1, 1) - roll(v, 1, 1)
    shear = (roll(u, -1, 1) - roll(u, 1, 1)) + (roll(v, -1, 0) - roll(v, 1, 0))
    rise_u = difference(get_u, z, layers)
    rise_v = difference(get_v, z, layers)
    strain = stretch_x * stretch_x + stretch_y * (stretch_y + stretch_x)
    strain = strain + 0.25 * (shear * shear + (rise_u * rise_u + rise_v * rise_v))
    return cover * jnp.exp(jnp.log(0.25 * strain + 0.1) * (-1.0 / 6.0))


def with_neighbours(get, z, layers):
    if z == 0:
        return get(0) + 0.5 * get(1)
    if z + 1 == layers:
        return get(z) + 0.5 * get(z - 1)
    return get(z) + 0.5 * (get(z - 1) + get(z + 1))


def apply(get, put, roots, scale, weight_i, weight_j, friction, empty, layers, kept=24):
    def kept_rows(x):
        return x[0:kept] if x.ndim else x

    def filtered(z):
        product = roots(z) * get(z)
        product = (product + weight_i * around_i(product))[0:kept]
        return product + kept_rows(weight_j) * around_j(product)

    done = {}
    for z in range(layers + 1):
        if z < layers:
            done[z] = filtered(z)
        if z > 0:
            at = z - 1
            total = with_neighbours(lambda y: done[y], at, layers)
            field = get(at)[0:kept]
            result = 4.0 * roots(at)[0:kept] * (scale(at)[0:kept] * field - total)
            put(at, result + (friction if at == 0 else empty)[0:kept] * field)


def products(field, image, second, layers, totals):
    totals = list(totals)
    for z in range(layers):
        for t in range(2):
            at = slice(8 * t, 8 * t + 8)
            r, a, b = field(z)[at], image(z)[at], second(z)[at]
            for i, (x, y) in enumerate(((r, r), (r, a), (a, a), (a, b))):
                totals[i] = totals[i] + x * y
    return totals


def main_part(
    row_place_ref, u_ref, geo_ref, by_odd_ref, by_even_ref,
    residual_ref, image_ref, start_ref, table_ref,
    geo_wide_ref, wide_ref, roots_ref, scale_ref, field_ref, next_ref, second_ref, *, total_x,
):
    layers = u_ref.shape[2]
    row_start = row_place_ref[0] * 16

    odd = row_place_ref[0] % 2 == 1
    for pair in range(2):
        outer = outer_rows(odd, by_odd_ref[layers, pair], by_even_ref[layers, pair])
        for i in range(2):
            geo_wide_ref[2 * pair + i, 0:16] = geo_ref[2 * pair + i]
            geo_wide_ref[2 * pair + i, 16:24] = outer[i]
    mask = geo_wide_ref[0]
    bare = 1.0 - mask
    force = forces(mask, geo_wide_ref[1], row_start, total_x)
    lane8 = lanes((8, 128))
    inside = (lane8 >= HALO) & (lane8 < 128 - HALO)
    row8 = rows((8, 128))
    table_ref[...] = jnp.zeros((8, 128), jnp.float32)

    def sample(s, carry):
        friction = mask * geo_wide_ref[2 + s] + bare
        for c in range(2):
            for z in range(layers):
                wide_ref[c, z, 0:16] = u_ref[s, c, z]
                outer = outer_rows(odd, by_odd_ref[z, c], by_even_ref[z, c])
                wide_ref[c, z, 16:24] = jnp.where(s == 0, outer[0], outer[1])
        for z in range(layers):
            roots_ref[z] = viscosity(
                lambda y: wide_ref[0, y], lambda y: wide_ref[1, y], z, layers, mask
            )
        for z in range(layers):
            centre = with_neighbours(lambda y: roots_ref[y], z, layers)
            along_i = around_i(centre)
            along_j = around_j(centre)
            both = centre + 0.03125 * around_j(along_i)
            for c in range(2):
                scale_ref[c, z] = both + MAIN_I[c] * along_i + MAIN_J[c] * along_j

        def component(c, carry):
            first = c == 0
            weight_i = jnp.where(first, MAIN_I[0], MAIN_I[1])
            weight_j = jnp.where(first, MAIN_J[0], MAIN_J[1])
            pull = jnp.where(first, force[0], force[1])
            shared = (
                lambda z: roots_ref[z], lambda z: scale_ref[c, z],
                weight_i, weight_j, friction, bare, layers,
            )

            def put_residual(z, value):
                residual = pull - value
                field_ref[z] = residual
                residual_ref[2 * c + s, z] = residual[0:16]

            def put_image(z, value):
                next_ref[z] = value
                image_ref[2 * c + s, z] = value[0:16]

            def put_second(z, value):
                second_ref[z] = value

            apply(lambda z: mask * wide_ref[c, z], put_residual, *shared)
            apply(lambda z: field_ref[z], put_image, *shared)
            apply(lambda z: next_ref[z], put_second, *shared, kept=16)
            totals = products(
                lambda z: field_ref[z], lambda z: next_ref[z], lambda z: second_ref[z], layers,
                [jnp.zeros((8, 128), jnp.float32)] * 4,
            )
            for g in range(4):
                line = jnp.sum(jnp.where(inside, totals[g], 0.0), axis=0, keepdims=True)
                table_ref[...] += jnp.where(row8 == 2 * g + s, line, 0.0)
            return carry

        return lax.fori_loop(0, 2, component, carry)

    lax.fori_loop(0, 2, sample, 0)
    for c in range(2):
        for z in range(layers):
            start_ref[c, z] = mask[0:16] * u_ref[0, c, z] + mask[0:16] * u_ref[1, c, z]


def strip_part(
    row_place_ref, column_place_ref, strip_ref, by_odd_ref, by_even_ref, table_ref,
    residual_ref, image_ref, gram_ref,
    wide_ref, roots_ref, scale_ref, field_ref, next_ref, second_ref, *, total_x,
):
    layers = strip_ref.shape[0] - 1
    shape = (24, 128)
    lane = lanes(shape)
    used = lane < 4 * STRIP
    place = lane % STRIP
    number = lane // STRIP
    low = lane < 2 * STRIP

    geo = None
    odd = column_place_ref[0] % 2 == 1
    from_left = [jnp.where(odd, by_even_ref[g], by_odd_ref[g]) for g in range(2)]
    from_right = [jnp.where(odd, by_odd_ref[g], by_even_ref[g]) for g in range(2)]
    for layer in range(layers + 1):
        group, index = layer // GROUPED, layer % GROUPED
        strip = strip_ref[layer]
        strip = jnp.where(used & (place < 4), roll(from_left[group], -HALO * index, 1), strip)
        strip = jnp.where(used & (place >= 20), roll(from_right[group], 20 - HALO * index, 1), strip)
        if layer < layers:
            wide_ref[layer] = strip
        else:
            geo = strip

    def spread(to):
        result = jnp.zeros(shape, jnp.float32)
        for k in range(4):
            result = jnp.where(number == k, roll(geo, STRIP * (k - to), 1), result)
        return result

    mask = spread(0)
    bare = 1.0 - mask
    friction = mask * jnp.where(low, roll(geo, -2 * STRIP, 1), geo) + bare
    force_x, force_y = forces(mask, spread(1), row_place_ref[0] * 16, total_x)
    force = jnp.where(low, force_x, force_y)
    weight_i = jnp.where(low, MAIN_I[0], MAIN_I[1])
    weight_j = jnp.where(low, MAIN_J[0], MAIN_J[1])

    for z in range(layers):
        found = viscosity(
            lambda y: wide_ref[y], lambda y: roll(wide_ref[y], -2 * STRIP, 1), z, layers, mask
        )
        roots_ref[z] = jnp.where(low, found, roll(found, 2 * STRIP, 1))
    for z in range(layers):
        centre = with_neighbours(lambda y: roots_ref[y], z, layers)
        centre = centre + weight_i * around_i(centre)
        scale_ref[z] = centre + weight_j * around_j(centre)

    def put_residual(z, value):
        residual = force - value
        field_ref[z] = residual
        residual_ref[z] = residual[0:16]

    def put_image(z, value):
        next_ref[z] = value
        image_ref[z] = value[0:16]

    def put_second(z, value):
        second_ref[z] = value

    shared = (
        lambda z: roots_ref[z], lambda z: scale_ref[z], weight_i, weight_j, friction, bare, layers,
    )
    apply(lambda z: mask * wide_ref[z], put_residual, *shared)
    apply(lambda z: field_ref[z], put_image, *shared)
    apply(lambda z: next_ref[z], put_second, *shared, kept=16)
    totals = products(
        lambda z: field_ref[z], lambda z: next_ref[z], lambda z: second_ref[z], layers,
        [jnp.zeros((8, 128), jnp.float32)] * 4,
    )

    lane8 = lanes((8, 128))
    row8 = rows((8, 128))
    spot = lane8 % STRIP
    edge = (lane8 < 4 * STRIP) & (((spot >= 4) & (spot < 8)) | ((spot >= 16) & (spot < 20)))
    table = table_ref[...]
    for g in range(4):
        line = jnp.broadcast_to(jnp.sum(totals[g], axis=0, keepdims=True), (8, 128))
        for s in range(2):
            here = edge & ((lane8 // STRIP) % 2 == s) & (row8 == 2 * g + s)
            table = table + jnp.where(here, line, 0.0)
    table = jnp.sum(table, axis=1, keepdims=True)
    line = jnp.sum(jnp.where(lane8 == row8, table, 0.0), axis=0, keepdims=True)
    gram_ref[...] = jnp.broadcast_to(line, gram_ref.shape)


def combine(
    gram_ref, residual_ref, image_ref, start_ref, side_residual_ref, side_image_ref, out_ref
):
    layers = start_ref.shape[1]
    shape = (8, 128)
    lane = lanes(shape)
    total = jnp.broadcast_to(jnp.sum(gram_ref[...], axis=0, keepdims=True), shape)
    rr = total
    ra = roll(total, -2, 1)
    aa = roll(total, -4, 1)
    ab = roll(total, -6, 1)
    first = rr / ra
    norm_next = rr - 2.0 * first * ra + first * first * aa
    growth = 1.0 + norm_next / rr
    curve = growth * growth * ra - 2.0 * growth * first * aa + first * first * ab
    second = norm_next / curve
    residual_part = first + second * growth
    image_part = second * first
    ks = [jnp.broadcast_to(residual_part[:, s : s + 1], shape) for s in range(2)]
    ms = [jnp.broadcast_to(image_part[:, s : s + 1], shape) for s in range(2)]
    odd = (lane // STRIP) % 2 == 1
    k_side = jnp.where(odd, ks[1], ks[0])
    m_side = jnp.where(odd, ms[1], ms[0])
    for z in range(layers):
        for t in range(2):
            at = slice(8 * t, 8 * t + 8)
            side = k_side * side_residual_ref[z, at] - m_side * side_image_ref[z, at]
            side = side + roll(side, -STRIP, 1)
            for c in range(2):
                step = ks[0] * residual_ref[2 * c, z, at] - ms[0] * image_ref[2 * c, z, at]
                step = step + ks[1] * residual_ref[2 * c + 1, z, at]
                step = step - ms[1] * image_ref[2 * c + 1, z, at]
                base = 2 * STRIP * c
                step = jnp.where(lane < HALO, roll(side, -(base + 4), 1), step)
                step = jnp.where(lane >= 128 - HALO, roll(side, 124 - base - 16, 1), step)
                out_ref[c, z, at] = start_ref[c, z, at] + step


def f32(*shape):
    return pltpu.VMEM(shape, jnp.float32)


def call(kernel, outs, ins, scratch=(), in_specs=None):
    specs = in_specs or [VMEM] * len(ins)
    ins = [
        pltpu.with_memory_space_constraint(x, pltpu.VMEM) if spec is VMEM else x
        for x, spec in zip(ins, specs)
    ]
    return pl.pallas_call(
        kernel,
        in_specs=specs,
        out_specs=[VMEM] * len(outs),
        out_shape=list(outs),
        scratch_shapes=list(scratch),
    )(*ins)


def swap_sides(by_odd, by_even, axis):
    count = lax.axis_size(axis)

    def swap(message, first):
        pairs = [(i, i + 1) for i in range(first, count - 1, 2)]
        return lax.ppermute(message, axis, pairs + [(j, i) for i, j in pairs])

    return swap(by_odd, 1), swap(by_even, 0)


def copies_of_all(copies, axis):
    return lax.all_to_all(copies, axis, 0, 0, tiled=True)


def body(u_prior, friction_rows, friction_table, bed_fixed, ice_mask):
    members, _, layers, rows_x, rows_y = u_prior.shape
    total_x = rows_x * lax.axis_size("plane")
    row_place = lax.axis_index("plane").reshape(1)
    column_place = lax.axis_index("planey").reshape(1)
    side_pairs = (layers + 2) // 2
    by_odd, by_even, side_odd, side_even, geo, u_near, own_strip = call(
        pack_rows,
        [
            f32(layers + 1, 2, 8, rows_y),
            f32(layers + 1, 2, 8, rows_y),
            f32(side_pairs, 8, rows_y),
            f32(side_pairs, 8, rows_y),
            f32(4, rows_x, rows_y),
            f32(*u_prior.shape),
            f32(layers + 1, rows_x, rows_y),
        ],
        [row_place, friction_rows, u_prior, friction_table, bed_fixed, ice_mask],
        scratch=[
            pltpu.SMEM(friction_rows.shape, jnp.int32),
            pltpu.VMEM(friction_table.shape, jnp.float32),
            pltpu.VMEM((2, rows_x, rows_y), jnp.int32),
            pltpu.SemaphoreType.DMA((5,)),
        ],
        in_specs=[SMEM] + [ANY] * 5,
    )
    side_odd, side_even = swap_sides(side_odd, side_even, "plane")
    by_odd, by_even = swap_sides(by_odd, by_even, "plane")
    strip, side_odd, side_even = call(
        pack_columns,
        [f32(layers + 1, 24, 128), f32(2, 24, 128), f32(2, 24, 128)],
        [row_place, column_place, own_strip, side_odd, side_even],
        in_specs=[SMEM, SMEM] + [VMEM] * 3,
    )
    side_odd, side_even = swap_sides(side_odd, side_even, "planey")
    residual, image, start, table = call(
        lambda *refs: main_part(*refs, total_x=total_x),
        [
            f32(4, layers, rows_x, 128),
            f32(4, layers, rows_x, 128),
            f32(2, layers, rows_x, 128),
            f32(8, 128),
        ],
        [row_place, u_near, geo, by_odd, by_even],
        scratch=[
            pltpu.VMEM((4, 24, 128), jnp.float32),
            pltpu.VMEM((2, layers, 24, 128), jnp.float32),
            pltpu.VMEM((layers, 24, 128), jnp.float32),
            pltpu.VMEM((2, layers, 24, 128), jnp.float32),
            pltpu.VMEM((layers, 24, 128), jnp.float32),
            pltpu.VMEM((layers, 24, 128), jnp.float32),
            pltpu.VMEM((layers, 16, 128), jnp.float32),
        ],
        in_specs=[SMEM] + [VMEM] * 4,
    )
    side_residual, side_image, gram = call(
        lambda *refs: strip_part(*refs, total_x=total_x),
        [
            f32(layers, rows_x, 128),
            f32(layers, rows_x, 128),
            f32(lax.axis_size("plane"), 128),
        ],
        [row_place, column_place, strip, side_odd, side_even, table],
        scratch=[pltpu.VMEM((layers, 24, 128), jnp.float32)] * 5
        + [pltpu.VMEM((layers, 16, 128), jnp.float32)],
        in_specs=[SMEM, SMEM] + [VMEM] * 4,
    )
    gathered = copies_of_all(gram, "plane")
    line = jnp.sum(gathered, axis=0, keepdims=True)
    gathered = copies_of_all(jnp.broadcast_to(line, (lax.axis_size("planey"), 128)), "planey")
    (local_sum,) = call(
        combine, [f32(2, layers, rows_x, 128)], [gathered, residual, image, start, side_residual, side_image],
    )
    summed = lax.all_gather(local_sum, "ens").sum(axis=0)
    return summed / (members * lax.axis_size("ens"))


def solution(mesh):
    in_specs = (
        P(("group", "ens"), None, None, "plane", "planey"),
        P(("group", "ens")),
        P("group", "plane", "planey"),
        P("plane", "planey"),
        P("plane", "planey"),
    )
    out_specs = P("group", None, "plane", "planey")

    return jax.shard_map(body, mesh=mesh, in_specs=in_specs, out_specs=out_specs, check_vma=False)
```

```python
import jax
import jax.numpy as jnp
from jax import lax
from jax.experimental import pallas as pl
from jax.experimental.pallas import tpu as pltpu
from jax.sharding import PartitionSpec as P

bed_unit = 2.0 ** (-29)
HALO = 4
STRIP = 24
GROUPED = STRIP // HALO
MAIN_I = (0.25, 0.125)
MAIN_J = (0.125, 0.25)


VMEM = pl.BlockSpec(memory_space=pltpu.VMEM)
SMEM = pl.BlockSpec(memory_space=pltpu.SMEM)
ANY = pl.BlockSpec(memory_space=pl.ANY)


def roll(x, shift, axis):
    return pltpu.roll(x, shift % x.shape[axis], axis)


def lanes(shape):
    return lax.broadcasted_iota(jnp.int32, shape, len(shape) - 1)


def rows(shape):
    return lax.broadcasted_iota(jnp.int32, shape, len(shape) - 2)


def pack_rows(
    place_ref, rows_hbm, u_hbm, table_hbm, bed_hbm, mask_hbm,
    odd_ref, even_ref, geo_ref, u_ref, rows_ref, table_ref, ints_ref, sems,
):
    layers = u_ref.shape[2]
    moves = [
        (u_hbm, u_ref),
        (rows_hbm, rows_ref),
        (table_hbm, table_ref),
        (mask_hbm, ints_ref.at[0]),
        (bed_hbm, ints_ref.at[1]),
    ]
    copies = [pltpu.make_async_copy(*move, sems.at[i]) for i, move in enumerate(moves)]
    for copy in copies:
        copy.start()
    for copy in copies:
        copy.wait()
    geo_ref[0] = ints_ref[0].astype(jnp.float32)
    geo_ref[1] = ints_ref[1].astype(jnp.float32) * bed_unit
    for s in range(2):
        geo_ref[2 + s] = table_ref[rows_ref[s]]
    low = rows((8, 128)) < HALO
    odd = place_ref[0] % 2 == 1
    for layer in range(layers + 1):
        for pair in range(2):
            tiles = [
                u_ref[s, pair, layer] if layer < layers else geo_ref[2 * pair + s] for s in range(2)
            ]
            top = [tile[0:8] for tile in tiles]
            end = [tile[8:16] for tile in tiles]
            up = jnp.where(low, roll(end[0], HALO, 0), end[1])
            down = jnp.where(low, top[0], roll(top[1], HALO, 0))
            odd_ref[layer, pair] = jnp.where(odd, up, down)
            even_ref[layer, pair] = jnp.where(odd, down, up)


def strip_tile(tiles):
    lane = lanes((8, 128))
    strip = jnp.zeros((8, 128), jnp.float32)
    for k, tile in enumerate(tiles):
        at = lane - STRIP * k
        strip = jnp.where((at >= 4) & (at < 12), roll(tile, STRIP * k + 4, 1), strip)
        strip = jnp.where((at >= 12) & (at < 20), roll(tile, STRIP * k + 12 - 120, 1), strip)
    return strip


def side_messages(strip_of, layers, swapped):
    lane = lanes((8, 128))
    used = lane < 4 * STRIP
    slot = (lane % STRIP) // HALO
    for group in range(2):
        right = jnp.zeros((8, 128), jnp.float32)
        left = right
        for index in range(min(GROUPED, layers + 1 - GROUPED * group)):
            strip = strip_of(GROUPED * group + index)
            here = used & (slot == index)
            right = jnp.where(here, roll(strip, HALO * index - 16, 1), right)
            left = jnp.where(here, roll(strip, HALO * index - 4, 1), left)
        yield group, jnp.where(swapped, right, left), jnp.where(swapped, left, right)


def pack_strips(column_place_ref, u_ref, geo_ref, own_ref, odd_ref, even_ref):
    layers = u_ref.shape[2]
    for layer in range(layers + 1):
        for t in range(2):
            at = slice(8 * t, 8 * t + 8)
            own_ref[layer, at] = strip_tile(
                [u_ref[k % 2, k // 2, layer, at] if layer < layers else geo_ref[k, at] for k in range(4)]
            )
    swapped = column_place_ref[0] % 2 == 1

    def send(t, carry):
        at = pl.ds(pl.multiple_of(8 * t, 8), 8)
        for group, by_odd, by_even in side_messages(lambda layer: own_ref[layer, at], layers, swapped):
            odd_ref[group, at] = by_odd
            even_ref[group, at] = by_even
        return carry

    lax.fori_loop(0, 2, send, 0)


def pack_columns(
    row_place_ref, column_place_ref, own_ref, own_odd_ref, own_even_ref, by_odd_ref, by_even_ref,
    outer_ref, strip_ref, odd_ref, even_ref,
):
    layers = own_ref.shape[0] - 1
    low = rows((8, 128)) < HALO
    odd = row_place_ref[0] % 2 == 1
    for layer in range(layers + 1):
        outer = []
        for pair in range(2):
            by_odd = by_odd_ref[layer, pair]
            by_even = by_even_ref[layer, pair]
            below = jnp.where(odd, by_even, by_odd)
            above = jnp.where(odd, by_odd, by_even)
            outer.append(jnp.where(low, above, roll(below, HALO, 0)))
            outer.append(jnp.where(low, roll(above, HALO, 0), below))
        for k in range(4):
            outer_ref[layer, k] = outer[k]
        strip_ref[layer, 0:16] = own_ref[layer]
        strip_ref[layer, 16:24] = strip_tile(outer)
    for group in range(2):
        odd_ref[group, 0:16] = own_odd_ref[group]
        even_ref[group, 0:16] = own_even_ref[group]
    swapped = column_place_ref[0] % 2 == 1

    for group, by_odd, by_even in side_messages(lambda layer: strip_ref[layer, 16:24], layers, swapped):
        odd_ref[group, 16:24] = by_odd
        even_ref[group, 16:24] = by_even


def around_i(x):
    return roll(x, 1, 0) + roll(x, -1, 0)


def around_j(x):
    return roll(x, 1, 1) + roll(x, -1, 1)


def forces(cover, ground, row_start, total_x):
    row = rows(cover.shape)
    position = (jnp.where(row < 20, row, row - 24) + row_start).astype(jnp.float32)
    thickness = 1.0 + 2.0 * position / (total_x - 1)
    slope_x = (roll(ground, -1, 0) - roll(ground, 1, 0)) * 0.5
    slope_y = (roll(ground, -1, 1) - roll(ground, 1, 1)) * 0.5
    return -(cover * thickness * slope_x), -(cover * thickness * slope_y)


def difference(get, z, layers):
    if z == 0:
        return get(1)
    if z + 1 == layers:
        return -get(z - 1)
    return get(z + 1) - get(z - 1)


def viscosity(get_u, get_v, z, layers, cover):
    u, v = get_u(z), get_v(z)
    stretch_x = roll(u, -1, 0) - roll(u, 1, 0)
    stretch_y = roll(v, -1, 1) - roll(v, 1, 1)
    shear = (roll(u, -1, 1) - roll(u, 1, 1)) + (roll(v, -1, 0) - roll(v, 1, 0))
    rise_u = difference(get_u, z, layers)
    rise_v = difference(get_v, z, layers)
    strain = stretch_x * stretch_x + stretch_y * (stretch_y + stretch_x)
    strain = strain + 0.25 * (shear * shear + (rise_u * rise_u + rise_v * rise_v))
    return cover * jnp.exp(jnp.log(0.25 * strain + 0.1) * (-1.0 / 6.0))


def with_neighbours(get, z, layers):
    if z == 0:
        return get(0) + 0.5 * get(1)
    if z + 1 == layers:
        return get(z) + 0.5 * get(z - 1)
    return get(z) + 0.5 * (get(z - 1) + get(z + 1))


def apply(get, put, roots, scale, weight_i, weight_j, friction, empty, layers, kept=24):
    def kept_rows(x):
        return x[0:kept] if x.ndim else x

    def filtered(z):
        product = roots(z) * get(z)
        product = (product + weight_i * around_i(product))[0:kept]
        return product + kept_rows(weight_j) * around_j(product)

    done = {}
    for z in range(layers + 1):
        if z < layers:
            done[z] = filtered(z)
        if z > 0:
            at = z - 1
            total = with_neighbours(lambda y: done[y], at, layers)
            field = get(at)[0:kept]
            result = 4.0 * roots(at)[0:kept] * (scale(at)[0:kept] * field - total)
            put(at, result + (friction if at == 0 else empty)[0:kept] * field)


def products(field, image, second, layers, totals):
    totals = list(totals)
    for z in range(layers):
        for t in range(2):
            at = slice(8 * t, 8 * t + 8)
            r, a, b = field(z)[at], image(z)[at], second(z)[at]
            for i, (x, y) in enumerate(((r, r), (r, a), (a, a), (a, b))):
                totals[i] = totals[i] + x * y
    return totals


def main_part(
    row_place_ref, u_ref, geo_ref, outer_ref,
    residual_ref, image_ref, start_ref, table_ref,
    wide_ref, roots_ref, scale_ref, field_ref, next_ref, second_ref, *, total_x,
):
    layers = u_ref.shape[2]
    row_start = row_place_ref[0] * 16

    def geo(k):
        return jnp.concatenate([geo_ref[k], outer_ref[layers, k]], axis=0)

    mask = geo(0)
    bare = 1.0 - mask
    force = forces(mask, geo(1), row_start, total_x)
    lane8 = lanes((8, 128))
    inside = (lane8 >= HALO) & (lane8 < 128 - HALO)
    row8 = rows((8, 128))
    table_ref[...] = jnp.zeros((8, 128), jnp.float32)

    def sample(s, carry):
        friction = mask * jnp.concatenate([geo_ref[2 + s], outer_ref[layers, 2 + s]], axis=0) + bare
        for c in range(2):
            for z in range(layers):
                wide_ref[c, z, 0:16] = u_ref[s, c, z]
                wide_ref[c, z, 16:24] = outer_ref[z, 2 * c + s]
        for z in range(layers):
            roots_ref[z] = viscosity(
                lambda y: wide_ref[0, y], lambda y: wide_ref[1, y], z, layers, mask
            )
        for z in range(layers):
            centre = with_neighbours(lambda y: roots_ref[y], z, layers)
            along_i = around_i(centre)
            along_j = around_j(centre)
            both = centre + 0.03125 * around_j(along_i)
            for c in range(2):
                scale_ref[c, z] = both + MAIN_I[c] * along_i + MAIN_J[c] * along_j

        def component(c, carry):
            first = c == 0
            weight_i = jnp.where(first, MAIN_I[0], MAIN_I[1])
            weight_j = jnp.where(first, MAIN_J[0], MAIN_J[1])
            pull = jnp.where(first, force[0], force[1])
            shared = (
                lambda z: roots_ref[z], lambda z: scale_ref[c, z],
                weight_i, weight_j, friction, bare, layers,
            )

            def put_residual(z, value):
                residual = pull - value
                field_ref[z] = residual
                residual_ref[2 * c + s, z] = residual[0:16]

            def put_image(z, value):
                next_ref[z] = value
                image_ref[2 * c + s, z] = value[0:16]

            def put_second(z, value):
                second_ref[z] = value

            apply(lambda z: mask * wide_ref[c, z], put_residual, *shared)
            apply(lambda z: field_ref[z], put_image, *shared)
            apply(lambda z: next_ref[z], put_second, *shared, kept=16)
            totals = products(
                lambda z: field_ref[z], lambda z: next_ref[z], lambda z: second_ref[z], layers,
                [jnp.zeros((8, 128), jnp.float32)] * 4,
            )
            for g in range(4):
                line = jnp.sum(jnp.where(inside, totals[g], 0.0), axis=0, keepdims=True)
                table_ref[...] += jnp.where(row8 == 2 * g + s, line, 0.0)
            return carry

        return lax.fori_loop(0, 2, component, carry)

    lax.fori_loop(0, 2, sample, 0)
    for c in range(2):
        for z in range(layers):
            start_ref[c, z] = mask[0:16] * u_ref[0, c, z] + mask[0:16] * u_ref[1, c, z]


def strip_part(
    row_place_ref, column_place_ref, strip_ref, by_odd_ref, by_even_ref, table_ref,
    residual_ref, image_ref, gram_ref,
    wide_ref, roots_ref, scale_ref, field_ref, next_ref, second_ref, *, total_x,
):
    layers = strip_ref.shape[0] - 1
    shape = (24, 128)
    lane = lanes(shape)
    used = lane < 4 * STRIP
    place = lane % STRIP
    number = lane // STRIP
    low = lane < 2 * STRIP

    geo = None
    odd = column_place_ref[0] % 2 == 1
    from_left = [jnp.where(odd, by_even_ref[g], by_odd_ref[g]) for g in range(2)]
    from_right = [jnp.where(odd, by_odd_ref[g], by_even_ref[g]) for g in range(2)]
    for layer in range(layers + 1):
        group, index = layer // GROUPED, layer % GROUPED
        strip = strip_ref[layer]
        strip = jnp.where(used & (place < 4), roll(from_left[group], -HALO * index, 1), strip)
        strip = jnp.where(used & (place >= 20), roll(from_right[group], 20 - HALO * index, 1), strip)
        if layer < layers:
            wide_ref[layer] = strip
        else:
            geo = strip

    def spread(to):
        result = jnp.zeros(shape, jnp.float32)
        for k in range(4):
            result = jnp.where(number == k, roll(geo, STRIP * (k - to), 1), result)
        return result

    mask = spread(0)
    bare = 1.0 - mask
    friction = mask * jnp.where(low, roll(geo, -2 * STRIP, 1), geo) + bare
    force_x, force_y = forces(mask, spread(1), row_place_ref[0] * 16, total_x)
    force = jnp.where(low, force_x, force_y)
    weight_i = jnp.where(low, MAIN_I[0], MAIN_I[1])
    weight_j = jnp.where(low, MAIN_J[0], MAIN_J[1])

    for z in range(layers):
        found = viscosity(
            lambda y: wide_ref[y], lambda y: roll(wide_ref[y], -2 * STRIP, 1), z, layers, mask
        )
        roots_ref[z] = jnp.where(low, found, roll(found, 2 * STRIP, 1))
    for z in range(layers):
        centre = with_neighbours(lambda y: roots_ref[y], z, layers)
        centre = centre + weight_i * around_i(centre)
        scale_ref[z] = centre + weight_j * around_j(centre)

    def put_residual(z, value):
        residual = force - value
        field_ref[z] = residual
        residual_ref[z] = residual[0:16]

    def put_image(z, value):
        next_ref[z] = value
        image_ref[z] = value[0:16]

    def put_second(z, value):
        second_ref[z] = value

    shared = (
        lambda z: roots_ref[z], lambda z: scale_ref[z], weight_i, weight_j, friction, bare, layers,
    )
    apply(lambda z: mask * wide_ref[z], put_residual, *shared)
    apply(lambda z: field_ref[z], put_image, *shared)
    apply(lambda z: next_ref[z], put_second, *shared, kept=16)
    totals = products(
        lambda z: field_ref[z], lambda z: next_ref[z], lambda z: second_ref[z], layers,
        [jnp.zeros((8, 128), jnp.float32)] * 4,
    )

    lane8 = lanes((8, 128))
    row8 = rows((8, 128))
    spot = lane8 % STRIP
    edge = (lane8 < 4 * STRIP) & (((spot >= 4) & (spot < 8)) | ((spot >= 16) & (spot < 20)))
    table = table_ref[...]
    for g in range(4):
        line = jnp.broadcast_to(jnp.sum(totals[g], axis=0, keepdims=True), (8, 128))
        for s in range(2):
            here = edge & ((lane8 // STRIP) % 2 == s) & (row8 == 2 * g + s)
            table = table + jnp.where(here, line, 0.0)
    table = jnp.sum(table, axis=1, keepdims=True)
    line = jnp.sum(jnp.where(lane8 == row8, table, 0.0), axis=0, keepdims=True)
    gram_ref[...] = jnp.broadcast_to(line, gram_ref.shape)


def combine(
    gram_ref, residual_ref, image_ref, start_ref, side_residual_ref, side_image_ref, out_ref
):
    layers = start_ref.shape[1]
    shape = (8, 128)
    lane = lanes(shape)
    total = jnp.broadcast_to(jnp.sum(gram_ref[...], axis=0, keepdims=True), shape)
    rr = total
    ra = roll(total, -2, 1)
    aa = roll(total, -4, 1)
    ab = roll(total, -6, 1)
    first = rr / ra
    norm_next = rr - 2.0 * first * ra + first * first * aa
    growth = 1.0 + norm_next / rr
    curve = growth * growth * ra - 2.0 * growth * first * aa + first * first * ab
    second = norm_next / curve
    residual_part = first + second * growth
    image_part = second * first
    ks = [jnp.broadcast_to(residual_part[:, s : s + 1], shape) for s in range(2)]
    ms = [jnp.broadcast_to(image_part[:, s : s + 1], shape) for s in range(2)]
    odd = (lane // STRIP) % 2 == 1
    k_side = jnp.where(odd, ks[1], ks[0])
    m_side = jnp.where(odd, ms[1], ms[0])
    for z in range(layers):
        for t in range(2):
            at = slice(8 * t, 8 * t + 8)
            side = k_side * side_residual_ref[z, at] - m_side * side_image_ref[z, at]
            side = side + roll(side, -STRIP, 1)
            for c in range(2):
                step = ks[0] * residual_ref[2 * c, z, at] - ms[0] * image_ref[2 * c, z, at]
                step = step + ks[1] * residual_ref[2 * c + 1, z, at]
                step = step - ms[1] * image_ref[2 * c + 1, z, at]
                base = 2 * STRIP * c
                step = jnp.where(lane < HALO, roll(side, -(base + 4), 1), step)
                step = jnp.where(lane >= 128 - HALO, roll(side, 124 - base - 16, 1), step)
                out_ref[c, z, at] = start_ref[c, z, at] + step


def f32(*shape):
    return pltpu.VMEM(shape, jnp.float32)


def call(kernel, outs, ins, name, scratch=(), in_specs=None):
    specs = in_specs or [VMEM] * len(ins)
    ins = [
        pltpu.with_memory_space_constraint(x, pltpu.VMEM) if spec is VMEM else x
        for x, spec in zip(ins, specs)
    ]
    return pl.pallas_call(
        kernel,
        in_specs=specs,
        out_specs=[VMEM] * len(outs),
        out_shape=list(outs),
        scratch_shapes=list(scratch),
        name=name,
    )(*ins)


def swap_sides(by_odd, by_even, axis):
    count = lax.axis_size(axis)

    def swap(message, first):
        pairs = [(i, i + 1) for i in range(first, count - 1, 2)]
        return lax.ppermute(message, axis, pairs + [(j, i) for i, j in pairs])

    return swap(by_odd, 1), swap(by_even, 0)


def body(u_prior, friction_rows, friction_table, bed_fixed, ice_mask):
    members, parts, layers, rows_x, rows_y = u_prior.shape
    total_x = rows_x * lax.axis_size("plane")
    row_place = lax.axis_index("plane").reshape(1)
    column_place = lax.axis_index("planey").reshape(1)
    by_odd, by_even, geo, u_near = call(
        pack_rows,
        [
            f32(layers + 1, 2, 8, rows_y),
            f32(layers + 1, 2, 8, rows_y),
            f32(4, rows_x, rows_y),
            f32(*u_prior.shape),
        ],
        [row_place, friction_rows, u_prior, friction_table, bed_fixed, ice_mask],
        "pack_rows",
        scratch=[
            pltpu.SMEM(friction_rows.shape, jnp.int32),
            pltpu.VMEM(friction_table.shape, jnp.float32),
            pltpu.VMEM((2, rows_x, rows_y), jnp.int32),
            pltpu.SemaphoreType.DMA((5,)),
        ],
        in_specs=[SMEM] + [ANY] * 5,
    )
    by_odd, by_even = swap_sides(by_odd, by_even, "plane")
    own = call(
        pack_strips,
        [f32(layers + 1, rows_x, 128), f32(2, rows_x, 128), f32(2, rows_x, 128)],
        [column_place, u_near, geo],
        "pack_strips",
        in_specs=[SMEM, VMEM, VMEM],
    )
    outer, strip, side_odd, side_even = call(
        pack_columns,
        [f32(layers + 1, 4, 8, rows_y), f32(layers + 1, 24, 128), f32(2, 24, 128), f32(2, 24, 128)],
        [row_place, column_place, *own, by_odd, by_even],
        "pack_columns",
        in_specs=[SMEM, SMEM] + [VMEM] * 5,
    )
    side_odd, side_even = swap_sides(side_odd, side_even, "planey")
    residual, image, start, table = call(
        lambda *refs: main_part(*refs, total_x=total_x),
        [
            f32(4, layers, rows_x, 128),
            f32(4, layers, rows_x, 128),
            f32(2, layers, rows_x, 128),
            f32(8, 128),
        ],
        [row_place, u_near, geo, outer],
        "main_part",
        scratch=[
            pltpu.VMEM((2, layers, 24, 128), jnp.float32),
            pltpu.VMEM((layers, 24, 128), jnp.float32),
            pltpu.VMEM((2, layers, 24, 128), jnp.float32),
            pltpu.VMEM((layers, 24, 128), jnp.float32),
            pltpu.VMEM((layers, 24, 128), jnp.float32),
            pltpu.VMEM((layers, 16, 128), jnp.float32),
        ],
        in_specs=[SMEM] + [VMEM] * 3,
    )
    side_residual, side_image, gram = call(
        lambda *refs: strip_part(*refs, total_x=total_x),
        [
            f32(layers, rows_x, 128),
            f32(layers, rows_x, 128),
            f32(lax.axis_size("plane") * lax.axis_size("planey"), 128),
        ],
        [row_place, column_place, strip, side_odd, side_even, table],
        "strip_part",
        scratch=[pltpu.VMEM((layers, 24, 128), jnp.float32)] * 5
        + [pltpu.VMEM((layers, 16, 128), jnp.float32)],
        in_specs=[SMEM, SMEM] + [VMEM] * 4,
    )
    gathered = lax.all_to_all(gram, ("plane", "planey"), 0, 0, tiled=True)
    (local_sum,) = call(
        combine, [f32(2, layers, rows_x, 128)], [gathered, residual, image, start, side_residual, side_image],
        "combine",

    )
    summed = lax.all_gather(local_sum, "ens").sum(axis=0)
    return summed / (members * lax.axis_size("ens"))


def solution(mesh):
    in_specs = (
        P(("group", "ens"), None, None, "plane", "planey"),
        P(("group", "ens")),
        P("group", "plane", "planey"),
        P("plane", "planey"),
        P("plane", "planey"),
    )
    out_specs = P("group", None, "plane", "planey")
    return jax.shard_map(body, mesh=mesh, in_specs=in_specs, out_specs=out_specs, check_vma=False)
```

```python
import jax
import jax.numpy as jnp
from jax import lax
from jax.experimental import pallas as pl
from jax.experimental.pallas import tpu as pltpu
from jax.sharding import PartitionSpec as P

bed_unit = 2.0 ** (-29)
HALO = 4
STRIP = 24
GROUPED = STRIP // HALO
MAIN_I = (0.25, 0.125)
MAIN_J = (0.125, 0.25)


VMEM = pl.BlockSpec(memory_space=pltpu.VMEM)
SMEM = pl.BlockSpec(memory_space=pltpu.SMEM)
ANY = pl.BlockSpec(memory_space=pl.ANY)


def roll(x, shift, axis):
    return pltpu.roll(x, shift % x.shape[axis], axis)


def lanes(shape):
    return lax.broadcasted_iota(jnp.int32, shape, len(shape) - 1)


def rows(shape):
    return lax.broadcasted_iota(jnp.int32, shape, len(shape) - 2)


def pack_rows(
    row_turn_ref, rows_hbm, u_hbm, table_hbm, bed_hbm, mask_hbm,
    odd_ref, even_ref, geo_ref, u_ref, rows_ref, table_ref, ints_ref, sems,
):
    layers = u_ref.shape[2]
    moves = [
        (u_hbm, u_ref),
        (rows_hbm, rows_ref),
        (table_hbm, table_ref),
        (mask_hbm, ints_ref.at[0]),
        (bed_hbm, ints_ref.at[1]),
    ]
    copies = [pltpu.make_async_copy(*move, sems.at[i]) for i, move in enumerate(moves)]
    for copy in copies:
        copy.start()
    for copy in copies:
        copy.wait()
    geo_ref[0] = ints_ref[0].astype(jnp.float32)
    geo_ref[1] = ints_ref[1].astype(jnp.float32) * bed_unit
    for s in range(2):
        geo_ref[2 + s] = table_ref[rows_ref[s]]
    low = rows((8, 128)) < HALO
    odd = row_turn_ref[0] % 2 == 1
    for layer in range(layers + 1):
        for pair in range(2):
            tiles = [
                u_ref[s, pair, layer] if layer < layers else geo_ref[2 * pair + s] for s in range(2)
            ]
            top = [tile[0:8] for tile in tiles]
            end = [tile[8:16] for tile in tiles]
            up = jnp.where(low, roll(end[0], HALO, 0), end[1])
            down = jnp.where(low, top[0], roll(top[1], HALO, 0))
            odd_ref[layer, pair] = jnp.where(odd, up, down)
            even_ref[layer, pair] = jnp.where(odd, down, up)


def strip_tile(tiles):
    lane = lanes((8, 128))
    strip = jnp.zeros((8, 128), jnp.float32)
    for k, tile in enumerate(tiles):
        at = lane - STRIP * k
        strip = jnp.where((at >= 4) & (at < 12), roll(tile, STRIP * k + 4, 1), strip)
        strip = jnp.where((at >= 12) & (at < 20), roll(tile, STRIP * k + 12 - 120, 1), strip)
    return strip


def side_messages(strip_of, layers, swapped):
    lane = lanes((8, 128))
    used = lane < 4 * STRIP
    slot = (lane % STRIP) // HALO
    for group in range(2):
        right = jnp.zeros((8, 128), jnp.float32)
        left = right
        for index in range(min(GROUPED, layers + 1 - GROUPED * group)):
            strip = strip_of(GROUPED * group + index)
            here = used & (slot == index)
            right = jnp.where(here, roll(strip, HALO * index - 16, 1), right)
            left = jnp.where(here, roll(strip, HALO * index - 4, 1), left)
        yield group, jnp.where(swapped, right, left), jnp.where(swapped, left, right)


def pack_strips(column_place_ref, u_ref, geo_ref, own_ref, odd_ref, even_ref):
    layers = u_ref.shape[2]
    for layer in range(layers + 1):
        for t in range(2):
            at = slice(8 * t, 8 * t + 8)
            own_ref[layer, at] = strip_tile(
                [u_ref[k % 2, k // 2, layer, at] if layer < layers else geo_ref[k, at] for k in range(4)]
            )
    swapped = column_place_ref[0] % 2 == 1

    def send(t, carry):
        at = pl.ds(pl.multiple_of(8 * t, 8), 8)
        for group, by_odd, by_even in side_messages(lambda layer: own_ref[layer, at], layers, swapped):
            odd_ref[group, at] = by_odd
            even_ref[group, at] = by_even
        return carry

    lax.fori_loop(0, 2, send, 0)


def pack_columns(
    row_turn_ref, column_place_ref, own_ref, own_odd_ref, own_even_ref, by_odd_ref, by_even_ref,
    outer_ref, strip_ref, odd_ref, even_ref,
):
    layers = own_ref.shape[0] - 1
    low = rows((8, 128)) < HALO
    odd = row_turn_ref[0] % 2 == 1
    for layer in range(layers + 1):
        outer = []
        for pair in range(2):
            by_odd = by_odd_ref[layer, pair]
            by_even = by_even_ref[layer, pair]
            below = jnp.where(odd, by_even, by_odd)
            above = jnp.where(odd, by_odd, by_even)
            outer.append(jnp.where(low, above, roll(below, HALO, 0)))
            outer.append(jnp.where(low, roll(above, HALO, 0), below))
        for k in range(4):
            outer_ref[layer, k] = outer[k]
        strip_ref[layer, 0:16] = own_ref[layer]
        strip_ref[layer, 16:24] = strip_tile(outer)
    for group in range(2):
        odd_ref[group, 0:16] = own_odd_ref[group]
        even_ref[group, 0:16] = own_even_ref[group]
    swapped = column_place_ref[0] % 2 == 1

    for group, by_odd, by_even in side_messages(lambda layer: strip_ref[layer, 16:24], layers, swapped):
        odd_ref[group, 16:24] = by_odd
        even_ref[group, 16:24] = by_even


def around_i(x):
    return roll(x, 1, 0) + roll(x, -1, 0)


def around_j(x):
    return roll(x, 1, 1) + roll(x, -1, 1)


def forces(cover, ground, row_start, total_x):
    row = rows(cover.shape)
    position = (jnp.where(row < 20, row, row - 24) + row_start).astype(jnp.float32)
    thickness = 1.0 + 2.0 * position / (total_x - 1)
    slope_x = (roll(ground, -1, 0) - roll(ground, 1, 0)) * 0.5
    slope_y = (roll(ground, -1, 1) - roll(ground, 1, 1)) * 0.5
    return -(cover * thickness * slope_x), -(cover * thickness * slope_y)


def difference(get, z, layers):
    if z == 0:
        return get(1)
    if z + 1 == layers:
        return -get(z - 1)
    return get(z + 1) - get(z - 1)


def viscosity(get_u, get_v, z, layers, cover):
    u, v = get_u(z), get_v(z)
    stretch_x = roll(u, -1, 0) - roll(u, 1, 0)
    stretch_y = roll(v, -1, 1) - roll(v, 1, 1)
    shear = (roll(u, -1, 1) - roll(u, 1, 1)) + (roll(v, -1, 0) - roll(v, 1, 0))
    rise_u = difference(get_u, z, layers)
    rise_v = difference(get_v, z, layers)
    strain = stretch_x * stretch_x + stretch_y * (stretch_y + stretch_x)
    strain = strain + 0.25 * (shear * shear + (rise_u * rise_u + rise_v * rise_v))
    return cover * jnp.exp(jnp.log(0.25 * strain + 0.1) * (-1.0 / 6.0))


def with_neighbours(get, z, layers):
    if z == 0:
        return get(0) + 0.5 * get(1)
    if z + 1 == layers:
        return get(z) + 0.5 * get(z - 1)
    return get(z) + 0.5 * (get(z - 1) + get(z + 1))


def apply(get, put, roots, scale, weight_i, weight_j, friction, empty, layers, kept=24):
    def kept_rows(x):
        return x[0:kept] if x.ndim else x

    def filtered(z):
        product = roots(z) * get(z)
        product = (product + weight_i * around_i(product))[0:kept]
        return product + kept_rows(weight_j) * around_j(product)

    done = {}
    for z in range(layers + 1):
        if z < layers:
            done[z] = filtered(z)
        if z > 0:
            at = z - 1
            total = with_neighbours(lambda y: done[y], at, layers)
            field = get(at)[0:kept]
            result = 4.0 * roots(at)[0:kept] * (scale(at)[0:kept] * field - total)
            put(at, result + (friction if at == 0 else empty)[0:kept] * field)


def products(field, image, second, layers, totals):
    totals = list(totals)
    for z in range(layers):
        for t in range(2):
            at = slice(8 * t, 8 * t + 8)
            r, a, b = field(z)[at], image(z)[at], second(z)[at]
            for i, (x, y) in enumerate(((r, r), (r, a), (a, a), (a, b))):
                totals[i] = totals[i] + x * y
    return totals


def main_part(
    row_place_ref, u_ref, geo_ref, outer_ref,
    residual_ref, image_ref, start_ref, table_ref,
    wide_ref, roots_ref, scale_ref, field_ref, next_ref, second_ref, *, total_x,
):
    layers = u_ref.shape[2]
    row_start = row_place_ref[0] * 16

    def geo(k):
        return jnp.concatenate([geo_ref[k], outer_ref[layers, k]], axis=0)

    mask = geo(0)
    bare = 1.0 - mask
    force = forces(mask, geo(1), row_start, total_x)
    lane8 = lanes((8, 128))
    inside = (lane8 >= HALO) & (lane8 < 128 - HALO)
    row8 = rows((8, 128))
    table_ref[...] = jnp.zeros((8, 128), jnp.float32)

    def sample(s, carry):
        friction = mask * jnp.concatenate([geo_ref[2 + s], outer_ref[layers, 2 + s]], axis=0) + bare
        for c in range(2):
            for z in range(layers):
                wide_ref[c, z, 0:16] = u_ref[s, c, z]
                wide_ref[c, z, 16:24] = outer_ref[z, 2 * c + s]
        for z in range(layers):
            roots_ref[z] = viscosity(
                lambda y: wide_ref[0, y], lambda y: wide_ref[1, y], z, layers, mask
            )
        for z in range(layers):
            centre = with_neighbours(lambda y: roots_ref[y], z, layers)
            along_i = around_i(centre)
            along_j = around_j(centre)
            both = centre + 0.03125 * around_j(along_i)
            for c in range(2):
                scale_ref[c, z] = both + MAIN_I[c] * along_i + MAIN_J[c] * along_j

        def component(c, carry):
            first = c == 0
            weight_i = jnp.where(first, MAIN_I[0], MAIN_I[1])
            weight_j = jnp.where(first, MAIN_J[0], MAIN_J[1])
            pull = jnp.where(first, force[0], force[1])
            shared = (
                lambda z: roots_ref[z], lambda z: scale_ref[c, z],
                weight_i, weight_j, friction, bare, layers,
            )

            def put_residual(z, value):
                residual = pull - value
                field_ref[z] = residual
                residual_ref[2 * c + s, z] = residual[0:16]

            def put_image(z, value):
                next_ref[z] = value
                image_ref[2 * c + s, z] = value[0:16]

            def put_second(z, value):
                second_ref[z] = value

            apply(lambda z: mask * wide_ref[c, z], put_residual, *shared)
            apply(lambda z: field_ref[z], put_image, *shared)
            apply(lambda z: next_ref[z], put_second, *shared, kept=16)
            totals = products(
                lambda z: field_ref[z], lambda z: next_ref[z], lambda z: second_ref[z], layers,
                [jnp.zeros((8, 128), jnp.float32)] * 4,
            )
            for g in range(4):
                line = jnp.sum(jnp.where(inside, totals[g], 0.0), axis=0, keepdims=True)
                table_ref[...] += jnp.where(row8 == 2 * g + s, line, 0.0)
            return carry

        return lax.fori_loop(0, 2, component, carry)

    lax.fori_loop(0, 2, sample, 0)
    for c in range(2):
        for z in range(layers):
            start_ref[c, z] = mask[0:16] * u_ref[0, c, z] + mask[0:16] * u_ref[1, c, z]


def strip_part(
    row_place_ref, column_place_ref, strip_ref, by_odd_ref, by_even_ref, table_ref,
    residual_ref, image_ref, gram_ref,
    wide_ref, roots_ref, scale_ref, field_ref, next_ref, second_ref, *, total_x,
):
    layers = strip_ref.shape[0] - 1
    shape = (24, 128)
    lane = lanes(shape)
    used = lane < 4 * STRIP
    place = lane % STRIP
    number = lane // STRIP
    low = lane < 2 * STRIP

    geo = None
    odd = column_place_ref[0] % 2 == 1
    from_left = [jnp.where(odd, by_even_ref[g], by_odd_ref[g]) for g in range(2)]
    from_right = [jnp.where(odd, by_odd_ref[g], by_even_ref[g]) for g in range(2)]
    for layer in range(layers + 1):
        group, index = layer // GROUPED, layer % GROUPED
        strip = strip_ref[layer]
        strip = jnp.where(used & (place < 4), roll(from_left[group], -HALO * index, 1), strip)
        strip = jnp.where(used & (place >= 20), roll(from_right[group], 20 - HALO * index, 1), strip)
        if layer < layers:
            wide_ref[layer] = strip
        else:
            geo = strip

    def spread(to):
        result = jnp.zeros(shape, jnp.float32)
        for k in range(4):
            result = jnp.where(number == k, roll(geo, STRIP * (k - to), 1), result)
        return result

    mask = spread(0)
    bare = 1.0 - mask
    friction = mask * jnp.where(low, roll(geo, -2 * STRIP, 1), geo) + bare
    force_x, force_y = forces(mask, spread(1), row_place_ref[0] * 16, total_x)
    force = jnp.where(low, force_x, force_y)
    weight_i = jnp.where(low, MAIN_I[0], MAIN_I[1])
    weight_j = jnp.where(low, MAIN_J[0], MAIN_J[1])

    for z in range(layers):
        found = viscosity(
            lambda y: wide_ref[y], lambda y: roll(wide_ref[y], -2 * STRIP, 1), z, layers, mask
        )
        roots_ref[z] = jnp.where(low, found, roll(found, 2 * STRIP, 1))
    for z in range(layers):
        centre = with_neighbours(lambda y: roots_ref[y], z, layers)
        centre = centre + weight_i * around_i(centre)
        scale_ref[z] = centre + weight_j * around_j(centre)

    def put_residual(z, value):
        residual = force - value
        field_ref[z] = residual
        residual_ref[z] = residual[0:16]

    def put_image(z, value):
        next_ref[z] = value
        image_ref[z] = value[0:16]

    def put_second(z, value):
        second_ref[z] = value

    shared = (
        lambda z: roots_ref[z], lambda z: scale_ref[z], weight_i, weight_j, friction, bare, layers,
    )
    apply(lambda z: mask * wide_ref[z], put_residual, *shared)
    apply(lambda z: field_ref[z], put_image, *shared)
    apply(lambda z: next_ref[z], put_second, *shared, kept=16)
    totals = products(
        lambda z: field_ref[z], lambda z: next_ref[z], lambda z: second_ref[z], layers,
        [jnp.zeros((8, 128), jnp.float32)] * 4,
    )

    lane8 = lanes((8, 128))
    row8 = rows((8, 128))
    spot = lane8 % STRIP
    edge = (lane8 < 4 * STRIP) & (((spot >= 4) & (spot < 8)) | ((spot >= 16) & (spot < 20)))
    table = table_ref[...]
    for g in range(4):
        line = jnp.broadcast_to(jnp.sum(totals[g], axis=0, keepdims=True), (8, 128))
        for s in range(2):
            here = edge & ((lane8 // STRIP) % 2 == s) & (row8 == 2 * g + s)
            table = table + jnp.where(here, line, 0.0)
    table = jnp.sum(table, axis=1, keepdims=True)
    line = jnp.sum(jnp.where(lane8 == row8, table, 0.0), axis=0, keepdims=True)
    gram_ref[...] = jnp.broadcast_to(line, gram_ref.shape)


def combine(
    gram_ref, residual_ref, image_ref, start_ref, side_residual_ref, side_image_ref, out_ref
):
    layers = start_ref.shape[1]
    shape = (8, 128)
    lane = lanes(shape)
    total = jnp.broadcast_to(jnp.sum(gram_ref[...], axis=0, keepdims=True), shape)
    ks, ms = [], []
    for s in range(2):
        rr, ra, aa, ab = (
            jnp.broadcast_to(total[:, q : q + 1], shape) for q in (s, 2 + s, 4 + s, 6 + s)
        )
        first = rr / ra
        norm_next = rr - 2.0 * first * ra + first * first * aa
        growth = 1.0 + norm_next / rr
        curve = growth * growth * ra - 2.0 * growth * first * aa + first * first * ab
        second = norm_next / curve
        ks.append(first + second * growth)
        ms.append(second * first)
    odd = (lane // STRIP) % 2 == 1
    k_side = jnp.where(odd, ks[1], ks[0])
    m_side = jnp.where(odd, ms[1], ms[0])
    for z in range(layers):
        for t in range(2):
            at = slice(8 * t, 8 * t + 8)
            side = k_side * side_residual_ref[z, at] - m_side * side_image_ref[z, at]
            for c in range(2):
                step = ks[0] * residual_ref[2 * c, z, at] - ms[0] * image_ref[2 * c, z, at]
                step = step + ks[1] * residual_ref[2 * c + 1, z, at]
                step = step - ms[1] * image_ref[2 * c + 1, z, at]
                base = 2 * STRIP * c
                left = roll(side, -(base + 4), 1) + roll(side, -(base + STRIP + 4), 1)
                right = roll(side, 124 - base - 16, 1) + roll(side, 124 - base - STRIP - 16, 1)
                step = jnp.where(lane < HALO, left, step)
                step = jnp.where(lane >= 128 - HALO, right, step)
                out_ref[c, z, at] = start_ref[c, z, at] + step


def f32(*shape):
    return pltpu.VMEM(shape, jnp.float32)


def call(kernel, outs, ins, name, scratch=(), in_specs=None):
    specs = in_specs or [VMEM] * len(ins)
    ins = [
        pltpu.with_memory_space_constraint(x, pltpu.VMEM) if spec is VMEM else x
        for x, spec in zip(ins, specs)
    ]
    return pl.pallas_call(
        kernel,
        in_specs=specs,
        out_specs=[VMEM] * len(outs),
        out_shape=list(outs),
        scratch_shapes=list(scratch),
        name=name,
    )(*ins)


def swap_sides(by_odd, by_even, axis, other="ens"):
    count = lax.axis_size(axis)
    others = lax.axis_size(other) if other else 1

    def swap(message, first):
        pairs = []
        for o in range(others):
            for i in range((first + o) % 2, count - 1, 2):
                low, high = i * others + o, (i + 1) * others + o
                pairs += [(low, high), (high, low)]
        return lax.ppermute(message, (axis, other) if other else axis, pairs)

    return swap(by_odd, 1), swap(by_even, 0)


def body(u_prior, friction_rows, friction_table, bed_fixed, ice_mask):
    members, parts, layers, rows_x, rows_y = u_prior.shape
    total_x = rows_x * lax.axis_size("plane")
    row_place = lax.axis_index("plane").reshape(1)
    row_turn = row_place + lax.axis_index("ens")
    column_place = lax.axis_index("planey").reshape(1)
    by_odd, by_even, geo, u_near = call(
        pack_rows,
        [
            f32(layers + 1, 2, 8, rows_y),
            f32(layers + 1, 2, 8, rows_y),
            f32(4, rows_x, rows_y),
            f32(*u_prior.shape),
        ],
        [row_turn, friction_rows, u_prior, friction_table, bed_fixed, ice_mask],
        "pack_rows",
        scratch=[
            pltpu.SMEM(friction_rows.shape, jnp.int32),
            pltpu.VMEM(friction_table.shape, jnp.float32),
            pltpu.VMEM((2, rows_x, rows_y), jnp.int32),
            pltpu.SemaphoreType.DMA((5,)),
        ],
        in_specs=[SMEM] + [ANY] * 5,
    )
    by_odd, by_even = swap_sides(by_odd, by_even, "plane")
    own = call(
        pack_strips,
        [f32(layers + 1, rows_x, 128), f32(2, rows_x, 128), f32(2, rows_x, 128)],
        [column_place, u_near, geo],
        "pack_strips",
        in_specs=[SMEM, VMEM, VMEM],
    )
    outer, strip, side_odd, side_even = call(
        pack_columns,
        [f32(layers + 1, 4, 8, rows_y), f32(layers + 1, 24, 128), f32(2, 24, 128), f32(2, 24, 128)],
        [row_turn, column_place, *own, by_odd, by_even],
        "pack_columns",
        in_specs=[SMEM, SMEM] + [VMEM] * 5,
    )
    side_odd, side_even = swap_sides(side_odd, side_even, "planey", None)
    residual, image, start, table = call(
        lambda *refs: main_part(*refs, total_x=total_x),
        [
            f32(4, layers, rows_x, 128),
            f32(4, layers, rows_x, 128),
            f32(2, layers, rows_x, 128),
            f32(8, 128),
        ],
        [row_place, u_near, geo, outer],
        "main_part",
        scratch=[
            pltpu.VMEM((2, layers, 24, 128), jnp.float32),
            pltpu.VMEM((layers, 24, 128), jnp.float32),
            pltpu.VMEM((2, layers, 24, 128), jnp.float32),
            pltpu.VMEM((layers, 24, 128), jnp.float32),
            pltpu.VMEM((layers, 24, 128), jnp.float32),
            pltpu.VMEM((layers, 16, 128), jnp.float32),
        ],
        in_specs=[SMEM] + [VMEM] * 3,
    )
    side_residual, side_image, gram = call(
        lambda *refs: strip_part(*refs, total_x=total_x),
        [
            f32(layers, rows_x, 128),
            f32(layers, rows_x, 128),
            f32(lax.axis_size("plane") * lax.axis_size("planey"), 128),
        ],
        [row_place, column_place, strip, side_odd, side_even, table],
        "strip_part",
        scratch=[pltpu.VMEM((layers, 24, 128), jnp.float32)] * 5
        + [pltpu.VMEM((layers, 16, 128), jnp.float32)],
        in_specs=[SMEM, SMEM] + [VMEM] * 4,
    )
    gathered = lax.all_to_all(gram, ("plane", "planey"), 0, 0, tiled=True)
    (local_sum,) = call(
        combine, [f32(2, layers, rows_x, 128)], [gathered, residual, image, start, side_residual, side_image],
        "combine",

    )
    summed = lax.all_gather(local_sum, "ens").sum(axis=0)
    return summed / (members * lax.axis_size("ens"))


def solution(mesh):
    in_specs = (
        P(("group", "ens"), None, None, "plane", "planey"),
        P(("group", "ens")),
        P("group", "plane", "planey"),
        P("plane", "planey"),
        P("plane", "planey"),
    )
    out_specs = P("group", None, "plane", "planey")
    return jax.shard_map(body, mesh=mesh, in_specs=in_specs, out_specs=out_specs, check_vma=False)
```

```python
import jax
import jax.numpy as jnp
from jax import lax
from jax.experimental import pallas as pl
from jax.experimental.pallas import tpu as pltpu
from jax.sharding import PartitionSpec as P

bed_unit = 2.0 ** (-29)
HALO = 4
STRIP = 24
GROUPED = STRIP // HALO
MAIN_I = (0.25, 0.125)
MAIN_J = (0.125, 0.25)


VMEM = pl.BlockSpec(memory_space=pltpu.VMEM)
SMEM = pl.BlockSpec(memory_space=pltpu.SMEM)
ANY = pl.BlockSpec(memory_space=pl.ANY)


def roll(x, shift, axis):
    return pltpu.roll(x, shift % x.shape[axis], axis)


def lanes(shape):
    return lax.broadcasted_iota(jnp.int32, shape, len(shape) - 1)


def rows(shape):
    return lax.broadcasted_iota(jnp.int32, shape, len(shape) - 2)


def pack_rows(
    row_turn_ref, rows_hbm, u_hbm, table_hbm, bed_hbm, mask_hbm,
    odd_ref, even_ref, geo_ref, u_ref, rows_ref, table_ref, ints_ref, sems,
):
    layers = u_ref.shape[2]
    moves = [
        (u_hbm, u_ref),
        (rows_hbm, rows_ref),
        (table_hbm, table_ref),
        (mask_hbm, ints_ref.at[0]),
        (bed_hbm, ints_ref.at[1]),
    ]
    copies = [pltpu.make_async_copy(*move, sems.at[i]) for i, move in enumerate(moves)]
    for copy in copies:
        copy.start()
    for copy in copies:
        copy.wait()
    geo_ref[0] = ints_ref[0].astype(jnp.float32)
    geo_ref[1] = ints_ref[1].astype(jnp.float32) * bed_unit
    for s in range(2):
        geo_ref[2 + s] = table_ref[rows_ref[s]]
    low = rows((8, 128)) < HALO
    odd = row_turn_ref[0] % 2 == 1
    for layer in range(layers + 1):
        for pair in range(2):
            tiles = [
                u_ref[s, pair, layer] if layer < layers else geo_ref[2 * pair + s] for s in range(2)
            ]
            top = [tile[0:8] for tile in tiles]
            end = [tile[8:16] for tile in tiles]
            up = jnp.where(low, roll(end[0], HALO, 0), end[1])
            down = jnp.where(low, top[0], roll(top[1], HALO, 0))
            odd_ref[layer, pair] = jnp.where(odd, up, down)
            even_ref[layer, pair] = jnp.where(odd, down, up)


def strip_tile(tiles):
    lane = lanes((8, 128))
    strip = jnp.zeros((8, 128), jnp.float32)
    for k, tile in enumerate(tiles):
        at = lane - STRIP * k
        strip = jnp.where((at >= 4) & (at < 12), roll(tile, STRIP * k + 4, 1), strip)
        strip = jnp.where((at >= 12) & (at < 20), roll(tile, STRIP * k + 12 - 120, 1), strip)
    return strip


def side_messages(strip_of, layers, swapped):
    lane = lanes((8, 128))
    used = lane < 4 * STRIP
    slot = (lane % STRIP) // HALO
    for group in range(2):
        right = jnp.zeros((8, 128), jnp.float32)
        left = right
        for index in range(min(GROUPED, layers + 1 - GROUPED * group)):
            strip = strip_of(GROUPED * group + index)
            here = used & (slot == index)
            right = jnp.where(here, roll(strip, HALO * index - 16, 1), right)
            left = jnp.where(here, roll(strip, HALO * index - 4, 1), left)
        yield group, jnp.where(swapped, right, left), jnp.where(swapped, left, right)


def pack_strips(column_place_ref, u_ref, geo_ref, own_ref, odd_ref, even_ref):
    layers = u_ref.shape[2]
    for layer in range(layers + 1):
        for t in range(2):
            at = slice(8 * t, 8 * t + 8)
            own_ref[layer, at] = strip_tile(
                [u_ref[k % 2, k // 2, layer, at] if layer < layers else geo_ref[k, at] for k in range(4)]
            )
    swapped = column_place_ref[0] % 2 == 1

    def send(t, carry):
        at = pl.ds(pl.multiple_of(8 * t, 8), 8)
        for group, by_odd, by_even in side_messages(lambda layer: own_ref[layer, at], layers, swapped):
            odd_ref[group, at] = by_odd
            even_ref[group, at] = by_even
        return carry

    lax.fori_loop(0, 2, send, 0)


def pack_columns(
    row_turn_ref, column_place_ref, own_ref, own_odd_ref, own_even_ref, by_odd_ref, by_even_ref,
    outer_ref, strip_ref, odd_ref, even_ref,
):
    layers = own_ref.shape[0] - 1
    low = rows((8, 128)) < HALO
    odd = row_turn_ref[0] % 2 == 1
    for layer in range(layers + 1):
        outer = []
        for pair in range(2):
            by_odd = by_odd_ref[layer, pair]
            by_even = by_even_ref[layer, pair]
            below = jnp.where(odd, by_even, by_odd)
            above = jnp.where(odd, by_odd, by_even)
            outer.append(jnp.where(low, above, roll(below, HALO, 0)))
            outer.append(jnp.where(low, roll(above, HALO, 0), below))
        for k in range(4):
            outer_ref[layer, k] = outer[k]
        strip_ref[layer, 0:16] = own_ref[layer]
        strip_ref[layer, 16:24] = strip_tile(outer)
    for group in range(2):
        odd_ref[group, 0:16] = own_odd_ref[group]
        even_ref[group, 0:16] = own_even_ref[group]
    swapped = column_place_ref[0] % 2 == 1

    for group, by_odd, by_even in side_messages(lambda layer: strip_ref[layer, 16:24], layers, swapped):
        odd_ref[group, 16:24] = by_odd
        even_ref[group, 16:24] = by_even


def around_i(x):
    return roll(x, 1, 0) + roll(x, -1, 0)


def around_j(x):
    return roll(x, 1, 1) + roll(x, -1, 1)


def forces(cover, ground, row_start, total_x):
    row = rows(cover.shape)
    position = (jnp.where(row < 20, row, row - 24) + row_start).astype(jnp.float32)
    thickness = 1.0 + 2.0 * position / (total_x - 1)
    slope_x = (roll(ground, -1, 0) - roll(ground, 1, 0)) * 0.5
    slope_y = (roll(ground, -1, 1) - roll(ground, 1, 1)) * 0.5
    return -(cover * thickness * slope_x), -(cover * thickness * slope_y)


def difference(get, z, layers):
    if z == 0:
        return get(1)
    if z + 1 == layers:
        return -get(z - 1)
    return get(z + 1) - get(z - 1)


def viscosity(get_u, get_v, z, layers, cover):
    u, v = get_u(z), get_v(z)
    stretch_x = roll(u, -1, 0) - roll(u, 1, 0)
    stretch_y = roll(v, -1, 1) - roll(v, 1, 1)
    shear = (roll(u, -1, 1) - roll(u, 1, 1)) + (roll(v, -1, 0) - roll(v, 1, 0))
    rise_u = difference(get_u, z, layers)
    rise_v = difference(get_v, z, layers)
    strain = stretch_x * stretch_x + stretch_y * (stretch_y + stretch_x)
    strain = strain + 0.25 * (shear * shear + (rise_u * rise_u + rise_v * rise_v))
    return cover * jnp.exp(jnp.log(0.25 * strain + 0.1) * (-1.0 / 6.0))


def with_neighbours(get, z, layers):
    if z == 0:
        return get(0) + 0.5 * get(1)
    if z + 1 == layers:
        return get(z) + 0.5 * get(z - 1)
    return get(z) + 0.5 * (get(z - 1) + get(z + 1))


def apply(get, put, roots, scale, weight_i, weight_j, friction, empty, layers, kept=24):
    def kept_rows(x):
        return x[0:kept] if x.ndim else x

    def filtered(z):
        product = roots(z) * get(z)
        product = (product + weight_i * around_i(product))[0:kept]
        return product + kept_rows(weight_j) * around_j(product)

    done = {}
    for z in range(layers + 1):
        if z < layers:
            done[z] = filtered(z)
        if z > 0:
            at = z - 1
            total = with_neighbours(lambda y: done[y], at, layers)
            field = get(at)[0:kept]
            result = 4.0 * roots(at)[0:kept] * (scale(at)[0:kept] * field - total)
            put(at, result + (friction if at == 0 else empty)[0:kept] * field)


def products(field, image, second, layers, totals):
    totals = list(totals)
    for z in range(layers):
        for t in range(2):
            at = slice(8 * t, 8 * t + 8)
            r, a, b = field(z)[at], image(z)[at], second(z)[at]
            for i, (x, y) in enumerate(((r, r), (r, a), (a, a), (a, b))):
                totals[i] = totals[i] + x * y
    return totals


def main_part(
    row_place_ref, u_ref, geo_ref, outer_ref,
    residual_ref, image_ref, start_ref, table_ref,
    wide_ref, roots_ref, scale_ref, field_ref, next_ref, second_ref, *, total_x,
):
    layers = u_ref.shape[2]
    row_start = row_place_ref[0] * 16

    def geo(k):
        return jnp.concatenate([geo_ref[k], outer_ref[layers, k]], axis=0)

    mask = geo(0)
    bare = 1.0 - mask
    force = forces(mask, geo(1), row_start, total_x)
    lane8 = lanes((8, 128))
    inside = (lane8 >= HALO) & (lane8 < 128 - HALO)
    row8 = rows((8, 128))
    table_ref[...] = jnp.zeros((8, 128), jnp.float32)

    def sample(s, carry):
        friction = mask * jnp.concatenate([geo_ref[2 + s], outer_ref[layers, 2 + s]], axis=0) + bare
        for c in range(2):
            for z in range(layers):
                wide_ref[c, z, 0:16] = u_ref[s, c, z]
                wide_ref[c, z, 16:24] = outer_ref[z, 2 * c + s]
        for z in range(layers):
            roots_ref[z] = viscosity(
                lambda y: wide_ref[0, y], lambda y: wide_ref[1, y], z, layers, mask
            )
        for z in range(layers):
            centre = with_neighbours(lambda y: roots_ref[y], z, layers)
            along_i = around_i(centre)
            along_j = around_j(centre)
            both = centre + 0.03125 * around_j(along_i)
            for c in range(2):
                scale_ref[c, z] = both + MAIN_I[c] * along_i + MAIN_J[c] * along_j

        def component(c, carry):
            first = c == 0
            weight_i = jnp.where(first, MAIN_I[0], MAIN_I[1])
            weight_j = jnp.where(first, MAIN_J[0], MAIN_J[1])
            pull = jnp.where(first, force[0], force[1])
            shared = (
                lambda z: roots_ref[z], lambda z: scale_ref[c, z],
                weight_i, weight_j, friction, bare, layers,
            )

            def put_residual(z, value):
                residual = pull - value
                field_ref[z] = residual
                residual_ref[2 * c + s, z] = residual[0:16]

            def put_image(z, value):
                next_ref[z] = value
                image_ref[2 * c + s, z] = value[0:16]

            def put_second(z, value):
                second_ref[z] = value

            apply(lambda z: mask * wide_ref[c, z], put_residual, *shared)
            apply(lambda z: field_ref[z], put_image, *shared)
            apply(lambda z: next_ref[z], put_second, *shared, kept=16)
            totals = products(
                lambda z: field_ref[z], lambda z: next_ref[z], lambda z: second_ref[z], layers,
                [jnp.zeros((8, 128), jnp.float32)] * 4,
            )
            for g in range(4):
                line = jnp.sum(jnp.where(inside, totals[g], 0.0), axis=0, keepdims=True)
                table_ref[...] += jnp.where(row8 == 2 * g + s, line, 0.0)
            return carry

        return lax.fori_loop(0, 2, component, carry)

    lax.fori_loop(0, 2, sample, 0)
    for c in range(2):
        for z in range(layers):
            start_ref[c, z] = mask[0:16] * u_ref[0, c, z] + mask[0:16] * u_ref[1, c, z]


def strip_part(
    row_place_ref, column_place_ref, strip_ref, by_odd_ref, by_even_ref, table_ref,
    residual_ref, image_ref, gram_ref,
    wide_ref, roots_ref, scale_ref, field_ref, next_ref, second_ref, *, total_x,
):
    layers = strip_ref.shape[0] - 1
    shape = (24, 128)
    lane = lanes(shape)
    used = lane < 4 * STRIP
    place = lane % STRIP
    number = lane // STRIP
    low = lane < 2 * STRIP

    geo = None
    odd = column_place_ref[0] % 2 == 1
    from_left = [jnp.where(odd, by_even_ref[g], by_odd_ref[g]) for g in range(2)]
    from_right = [jnp.where(odd, by_odd_ref[g], by_even_ref[g]) for g in range(2)]
    for layer in range(layers + 1):
        group, index = layer // GROUPED, layer % GROUPED
        strip = strip_ref[layer]
        strip = jnp.where(used & (place < 4), roll(from_left[group], -HALO * index, 1), strip)
        strip = jnp.where(used & (place >= 20), roll(from_right[group], 20 - HALO * index, 1), strip)
        if layer < layers:
            wide_ref[layer] = strip
        else:
            geo = strip

    def spread(to):
        result = jnp.zeros(shape, jnp.float32)
        for k in range(4):
            result = jnp.where(number == k, roll(geo, STRIP * (k - to), 1), result)
        return result

    mask = spread(0)
    bare = 1.0 - mask
    friction = mask * jnp.where(low, roll(geo, -2 * STRIP, 1), geo) + bare
    force_x, force_y = forces(mask, spread(1), row_place_ref[0] * 16, total_x)
    force = jnp.where(low, force_x, force_y)
    weight_i = jnp.where(low, MAIN_I[0], MAIN_I[1])
    weight_j = jnp.where(low, MAIN_J[0], MAIN_J[1])

    for z in range(layers):
        wide = wide_ref[z]
        slope_i = roll(wide, -1, 0) - roll(wide, 1, 0)
        slope_j = roll(wide, -1, 1) - roll(wide, 1, 1)
        rise = difference(lambda y: wide_ref[y], z, layers)
        rise = rise * rise
        stretch = jnp.where(low, slope_i, slope_j)
        shear = jnp.where(low, slope_j, slope_i)
        stretch_y = roll(stretch, -2 * STRIP, 1)
        shear = shear + roll(shear, -2 * STRIP, 1)
        strain = stretch * stretch + stretch_y * (stretch_y + stretch)
        strain = strain + 0.25 * (shear * shear + (rise + roll(rise, -2 * STRIP, 1)))
        found = mask * jnp.exp(jnp.log(0.25 * strain + 0.1) * (-1.0 / 6.0))
        roots_ref[z] = jnp.where(low, found, roll(found, 2 * STRIP, 1))
    for z in range(layers):
        centre = with_neighbours(lambda y: roots_ref[y], z, layers)
        centre = centre + weight_i * around_i(centre)
        scale_ref[z] = centre + weight_j * around_j(centre)

    def put_residual(z, value):
        residual = force - value
        field_ref[z] = residual
        residual_ref[z] = residual[0:16]

    def put_image(z, value):
        next_ref[z] = value
        image_ref[z] = value[0:16]

    def put_second(z, value):
        second_ref[z] = value

    shared = (
        lambda z: roots_ref[z], lambda z: scale_ref[z], weight_i, weight_j, friction, bare, layers,
    )
    apply(lambda z: mask * wide_ref[z], put_residual, *shared)
    apply(lambda z: field_ref[z], put_image, *shared)
    apply(lambda z: next_ref[z], put_second, *shared, kept=16)
    totals = products(
        lambda z: field_ref[z], lambda z: next_ref[z], lambda z: second_ref[z], layers,
        [jnp.zeros((8, 128), jnp.float32)] * 4,
    )

    lane8 = lanes((8, 128))
    row8 = rows((8, 128))
    spot = lane8 % STRIP
    edge = (lane8 < 4 * STRIP) & (((spot >= 4) & (spot < 8)) | ((spot >= 16) & (spot < 20)))
    table = table_ref[...]
    for g in range(4):
        line = jnp.broadcast_to(jnp.sum(totals[g], axis=0, keepdims=True), (8, 128))
        for s in range(2):
            here = edge & ((lane8 // STRIP) % 2 == s) & (row8 == 2 * g + s)
            table = table + jnp.where(here, line, 0.0)
    table = jnp.sum(table, axis=1, keepdims=True)
    line = jnp.sum(jnp.where(lane8 == row8, table, 0.0), axis=0, keepdims=True)
    gram_ref[...] = jnp.broadcast_to(line, gram_ref.shape)


def combine(
    gram_ref, residual_ref, image_ref, start_ref, side_residual_ref, side_image_ref, out_ref
):
    layers = start_ref.shape[1]
    shape = (8, 128)
    lane = lanes(shape)
    total = jnp.broadcast_to(jnp.sum(gram_ref[...], axis=0, keepdims=True), shape)
    ks, ms = [], []
    for s in range(2):
        rr, ra, aa, ab = (
            jnp.broadcast_to(total[:, q : q + 1], shape) for q in (s, 2 + s, 4 + s, 6 + s)
        )
        first = rr / ra
        norm_next = rr - 2.0 * first * ra + first * first * aa
        growth = 1.0 + norm_next / rr
        curve = growth * growth * ra - 2.0 * growth * first * aa + first * first * ab
        second = norm_next / curve
        ks.append(first + second * growth)
        ms.append(second * first)
    odd = (lane // STRIP) % 2 == 1
    k_side = jnp.where(odd, ks[1], ks[0])
    m_side = jnp.where(odd, ms[1], ms[0])
    for z in range(layers):
        for t in range(2):
            at = slice(8 * t, 8 * t + 8)
            side = k_side * side_residual_ref[z, at] - m_side * side_image_ref[z, at]
            for c in range(2):
                step = ks[0] * residual_ref[2 * c, z, at] - ms[0] * image_ref[2 * c, z, at]
                step = step + ks[1] * residual_ref[2 * c + 1, z, at]
                step = step - ms[1] * image_ref[2 * c + 1, z, at]
                base = 2 * STRIP * c
                left = roll(side, -(base + 4), 1) + roll(side, -(base + STRIP + 4), 1)
                right = roll(side, 124 - base - 16, 1) + roll(side, 124 - base - STRIP - 16, 1)
                step = jnp.where(lane < HALO, left, step)
                step = jnp.where(lane >= 128 - HALO, right, step)
                out_ref[c, z, at] = start_ref[c, z, at] + step


def f32(*shape):
    return pltpu.VMEM(shape, jnp.float32)


def call(kernel, outs, ins, name, scratch=(), in_specs=None):
    specs = in_specs or [VMEM] * len(ins)
    ins = [
        pltpu.with_memory_space_constraint(x, pltpu.VMEM) if spec is VMEM else x
        for x, spec in zip(ins, specs)
    ]
    return pl.pallas_call(
        kernel,
        in_specs=specs,
        out_specs=[VMEM] * len(outs),
        out_shape=list(outs),
        scratch_shapes=list(scratch),
        name=name,
    )(*ins)


def swap_sides(by_odd, by_even, axis, other="ens"):
    count = lax.axis_size(axis)
    others = lax.axis_size(other) if other else 1

    def swap(message, first):
        pairs = []
        for o in range(others):
            for i in range((first + o) % 2, count - 1, 2):
                low, high = i * others + o, (i + 1) * others + o
                pairs += [(low, high), (high, low)]
        return lax.ppermute(message, (axis, other) if other else axis, pairs)

    return swap(by_odd, 1), swap(by_even, 0)


def body(u_prior, friction_rows, friction_table, bed_fixed, ice_mask):
    members, parts, layers, rows_x, rows_y = u_prior.shape
    total_x = rows_x * lax.axis_size("plane")
    row_place = lax.axis_index("plane").reshape(1)
    row_turn = row_place + lax.axis_index("ens")
    column_place = lax.axis_index("planey").reshape(1)
    by_odd, by_even, geo, u_near = call(
        pack_rows,
        [
            f32(layers + 1, 2, 8, rows_y),
            f32(layers + 1, 2, 8, rows_y),
            f32(4, rows_x, rows_y),
            f32(*u_prior.shape),
        ],
        [row_turn, friction_rows, u_prior, friction_table, bed_fixed, ice_mask],
        "pack_rows",
        scratch=[
            pltpu.SMEM(friction_rows.shape, jnp.int32),
            pltpu.VMEM(friction_table.shape, jnp.float32),
            pltpu.VMEM((2, rows_x, rows_y), jnp.int32),
            pltpu.SemaphoreType.DMA((5,)),
        ],
        in_specs=[SMEM] + [ANY] * 5,
    )
    by_odd, by_even = swap_sides(by_odd, by_even, "plane")
    own = call(
        pack_strips,
        [f32(layers + 1, rows_x, 128), f32(2, rows_x, 128), f32(2, rows_x, 128)],
        [column_place, u_near, geo],
        "pack_strips",
        in_specs=[SMEM, VMEM, VMEM],
    )
    outer, strip, side_odd, side_even = call(
        pack_columns,
        [f32(layers + 1, 4, 8, rows_y), f32(layers + 1, 24, 128), f32(2, 24, 128), f32(2, 24, 128)],
        [row_turn, column_place, *own, by_odd, by_even],
        "pack_columns",
        in_specs=[SMEM, SMEM] + [VMEM] * 5,
    )
    side_odd, side_even = swap_sides(side_odd, side_even, "planey", None)
    residual, image, start, table = call(
        lambda *refs: main_part(*refs, total_x=total_x),
        [
            f32(4, layers, rows_x, 128),
            f32(4, layers, rows_x, 128),
            f32(2, layers, rows_x, 128),
            f32(8, 128),
        ],
        [row_place, u_near, geo, outer],
        "main_part",
        scratch=[
            pltpu.VMEM((2, layers, 24, 128), jnp.float32),
            pltpu.VMEM((layers, 24, 128), jnp.float32),
            pltpu.VMEM((2, layers, 24, 128), jnp.float32),
            pltpu.VMEM((layers, 24, 128), jnp.float32),
            pltpu.VMEM((layers, 24, 128), jnp.float32),
            pltpu.VMEM((layers, 16, 128), jnp.float32),
        ],
        in_specs=[SMEM] + [VMEM] * 3,
    )
    side_residual, side_image, gram = call(
        lambda *refs: strip_part(*refs, total_x=total_x),
        [
            f32(layers, rows_x, 128),
            f32(layers, rows_x, 128),
            f32(lax.axis_size("plane") * lax.axis_size("planey"), 128),
        ],
        [row_place, column_place, strip, side_odd, side_even, table],
        "strip_part",
        scratch=[pltpu.VMEM((layers, 24, 128), jnp.float32)] * 5
        + [pltpu.VMEM((layers, 16, 128), jnp.float32)],
        in_specs=[SMEM, SMEM] + [VMEM] * 4,
    )
    gathered = lax.all_to_all(gram, ("plane", "planey"), 0, 0, tiled=True)
    (local_sum,) = call(
        combine, [f32(2, layers, rows_x, 128)], [gathered, residual, image, start, side_residual, side_image],
        "combine",

    )
    summed = lax.all_gather(local_sum, "ens").sum(axis=0)
    return summed / (members * lax.axis_size("ens"))


def solution(mesh):
    in_specs = (
        P(("group", "ens"), None, None, "plane", "planey"),
        P(("group", "ens")),
        P("group", "plane", "planey"),
        P("plane", "planey"),
        P("plane", "planey"),
    )
    out_specs = P("group", None, "plane", "planey")
    return jax.shard_map(body, mesh=mesh, in_specs=in_specs, out_specs=out_specs, check_vma=False)
```

```python
import jax
import jax.numpy as jnp
from jax import lax
from jax.experimental import pallas as pl
from jax.experimental.pallas import tpu as pltpu
from jax.sharding import PartitionSpec as P

bed_unit = 2.0 ** (-29)
HALO = 4
STRIP = 24
GROUPED = STRIP // HALO
SECOND = 64
STARTS = (0, STRIP, SECOND, SECOND + STRIP)
MAIN_I = (0.25, 0.125)
MAIN_J = (0.125, 0.25)


VMEM = pl.BlockSpec(memory_space=pltpu.VMEM)
SMEM = pl.BlockSpec(memory_space=pltpu.SMEM)
ANY = pl.BlockSpec(memory_space=pl.ANY)


def roll(x, shift, axis):
    return pltpu.roll(x, shift % x.shape[axis], axis)


def lanes(shape):
    return lax.broadcasted_iota(jnp.int32, shape, len(shape) - 1)


def rows(shape):
    return lax.broadcasted_iota(jnp.int32, shape, len(shape) - 2)


def pack_rows(
    row_turn_ref, rows_hbm, u_hbm, table_hbm, bed_hbm, mask_hbm,
    odd_ref, even_ref, geo_ref, u_ref, rows_ref, table_ref, ints_ref, sems,
):
    layers = u_ref.shape[2]
    moves = [
        (u_hbm, u_ref),
        (rows_hbm, rows_ref),
        (table_hbm, table_ref),
        (mask_hbm, ints_ref.at[0]),
        (bed_hbm, ints_ref.at[1]),
    ]
    copies = [pltpu.make_async_copy(*move, sems.at[i]) for i, move in enumerate(moves)]
    for copy in copies:
        copy.start()
    for copy in copies:
        copy.wait()
    geo_ref[0] = ints_ref[0].astype(jnp.float32)
    geo_ref[1] = ints_ref[1].astype(jnp.float32) * bed_unit
    for s in range(2):
        geo_ref[2 + s] = table_ref[rows_ref[s]]
    low = rows((8, 128)) < HALO
    odd = row_turn_ref[0] % 2 == 1
    for layer in range(layers + 1):
        for pair in range(2):
            tiles = [
                u_ref[s, pair, layer] if layer < layers else geo_ref[2 * pair + s] for s in range(2)
            ]
            top = [tile[0:8] for tile in tiles]
            end = [tile[8:16] for tile in tiles]
            up = jnp.where(low, roll(end[0], HALO, 0), end[1])
            down = jnp.where(low, top[0], roll(top[1], HALO, 0))
            odd_ref[layer, pair] = jnp.where(odd, up, down)
            even_ref[layer, pair] = jnp.where(odd, down, up)


def strip_tile(tiles):
    lane = lanes((8, 128))
    strip = jnp.zeros((8, 128), jnp.float32)
    for k, tile in enumerate(tiles):
        at = lane - STARTS[k]
        strip = jnp.where((at >= 4) & (at < 12), roll(tile, STARTS[k] + 4, 1), strip)
        strip = jnp.where((at >= 12) & (at < 20), roll(tile, STARTS[k] + 12 - 120, 1), strip)
    return strip


def side_messages(strip_of, layers, swapped):
    lane = lanes((8, 128))
    used = lane % SECOND < 2 * STRIP
    slot = (lane % SECOND % STRIP) // HALO
    for group in range(2):
        right = jnp.zeros((8, 128), jnp.float32)
        left = right
        for index in range(min(GROUPED, layers + 1 - GROUPED * group)):
            strip = strip_of(GROUPED * group + index)
            here = used & (slot == index)
            right = jnp.where(here, roll(strip, HALO * index - 16, 1), right)
            left = jnp.where(here, roll(strip, HALO * index - 4, 1), left)
        yield group, jnp.where(swapped, right, left), jnp.where(swapped, left, right)


def pack_strips(column_place_ref, u_ref, geo_ref, own_ref, odd_ref, even_ref):
    layers = u_ref.shape[2]
    for layer in range(layers + 1):
        for t in range(2):
            at = slice(8 * t, 8 * t + 8)
            own_ref[layer, at] = strip_tile(
                [u_ref[k % 2, k // 2, layer, at] if layer < layers else geo_ref[k, at] for k in range(4)]
            )
    swapped = column_place_ref[0] % 2 == 1

    def send(t, carry):
        at = pl.ds(pl.multiple_of(8 * t, 8), 8)
        for group, by_odd, by_even in side_messages(lambda layer: own_ref[layer, at], layers, swapped):
            odd_ref[group, at] = by_odd
            even_ref[group, at] = by_even
        return carry

    lax.fori_loop(0, 2, send, 0)


def pack_columns(
    row_turn_ref, column_place_ref, own_ref, own_odd_ref, own_even_ref, by_odd_ref, by_even_ref,
    outer_ref, strip_ref, odd_ref, even_ref,
):
    layers = own_ref.shape[0] - 1
    low = rows((8, 128)) < HALO
    odd = row_turn_ref[0] % 2 == 1
    for layer in range(layers + 1):
        outer = []
        for pair in range(2):
            by_odd = by_odd_ref[layer, pair]
            by_even = by_even_ref[layer, pair]
            below = jnp.where(odd, by_even, by_odd)
            above = jnp.where(odd, by_odd, by_even)
            outer.append(jnp.where(low, above, roll(below, HALO, 0)))
            outer.append(jnp.where(low, roll(above, HALO, 0), below))
        for k in range(4):
            outer_ref[layer, k] = outer[k]
        strip_ref[layer, 0:16] = own_ref[layer]
        strip_ref[layer, 16:24] = strip_tile(outer)
    for group in range(2):
        odd_ref[group, 0:16] = own_odd_ref[group]
        even_ref[group, 0:16] = own_even_ref[group]
    swapped = column_place_ref[0] % 2 == 1

    for group, by_odd, by_even in side_messages(lambda layer: strip_ref[layer, 16:24], layers, swapped):
        odd_ref[group, 16:24] = by_odd
        even_ref[group, 16:24] = by_even


def around_i(x):
    return roll(x, 1, 0) + roll(x, -1, 0)


def around_j(x):
    return roll(x, 1, 1) + roll(x, -1, 1)


def forces(cover, ground, row_start, total_x):
    row = rows(cover.shape)
    position = (jnp.where(row < 20, row, row - 24) + row_start).astype(jnp.float32)
    thickness = 1.0 + 2.0 * position / (total_x - 1)
    slope_x = (roll(ground, -1, 0) - roll(ground, 1, 0)) * 0.5
    slope_y = (roll(ground, -1, 1) - roll(ground, 1, 1)) * 0.5
    return -(cover * thickness * slope_x), -(cover * thickness * slope_y)


def difference(get, z, layers):
    if z == 0:
        return get(1)
    if z + 1 == layers:
        return -get(z - 1)
    return get(z + 1) - get(z - 1)


def viscosity(get_u, get_v, z, layers, cover):
    u, v = get_u(z), get_v(z)
    stretch_x = roll(u, -1, 0) - roll(u, 1, 0)
    stretch_y = roll(v, -1, 1) - roll(v, 1, 1)
    shear = (roll(u, -1, 1) - roll(u, 1, 1)) + (roll(v, -1, 0) - roll(v, 1, 0))
    rise_u = difference(get_u, z, layers)
    rise_v = difference(get_v, z, layers)
    strain = stretch_x * stretch_x + stretch_y * (stretch_y + stretch_x)
    strain = strain + 0.25 * (shear * shear + (rise_u * rise_u + rise_v * rise_v))
    return cover * jnp.exp(jnp.log(0.25 * strain + 0.1) * (-1.0 / 6.0))


def with_neighbours(get, z, layers):
    if z == 0:
        return get(0) + 0.5 * get(1)
    if z + 1 == layers:
        return get(z) + 0.5 * get(z - 1)
    return get(z) + 0.5 * (get(z - 1) + get(z + 1))


def apply(get, put, roots, scale, weight_i, weight_j, friction, empty, layers, kept=24):
    def kept_rows(x):
        return x[0:kept] if x.ndim else x

    def filtered(z):
        product = roots(z) * get(z)
        product = (product + weight_i * around_i(product))[0:kept]
        return product + kept_rows(weight_j) * around_j(product)

    done = {}
    for z in range(layers + 1):
        if z < layers:
            done[z] = filtered(z)
        if z > 0:
            at = z - 1
            total = with_neighbours(lambda y: done[y], at, layers)
            field = get(at)[0:kept]
            result = 4.0 * roots(at)[0:kept] * (scale(at)[0:kept] * field - total)
            put(at, result + (friction if at == 0 else empty)[0:kept] * field)


def products(field, image, second, layers, totals):
    totals = list(totals)
    for z in range(layers):
        for t in range(2):
            at = slice(8 * t, 8 * t + 8)
            r, a, b = field(z)[at], image(z)[at], second(z)[at]
            for i, (x, y) in enumerate(((r, r), (r, a), (a, a), (a, b))):
                totals[i] = totals[i] + x * y
    return totals


def main_part(
    row_place_ref, u_ref, geo_ref, outer_ref,
    residual_ref, image_ref, start_ref, table_ref,
    wide_ref, roots_ref, scale_ref, field_ref, next_ref, second_ref, *, total_x,
):
    layers = u_ref.shape[2]
    row_start = row_place_ref[0] * 16

    def geo(k):
        return jnp.concatenate([geo_ref[k], outer_ref[layers, k]], axis=0)

    mask = geo(0)
    bare = 1.0 - mask
    force = forces(mask, geo(1), row_start, total_x)
    lane8 = lanes((8, 128))
    inside = (lane8 >= HALO) & (lane8 < 128 - HALO)
    row8 = rows((8, 128))
    table_ref[...] = jnp.zeros((8, 128), jnp.float32)

    def sample(s, carry):
        friction = mask * jnp.concatenate([geo_ref[2 + s], outer_ref[layers, 2 + s]], axis=0) + bare
        for c in range(2):
            for z in range(layers):
                wide_ref[c, z, 0:16] = u_ref[s, c, z]
                wide_ref[c, z, 16:24] = outer_ref[z, 2 * c + s]
        for z in range(layers):
            roots_ref[z] = viscosity(
                lambda y: wide_ref[0, y], lambda y: wide_ref[1, y], z, layers, mask
            )
        for z in range(layers):
            centre = with_neighbours(lambda y: roots_ref[y], z, layers)
            along_i = around_i(centre)
            along_j = around_j(centre)
            both = centre + 0.03125 * around_j(along_i)
            for c in range(2):
                scale_ref[c, z] = both + MAIN_I[c] * along_i + MAIN_J[c] * along_j

        def component(c, carry):
            first = c == 0
            weight_i = jnp.where(first, MAIN_I[0], MAIN_I[1])
            weight_j = jnp.where(first, MAIN_J[0], MAIN_J[1])
            pull = jnp.where(first, force[0], force[1])
            shared = (
                lambda z: roots_ref[z], lambda z: scale_ref[c, z],
                weight_i, weight_j, friction, bare, layers,
            )

            def put_residual(z, value):
                residual = pull - value
                field_ref[z] = residual
                residual_ref[2 * c + s, z] = residual[0:16]

            def put_image(z, value):
                next_ref[z] = value
                image_ref[2 * c + s, z] = value[0:16]

            def put_second(z, value):
                second_ref[z] = value

            apply(lambda z: mask * wide_ref[c, z], put_residual, *shared)
            apply(lambda z: field_ref[z], put_image, *shared)
            apply(lambda z: next_ref[z], put_second, *shared, kept=16)
            totals = products(
                lambda z: field_ref[z], lambda z: next_ref[z], lambda z: second_ref[z], layers,
                [jnp.zeros((8, 128), jnp.float32)] * 4,
            )
            for g in range(4):
                line = jnp.sum(jnp.where(inside, totals[g], 0.0), axis=0, keepdims=True)
                table_ref[...] += jnp.where(row8 == 2 * g + s, line, 0.0)
            return carry

        return lax.fori_loop(0, 2, component, carry)

    lax.fori_loop(0, 2, sample, 0)
    for c in range(2):
        for z in range(layers):
            start_ref[c, z] = mask[0:16] * u_ref[0, c, z] + mask[0:16] * u_ref[1, c, z]


def strip_part(
    row_place_ref, column_place_ref, strip_ref, by_odd_ref, by_even_ref, table_ref,
    residual_ref, image_ref, gram_ref,
    wide_ref, roots_ref, scale_ref, field_ref, next_ref, second_ref, *, total_x,
):
    layers = strip_ref.shape[0] - 1
    shape = (24, 128)
    lane = lanes(shape)
    used = lane % SECOND < 2 * STRIP
    place = lane % SECOND % STRIP
    number = jnp.where(used, 2 * (lane // SECOND) + lane % SECOND // STRIP, -1)
    low = lane < SECOND

    geo = None
    odd = column_place_ref[0] % 2 == 1
    from_left = [jnp.where(odd, by_even_ref[g], by_odd_ref[g]) for g in range(2)]
    from_right = [jnp.where(odd, by_odd_ref[g], by_even_ref[g]) for g in range(2)]
    for layer in range(layers + 1):
        group, index = layer // GROUPED, layer % GROUPED
        strip = strip_ref[layer]
        strip = jnp.where(used & (place < 4), roll(from_left[group], -HALO * index, 1), strip)
        strip = jnp.where(used & (place >= 20), roll(from_right[group], 20 - HALO * index, 1), strip)
        if layer < layers:
            wide_ref[layer] = strip
        else:
            geo = strip

    def spread(to):
        result = jnp.zeros(shape, jnp.float32)
        for k in range(4):
            result = jnp.where(number == k, roll(geo, STARTS[k] - STARTS[to], 1), result)
        return result

    mask = spread(0)
    bare = 1.0 - mask
    friction = mask * jnp.where(low, roll(geo, -SECOND, 1), geo) + bare
    force_x, force_y = forces(mask, spread(1), row_place_ref[0] * 16, total_x)
    force = jnp.where(low, force_x, force_y)
    weight_i = jnp.where(low, MAIN_I[0], MAIN_I[1])
    weight_j = jnp.where(low, MAIN_J[0], MAIN_J[1])

    for z in range(layers):
        wide = wide_ref[z]
        slope_i = roll(wide, -1, 0) - roll(wide, 1, 0)
        slope_j = roll(wide, -1, 1) - roll(wide, 1, 1)
        rise = difference(lambda y: wide_ref[y], z, layers)
        rise = rise * rise
        stretch = jnp.where(low, slope_i, slope_j)
        shear = jnp.where(low, slope_j, slope_i)
        stretch_y = roll(stretch, SECOND, 1)
        shear = shear + roll(shear, SECOND, 1)
        strain = stretch * stretch + stretch_y * (stretch_y + stretch)
        strain = strain + 0.25 * (shear * shear + (rise + roll(rise, SECOND, 1)))
        roots_ref[z] = mask * jnp.exp(jnp.log(0.25 * strain + 0.1) * (-1.0 / 6.0))
    for z in range(layers):
        centre = with_neighbours(lambda y: roots_ref[y], z, layers)
        centre = centre + weight_i * around_i(centre)
        scale_ref[z] = centre + weight_j * around_j(centre)

    def put_residual(z, value):
        residual = force - value
        field_ref[z] = residual
        residual_ref[z] = residual[0:16]

    def put_image(z, value):
        next_ref[z] = value
        image_ref[z] = value[0:16]

    def put_second(z, value):
        second_ref[z] = value

    shared = (
        lambda z: roots_ref[z], lambda z: scale_ref[z], weight_i, weight_j, friction, bare, layers,
    )
    apply(lambda z: mask * wide_ref[z], put_residual, *shared)
    apply(lambda z: field_ref[z], put_image, *shared)
    apply(lambda z: next_ref[z], put_second, *shared, kept=16)
    totals = products(
        lambda z: field_ref[z], lambda z: next_ref[z], lambda z: second_ref[z], layers,
        [jnp.zeros((8, 128), jnp.float32)] * 4,
    )

    lane8 = lanes((8, 128))
    row8 = rows((8, 128))
    spot = lane8 % SECOND % STRIP
    edge = (lane8 % SECOND < 2 * STRIP) & (((spot >= 4) & (spot < 8)) | ((spot >= 16) & (spot < 20)))
    table = table_ref[...]
    for g in range(4):
        line = jnp.broadcast_to(jnp.sum(totals[g], axis=0, keepdims=True), (8, 128))
        for s in range(2):
            here = edge & (lane8 % SECOND // STRIP == s) & (row8 == 2 * g + s)
            table = table + jnp.where(here, line, 0.0)
    table = jnp.sum(table, axis=1, keepdims=True)
    line = jnp.sum(jnp.where(lane8 == row8, table, 0.0), axis=0, keepdims=True)
    gram_ref[...] = jnp.broadcast_to(line, gram_ref.shape)


def combine(
    gram_ref, residual_ref, image_ref, start_ref, side_residual_ref, side_image_ref, out_ref
):
    layers = start_ref.shape[1]
    shape = (8, 128)
    lane = lanes(shape)
    total = jnp.broadcast_to(jnp.sum(gram_ref[...], axis=0, keepdims=True), shape)
    ks, ms = [], []
    for s in range(2):
        rr, ra, aa, ab = (
            jnp.broadcast_to(total[:, q : q + 1], shape) for q in (s, 2 + s, 4 + s, 6 + s)
        )
        first = rr / ra
        norm_next = rr - 2.0 * first * ra + first * first * aa
        growth = 1.0 + norm_next / rr
        curve = growth * growth * ra - 2.0 * growth * first * aa + first * first * ab
        second = norm_next / curve
        ks.append(first + second * growth)
        ms.append(second * first)
    odd = lane % SECOND // STRIP == 1
    k_side = jnp.where(odd, ks[1], ks[0])
    m_side = jnp.where(odd, ms[1], ms[0])
    for z in range(layers):
        for t in range(2):
            at = slice(8 * t, 8 * t + 8)
            side = k_side * side_residual_ref[z, at] - m_side * side_image_ref[z, at]
            for c in range(2):
                step = ks[0] * residual_ref[2 * c, z, at] - ms[0] * image_ref[2 * c, z, at]
                step = step + ks[1] * residual_ref[2 * c + 1, z, at]
                step = step - ms[1] * image_ref[2 * c + 1, z, at]
                base = SECOND * c
                left = roll(side, -(base + 4), 1) + roll(side, -(base + STRIP + 4), 1)
                right = roll(side, 124 - base - 16, 1) + roll(side, 124 - base - STRIP - 16, 1)
                step = jnp.where(lane < HALO, left, step)
                step = jnp.where(lane >= 128 - HALO, right, step)
                out_ref[c, z, at] = start_ref[c, z, at] + step


def f32(*shape):
    return pltpu.VMEM(shape, jnp.float32)


def call(kernel, outs, ins, name, scratch=(), in_specs=None):
    specs = in_specs or [VMEM] * len(ins)
    ins = [
        pltpu.with_memory_space_constraint(x, pltpu.VMEM) if spec is VMEM else x
        for x, spec in zip(ins, specs)
    ]
    return pl.pallas_call(
        kernel,
        in_specs=specs,
        out_specs=[VMEM] * len(outs),
        out_shape=list(outs),
        scratch_shapes=list(scratch),
        name=name,
    )(*ins)


def swap_sides(by_odd, by_even, axis, other="ens"):
    count = lax.axis_size(axis)
    others = lax.axis_size(other) if other else 1

    def swap(message, first):
        pairs = []
        for o in range(others):
            for i in range((first + o) % 2, count - 1, 2):
                low, high = i * others + o, (i + 1) * others + o
                pairs += [(low, high), (high, low)]
        return lax.ppermute(message, (axis, other) if other else axis, pairs)

    return swap(by_odd, 1), swap(by_even, 0)


def body(u_prior, friction_rows, friction_table, bed_fixed, ice_mask):
    members, parts, layers, rows_x, rows_y = u_prior.shape
    total_x = rows_x * lax.axis_size("plane")
    row_place = lax.axis_index("plane").reshape(1)
    row_turn = row_place + lax.axis_index("ens")
    column_place = lax.axis_index("planey").reshape(1)
    by_odd, by_even, geo, u_near = call(
        pack_rows,
        [
            f32(layers + 1, 2, 8, rows_y),
            f32(layers + 1, 2, 8, rows_y),
            f32(4, rows_x, rows_y),
            f32(*u_prior.shape),
        ],
        [row_turn, friction_rows, u_prior, friction_table, bed_fixed, ice_mask],
        "pack_rows",
        scratch=[
            pltpu.SMEM(friction_rows.shape, jnp.int32),
            pltpu.VMEM(friction_table.shape, jnp.float32),
            pltpu.VMEM((2, rows_x, rows_y), jnp.int32),
            pltpu.SemaphoreType.DMA((5,)),
        ],
        in_specs=[SMEM] + [ANY] * 5,
    )
    by_odd, by_even = swap_sides(by_odd, by_even, "plane")
    own = call(
        pack_strips,
        [f32(layers + 1, rows_x, 128), f32(2, rows_x, 128), f32(2, rows_x, 128)],
        [column_place, u_near, geo],
        "pack_strips",
        in_specs=[SMEM, VMEM, VMEM],
    )
    outer, strip, side_odd, side_even = call(
        pack_columns,
        [f32(layers + 1, 4, 8, rows_y), f32(layers + 1, 24, 128), f32(2, 24, 128), f32(2, 24, 128)],
        [row_turn, column_place, *own, by_odd, by_even],
        "pack_columns",
        in_specs=[SMEM, SMEM] + [VMEM] * 5,
    )
    side_odd, side_even = swap_sides(side_odd, side_even, "planey", None)
    residual, image, start, table = call(
        lambda *refs: main_part(*refs, total_x=total_x),
        [
            f32(4, layers, rows_x, 128),
            f32(4, layers, rows_x, 128),
            f32(2, layers, rows_x, 128),
            f32(8, 128),
        ],
        [row_place, u_near, geo, outer],
        "main_part",
        scratch=[
            pltpu.VMEM((2, layers, 24, 128), jnp.float32),
            pltpu.VMEM((layers, 24, 128), jnp.float32),
            pltpu.VMEM((2, layers, 24, 128), jnp.float32),
            pltpu.VMEM((layers, 24, 128), jnp.float32),
            pltpu.VMEM((layers, 24, 128), jnp.float32),
            pltpu.VMEM((layers, 16, 128), jnp.float32),
        ],
        in_specs=[SMEM] + [VMEM] * 3,
    )
    side_residual, side_image, gram = call(
        lambda *refs: strip_part(*refs, total_x=total_x),
        [
            f32(layers, rows_x, 128),
            f32(layers, rows_x, 128),
            f32(lax.axis_size("plane") * lax.axis_size("planey"), 128),
        ],
        [row_place, column_place, strip, side_odd, side_even, table],
        "strip_part",
        scratch=[pltpu.VMEM((layers, 24, 128), jnp.float32)] * 5
        + [pltpu.VMEM((layers, 16, 128), jnp.float32)],
        in_specs=[SMEM, SMEM] + [VMEM] * 4,
    )
    gathered = lax.all_to_all(gram, ("plane", "planey"), 0, 0, tiled=True)
    (local_sum,) = call(
        combine, [f32(2, layers, rows_x, 128)], [gathered, residual, image, start, side_residual, side_image],
        "combine",

    )
    summed = lax.all_gather(local_sum, "ens").sum(axis=0)
    return summed / (members * lax.axis_size("ens"))


def solution(mesh):
    in_specs = (
        P(("group", "ens"), None, None, "plane", "planey"),
        P(("group", "ens")),
        P("group", "plane", "planey"),
        P("plane", "planey"),
        P("plane", "planey"),
    )
    out_specs = P("group", None, "plane", "planey")
    return jax.shard_map(body, mesh=mesh, in_specs=in_specs, out_specs=out_specs, check_vma=False)
```

```python
import jax
import jax.numpy as jnp
from jax import lax
from jax.experimental import pallas as pl
from jax.experimental.pallas import tpu as pltpu
from jax.sharding import PartitionSpec as P

bed_unit = 2.0 ** (-29)
HALO = 4
STRIP = 24
GROUPED = STRIP // HALO
MAIN_I = (0.25, 0.125)
MAIN_J = (0.125, 0.25)


VMEM = pl.BlockSpec(memory_space=pltpu.VMEM)
SMEM = pl.BlockSpec(memory_space=pltpu.SMEM)
ANY = pl.BlockSpec(memory_space=pl.ANY)


def roll(x, shift, axis):
    return pltpu.roll(x, shift % x.shape[axis], axis)


def lanes(shape):
    return lax.broadcasted_iota(jnp.int32, shape, len(shape) - 1)


def rows(shape):
    return lax.broadcasted_iota(jnp.int32, shape, len(shape) - 2)


def pack_rows(
    row_turn_ref, rows_hbm, u_hbm, table_hbm, bed_hbm, mask_hbm,
    odd_ref, even_ref, geo_ref, u_ref, rows_ref, table_ref, ints_ref, sems,
):
    layers = u_ref.shape[2]
    moves = [
        (u_hbm, u_ref),
        (rows_hbm, rows_ref),
        (table_hbm, table_ref),
        (mask_hbm, ints_ref.at[0]),
        (bed_hbm, ints_ref.at[1]),
    ]
    copies = [pltpu.make_async_copy(*move, sems.at[i]) for i, move in enumerate(moves)]
    for copy in copies:
        copy.start()
    for copy in copies:
        copy.wait()
    geo_ref[0] = ints_ref[0].astype(jnp.float32)
    geo_ref[1] = ints_ref[1].astype(jnp.float32) * bed_unit
    for s in range(2):
        geo_ref[2 + s] = table_ref[rows_ref[s]]
    low = rows((8, 128)) < HALO
    odd = row_turn_ref[0] % 2 == 1
    for layer in range(layers + 1):
        for pair in range(2):
            tiles = [
                u_ref[s, pair, layer] if layer < layers else geo_ref[2 * pair + s] for s in range(2)
            ]
            top = [tile[0:8] for tile in tiles]
            end = [tile[8:16] for tile in tiles]
            up = jnp.where(low, roll(end[0], HALO, 0), end[1])
            down = jnp.where(low, top[0], roll(top[1], HALO, 0))
            odd_ref[layer, pair] = jnp.where(odd, up, down)
            even_ref[layer, pair] = jnp.where(odd, down, up)


def strip_tile(tiles):
    lane = lanes((8, 128))
    strip = jnp.zeros((8, 128), jnp.float32)
    for k, tile in enumerate(tiles):
        at = lane - STRIP * k
        strip = jnp.where((at >= 4) & (at < 12), roll(tile, STRIP * k + 4, 1), strip)
        strip = jnp.where((at >= 12) & (at < 20), roll(tile, STRIP * k + 12 - 120, 1), strip)
    return strip


def side_messages(strip_of, layers, swapped):
    lane = lanes((8, 128))
    used = lane < 4 * STRIP
    slot = (lane % STRIP) // HALO
    for group in range(2):
        right = jnp.zeros((8, 128), jnp.float32)
        left = right
        for index in range(min(GROUPED, layers + 1 - GROUPED * group)):
            strip = strip_of(GROUPED * group + index)
            here = used & (slot == index)
            right = jnp.where(here, roll(strip, HALO * index - 16, 1), right)
            left = jnp.where(here, roll(strip, HALO * index - 4, 1), left)
        yield group, jnp.where(swapped, right, left), jnp.where(swapped, left, right)


def pack_strips(column_turn_ref, u_ref, geo_ref, own_ref, odd_ref, even_ref):
    layers = u_ref.shape[2]
    for layer in range(layers + 1):
        for t in range(2):
            at = slice(8 * t, 8 * t + 8)
            own_ref[layer, at] = strip_tile(
                [u_ref[k % 2, k // 2, layer, at] if layer < layers else geo_ref[k, at] for k in range(4)]
            )
    swapped = column_turn_ref[0] % 2 == 1

    def send(t, carry):
        at = pl.ds(pl.multiple_of(8 * t, 8), 8)
        for group, by_odd, by_even in side_messages(lambda layer: own_ref[layer, at], layers, swapped):
            odd_ref[group, at] = by_odd
            even_ref[group, at] = by_even
        return carry

    lax.fori_loop(0, 2, send, 0)


def pack_columns(
    row_turn_ref, column_turn_ref, own_ref, own_odd_ref, own_even_ref, by_odd_ref, by_even_ref,
    outer_ref, strip_ref, odd_ref, even_ref,
):
    layers = own_ref.shape[0] - 1
    low = rows((8, 128)) < HALO
    odd = row_turn_ref[0] % 2 == 1
    for layer in range(layers + 1):
        outer = []
        for pair in range(2):
            by_odd = by_odd_ref[layer, pair]
            by_even = by_even_ref[layer, pair]
            below = jnp.where(odd, by_even, by_odd)
            above = jnp.where(odd, by_odd, by_even)
            outer.append(jnp.where(low, above, roll(below, HALO, 0)))
            outer.append(jnp.where(low, roll(above, HALO, 0), below))
        for k in range(4):
            outer_ref[layer, k] = outer[k]
        strip_ref[layer, 0:16] = own_ref[layer]
        strip_ref[layer, 16:24] = strip_tile(outer)
    for group in range(2):
        odd_ref[group, 0:16] = own_odd_ref[group]
        even_ref[group, 0:16] = own_even_ref[group]
    swapped = column_turn_ref[0] % 2 == 1

    for group, by_odd, by_even in side_messages(lambda layer: strip_ref[layer, 16:24], layers, swapped):
        odd_ref[group, 16:24] = by_odd
        even_ref[group, 16:24] = by_even


def around_i(x):
    return roll(x, 1, 0) + roll(x, -1, 0)


def around_j(x):
    return roll(x, 1, 1) + roll(x, -1, 1)


def forces(cover, ground, row_start, total_x):
    row = rows(cover.shape)
    position = (jnp.where(row < 20, row, row - 24) + row_start).astype(jnp.float32)
    thickness = 1.0 + 2.0 * position / (total_x - 1)
    slope_x = (roll(ground, -1, 0) - roll(ground, 1, 0)) * 0.5
    slope_y = (roll(ground, -1, 1) - roll(ground, 1, 1)) * 0.5
    return -(cover * thickness * slope_x), -(cover * thickness * slope_y)


def difference(get, z, layers):
    if z == 0:
        return get(1)
    if z + 1 == layers:
        return -get(z - 1)
    return get(z + 1) - get(z - 1)


def viscosity(get_u, get_v, z, layers, cover):
    u, v = get_u(z), get_v(z)
    stretch_x = roll(u, -1, 0) - roll(u, 1, 0)
    stretch_y = roll(v, -1, 1) - roll(v, 1, 1)
    shear = (roll(u, -1, 1) - roll(u, 1, 1)) + (roll(v, -1, 0) - roll(v, 1, 0))
    rise_u = difference(get_u, z, layers)
    rise_v = difference(get_v, z, layers)
    strain = stretch_x * stretch_x + stretch_y * (stretch_y + stretch_x)
    strain = strain + 0.25 * (shear * shear + (rise_u * rise_u + rise_v * rise_v))
    return cover * jnp.exp(jnp.log(0.25 * strain + 0.1) * (-1.0 / 6.0))


def with_neighbours(get, z, layers):
    if z == 0:
        return get(0) + 0.5 * get(1)
    if z + 1 == layers:
        return get(z) + 0.5 * get(z - 1)
    return get(z) + 0.5 * (get(z - 1) + get(z + 1))


def apply(get, put, roots, scale, weight_i, weight_j, friction, empty, layers, kept=24):
    def kept_rows(x):
        return x[0:kept] if x.ndim else x

    def filtered(z):
        product = roots(z) * get(z)
        product = (product + weight_i * around_i(product))[0:kept]
        return product + kept_rows(weight_j) * around_j(product)

    done = {}
    for z in range(layers + 1):
        if z < layers:
            done[z] = filtered(z)
        if z > 0:
            at = z - 1
            total = with_neighbours(lambda y: done[y], at, layers)
            field = get(at)[0:kept]
            result = 4.0 * roots(at)[0:kept] * (scale(at)[0:kept] * field - total)
            put(at, result + (friction if at == 0 else empty)[0:kept] * field)


def products(field, image, second, layers, totals):
    totals = list(totals)
    for z in range(layers):
        for t in range(2):
            at = slice(8 * t, 8 * t + 8)
            r, a, b = field(z)[at], image(z)[at], second(z)[at]
            for i, (x, y) in enumerate(((r, r), (r, a), (a, a), (a, b))):
                totals[i] = totals[i] + x * y
    return totals


def main_part(
    row_place_ref, u_ref, geo_ref, outer_ref,
    residual_ref, image_ref, start_ref, table_ref,
    wide_ref, roots_ref, scale_ref, field_ref, next_ref, second_ref, *, total_x,
):
    layers = u_ref.shape[2]
    row_start = row_place_ref[0] * 16

    def geo(k):
        return jnp.concatenate([geo_ref[k], outer_ref[layers, k]], axis=0)

    mask = geo(0)
    bare = 1.0 - mask
    force = forces(mask, geo(1), row_start, total_x)
    lane8 = lanes((8, 128))
    inside = (lane8 >= HALO) & (lane8 < 128 - HALO)
    row8 = rows((8, 128))
    table_ref[...] = jnp.zeros((8, 128), jnp.float32)

    def sample(s, carry):
        friction = mask * jnp.concatenate([geo_ref[2 + s], outer_ref[layers, 2 + s]], axis=0) + bare
        for c in range(2):
            for z in range(layers):
                wide_ref[c, z, 0:16] = u_ref[s, c, z]
                wide_ref[c, z, 16:24] = outer_ref[z, 2 * c + s]
        for z in range(layers):
            roots_ref[z] = viscosity(
                lambda y: wide_ref[0, y], lambda y: wide_ref[1, y], z, layers, mask
            )
        for z in range(layers):
            centre = with_neighbours(lambda y: roots_ref[y], z, layers)
            along_i = around_i(centre)
            along_j = around_j(centre)
            both = centre + 0.03125 * around_j(along_i)
            for c in range(2):
                scale_ref[c, z] = both + MAIN_I[c] * along_i + MAIN_J[c] * along_j

        def component(c, carry):
            first = c == 0
            weight_i = jnp.where(first, MAIN_I[0], MAIN_I[1])
            weight_j = jnp.where(first, MAIN_J[0], MAIN_J[1])
            pull = jnp.where(first, force[0], force[1])
            shared = (
                lambda z: roots_ref[z], lambda z: scale_ref[c, z],
                weight_i, weight_j, friction, bare, layers,
            )

            def put_residual(z, value):
                residual = pull - value
                field_ref[z] = residual
                residual_ref[2 * c + s, z] = residual[0:16]

            def put_image(z, value):
                next_ref[z] = value
                image_ref[2 * c + s, z] = value[0:16]

            def put_second(z, value):
                second_ref[z] = value

            apply(lambda z: mask * wide_ref[c, z], put_residual, *shared)
            apply(lambda z: field_ref[z], put_image, *shared)
            apply(lambda z: next_ref[z], put_second, *shared, kept=16)
            totals = products(
                lambda z: field_ref[z], lambda z: next_ref[z], lambda z: second_ref[z], layers,
                [jnp.zeros((8, 128), jnp.float32)] * 4,
            )
            for g in range(4):
                line = jnp.sum(jnp.where(inside, totals[g], 0.0), axis=0, keepdims=True)
                table_ref[...] += jnp.where(row8 == 2 * g + s, line, 0.0)
            return carry

        return lax.fori_loop(0, 2, component, carry)

    lax.fori_loop(0, 2, sample, 0)
    for c in range(2):
        for z in range(layers):
            start_ref[c, z] = mask[0:16] * u_ref[0, c, z] + mask[0:16] * u_ref[1, c, z]


def strip_part(
    row_place_ref, column_turn_ref, strip_ref, by_odd_ref, by_even_ref, table_ref,
    residual_ref, image_ref, gram_ref,
    wide_ref, roots_ref, scale_ref, field_ref, next_ref, second_ref, *, total_x,
):
    layers = strip_ref.shape[0] - 1
    shape = (24, 128)
    lane = lanes(shape)
    used = lane < 4 * STRIP
    place = lane % STRIP
    number = lane // STRIP
    low = lane < 2 * STRIP

    geo = None
    odd = column_turn_ref[0] % 2 == 1
    from_left = [jnp.where(odd, by_even_ref[g], by_odd_ref[g]) for g in range(2)]
    from_right = [jnp.where(odd, by_odd_ref[g], by_even_ref[g]) for g in range(2)]
    for layer in range(layers + 1):
        group, index = layer // GROUPED, layer % GROUPED
        strip = strip_ref[layer]
        strip = jnp.where(used & (place < 4), roll(from_left[group], -HALO * index, 1), strip)
        strip = jnp.where(used & (place >= 20), roll(from_right[group], 20 - HALO * index, 1), strip)
        if layer < layers:
            wide_ref[layer] = strip
        else:
            geo = strip

    def spread(to):
        result = jnp.zeros(shape, jnp.float32)
        for k in range(4):
            result = jnp.where(number == k, roll(geo, STRIP * (k - to), 1), result)
        return result

    mask = spread(0)
    bare = 1.0 - mask
    friction = mask * jnp.where(low, roll(geo, -2 * STRIP, 1), geo) + bare
    force_x, force_y = forces(mask, spread(1), row_place_ref[0] * 16, total_x)
    force = jnp.where(low, force_x, force_y)
    weight_i = jnp.where(low, MAIN_I[0], MAIN_I[1])
    weight_j = jnp.where(low, MAIN_J[0], MAIN_J[1])

    for z in range(layers):
        wide = wide_ref[z]
        slope_i = roll(wide, -1, 0) - roll(wide, 1, 0)
        slope_j = roll(wide, -1, 1) - roll(wide, 1, 1)
        rise = difference(lambda y: wide_ref[y], z, layers)
        rise = rise * rise
        stretch = jnp.where(low, slope_i, slope_j)
        shear = jnp.where(low, slope_j, slope_i)
        stretch_y = roll(stretch, -2 * STRIP, 1)
        shear = shear + roll(shear, -2 * STRIP, 1)
        strain = stretch * stretch + stretch_y * (stretch_y + stretch)
        strain = strain + 0.25 * (shear * shear + (rise + roll(rise, -2 * STRIP, 1)))
        found = mask * jnp.exp(jnp.log(0.25 * strain + 0.1) * (-1.0 / 6.0))
        roots_ref[z] = jnp.where(low, found, roll(found, 2 * STRIP, 1))
    for z in range(layers):
        centre = with_neighbours(lambda y: roots_ref[y], z, layers)
        centre = centre + weight_i * around_i(centre)
        scale_ref[z] = centre + weight_j * around_j(centre)

    def put_residual(z, value):
        residual = force - value
        field_ref[z] = residual
        residual_ref[z] = residual[0:16]

    def put_image(z, value):
        next_ref[z] = value
        image_ref[z] = value[0:16]

    def put_second(z, value):
        second_ref[z] = value

    shared = (
        lambda z: roots_ref[z], lambda z: scale_ref[z], weight_i, weight_j, friction, bare, layers,
    )
    apply(lambda z: mask * wide_ref[z], put_residual, *shared)
    apply(lambda z: field_ref[z], put_image, *shared)
    apply(lambda z: next_ref[z], put_second, *shared, kept=16)
    totals = products(
        lambda z: field_ref[z], lambda z: next_ref[z], lambda z: second_ref[z], layers,
        [jnp.zeros((8, 128), jnp.float32)] * 4,
    )

    lane8 = lanes((8, 128))
    row8 = rows((8, 128))
    spot = lane8 % STRIP
    edge = (lane8 < 4 * STRIP) & (((spot >= 4) & (spot < 8)) | ((spot >= 16) & (spot < 20)))
    table = table_ref[...]
    for g in range(4):
        line = jnp.broadcast_to(jnp.sum(totals[g], axis=0, keepdims=True), (8, 128))
        for s in range(2):
            here = edge & ((lane8 // STRIP) % 2 == s) & (row8 == 2 * g + s)
            table = table + jnp.where(here, line, 0.0)
    table = jnp.sum(table, axis=1, keepdims=True)
    line = jnp.sum(jnp.where(lane8 == row8, table, 0.0), axis=0, keepdims=True)
    gram_ref[...] = jnp.broadcast_to(line, gram_ref.shape)


def combine(
    gram_ref, residual_ref, image_ref, start_ref, side_residual_ref, side_image_ref, out_ref
):
    layers = start_ref.shape[1]
    shape = (8, 128)
    lane = lanes(shape)
    total = jnp.broadcast_to(jnp.sum(gram_ref[...], axis=0, keepdims=True), shape)
    ks, ms = [], []
    for s in range(2):
        rr, ra, aa, ab = (
            jnp.broadcast_to(total[:, q : q + 1], shape) for q in (s, 2 + s, 4 + s, 6 + s)
        )
        first = rr / ra
        norm_next = rr - 2.0 * first * ra + first * first * aa
        growth = 1.0 + norm_next / rr
        curve = growth * growth * ra - 2.0 * growth * first * aa + first * first * ab
        second = norm_next / curve
        ks.append(first + second * growth)
        ms.append(second * first)
    odd = (lane // STRIP) % 2 == 1
    k_side = jnp.where(odd, ks[1], ks[0])
    m_side = jnp.where(odd, ms[1], ms[0])
    for z in range(layers):
        for t in range(2):
            at = slice(8 * t, 8 * t + 8)
            side = k_side * side_residual_ref[z, at] - m_side * side_image_ref[z, at]
            for c in range(2):
                step = ks[0] * residual_ref[2 * c, z, at] - ms[0] * image_ref[2 * c, z, at]
                step = step + ks[1] * residual_ref[2 * c + 1, z, at]
                step = step - ms[1] * image_ref[2 * c + 1, z, at]
                base = 2 * STRIP * c
                left = roll(side, -(base + 4), 1) + roll(side, -(base + STRIP + 4), 1)
                right = roll(side, 124 - base - 16, 1) + roll(side, 124 - base - STRIP - 16, 1)
                step = jnp.where(lane < HALO, left, step)
                step = jnp.where(lane >= 128 - HALO, right, step)
                out_ref[c, z, at] = start_ref[c, z, at] + step


def f32(*shape):
    return pltpu.VMEM(shape, jnp.float32)


def call(kernel, outs, ins, name, scratch=(), in_specs=None):
    specs = in_specs or [VMEM] * len(ins)
    ins = [
        pltpu.with_memory_space_constraint(x, pltpu.VMEM) if spec is VMEM else x
        for x, spec in zip(ins, specs)
    ]
    return pl.pallas_call(
        kernel,
        in_specs=specs,
        out_specs=[VMEM] * len(outs),
        out_shape=list(outs),
        scratch_shapes=list(scratch),
        name=name,
    )(*ins)


def swap_sides(by_odd, by_even, axis, other="ens"):
    count = lax.axis_size(axis)
    others = lax.axis_size(other) if other else 1

    def swap(message, first):
        pairs = []
        for o in range(others):
            for i in range((first + o) % 2, count - 1, 2):
                low, high = i * others + o, (i + 1) * others + o
                pairs += [(low, high), (high, low)]
        return lax.ppermute(message, (axis, other) if other else axis, pairs)

    return swap(by_odd, 1), swap(by_even, 0)


def body(u_prior, friction_rows, friction_table, bed_fixed, ice_mask):
    members, parts, layers, rows_x, rows_y = u_prior.shape
    total_x = rows_x * lax.axis_size("plane")
    row_place = lax.axis_index("plane").reshape(1)
    row_turn = row_place + lax.axis_index("ens")
    column_turn = (lax.axis_index("planey") + lax.axis_index("ens")).reshape(1)
    by_odd, by_even, geo, u_near = call(
        pack_rows,
        [
            f32(layers + 1, 2, 8, rows_y),
            f32(layers + 1, 2, 8, rows_y),
            f32(4, rows_x, rows_y),
            f32(*u_prior.shape),
        ],
        [row_turn, friction_rows, u_prior, friction_table, bed_fixed, ice_mask],
        "pack_rows",
        scratch=[
            pltpu.SMEM(friction_rows.shape, jnp.int32),
            pltpu.VMEM(friction_table.shape, jnp.float32),
            pltpu.VMEM((2, rows_x, rows_y), jnp.int32),
            pltpu.SemaphoreType.DMA((5,)),
        ],
        in_specs=[SMEM] + [ANY] * 5,
    )
    by_odd, by_even = swap_sides(by_odd, by_even, "plane")
    own = call(
        pack_strips,
        [f32(layers + 1, rows_x, 128), f32(2, rows_x, 128), f32(2, rows_x, 128)],
        [column_turn, u_near, geo],
        "pack_strips",
        in_specs=[SMEM, VMEM, VMEM],
    )
    outer, strip, side_odd, side_even = call(
        pack_columns,
        [f32(layers + 1, 4, 8, rows_y), f32(layers + 1, 24, 128), f32(2, 24, 128), f32(2, 24, 128)],
        [row_turn, column_turn, *own, by_odd, by_even],
        "pack_columns",
        in_specs=[SMEM, SMEM] + [VMEM] * 5,
    )
    side_odd, side_even = swap_sides(side_odd, side_even, "planey")
    residual, image, start, table = call(
        lambda *refs: main_part(*refs, total_x=total_x),
        [
            f32(4, layers, rows_x, 128),
            f32(4, layers, rows_x, 128),
            f32(2, layers, rows_x, 128),
            f32(8, 128),
        ],
        [row_place, u_near, geo, outer],
        "main_part",
        scratch=[
            pltpu.VMEM((2, layers, 24, 128), jnp.float32),
            pltpu.VMEM((layers, 24, 128), jnp.float32),
            pltpu.VMEM((2, layers, 24, 128), jnp.float32),
            pltpu.VMEM((layers, 24, 128), jnp.float32),
            pltpu.VMEM((layers, 24, 128), jnp.float32),
            pltpu.VMEM((layers, 16, 128), jnp.float32),
        ],
        in_specs=[SMEM] + [VMEM] * 3,
    )
    side_residual, side_image, gram = call(
        lambda *refs: strip_part(*refs, total_x=total_x),
        [
            f32(layers, rows_x, 128),
            f32(layers, rows_x, 128),
            f32(lax.axis_size("plane") * lax.axis_size("planey"), 128),
        ],
        [row_place, column_turn, strip, side_odd, side_even, table],
        "strip_part",
        scratch=[pltpu.VMEM((layers, 24, 128), jnp.float32)] * 5
        + [pltpu.VMEM((layers, 16, 128), jnp.float32)],
        in_specs=[SMEM, SMEM] + [VMEM] * 4,
    )
    gathered = lax.all_to_all(gram, ("plane", "planey"), 0, 0, tiled=True)
    (local_sum,) = call(
        combine, [f32(2, layers, rows_x, 128)], [gathered, residual, image, start, side_residual, side_image],
        "combine",

    )
    summed = lax.all_gather(local_sum, "ens").sum(axis=0)
    return summed / (members * lax.axis_size("ens"))


def solution(mesh):
    in_specs = (
        P(("group", "ens"), None, None, "plane", "planey"),
        P(("group", "ens")),
        P("group", "plane", "planey"),
        P("plane", "planey"),
        P("plane", "planey"),
    )
    out_specs = P("group", None, "plane", "planey")
    return jax.shard_map(body, mesh=mesh, in_specs=in_specs, out_specs=out_specs, check_vma=False)
```

```python
import jax
import jax.numpy as jnp
from jax import lax
from jax.experimental import pallas as pl
from jax.experimental.pallas import tpu as pltpu
from jax.sharding import PartitionSpec as P

bed_unit = 2.0 ** (-29)
HALO = 4
STRIP = 24
GROUPED = STRIP // HALO
SECOND = 64
STARTS = (0, STRIP, SECOND, SECOND + STRIP)
MAIN_I = (0.25, 0.125)
MAIN_J = (0.125, 0.25)


VMEM = pl.BlockSpec(memory_space=pltpu.VMEM)
SMEM = pl.BlockSpec(memory_space=pltpu.SMEM)
ANY = pl.BlockSpec(memory_space=pl.ANY)


def roll(x, shift, axis):
    return pltpu.roll(x, shift % x.shape[axis], axis)


def lanes(shape):
    return lax.broadcasted_iota(jnp.int32, shape, len(shape) - 1)


def rows(shape):
    return lax.broadcasted_iota(jnp.int32, shape, len(shape) - 2)


def pack_rows(
    row_turn_ref, rows_hbm, u_hbm, table_hbm, bed_hbm, mask_hbm,
    odd_ref, even_ref, geo_ref, u_ref, rows_ref, table_ref, ints_ref, sems,
):
    layers = u_ref.shape[2]
    moves = [
        (u_hbm, u_ref),
        (rows_hbm, rows_ref),
        (table_hbm, table_ref),
        (mask_hbm, ints_ref.at[0]),
        (bed_hbm, ints_ref.at[1]),
    ]
    copies = [pltpu.make_async_copy(*move, sems.at[i]) for i, move in enumerate(moves)]
    for copy in copies:
        copy.start()
    for copy in copies:
        copy.wait()
    geo_ref[0] = ints_ref[0].astype(jnp.float32)
    geo_ref[1] = ints_ref[1].astype(jnp.float32) * bed_unit
    for s in range(2):
        geo_ref[2 + s] = table_ref[rows_ref[s]]
    low = rows((8, 128)) < HALO
    odd = row_turn_ref[0] % 2 == 1
    for layer in range(layers + 1):
        for pair in range(2):
            tiles = [
                u_ref[s, pair, layer] if layer < layers else geo_ref[2 * pair + s] for s in range(2)
            ]
            top = [tile[0:8] for tile in tiles]
            end = [tile[8:16] for tile in tiles]
            up = jnp.where(low, roll(end[0], HALO, 0), end[1])
            down = jnp.where(low, top[0], roll(top[1], HALO, 0))
            odd_ref[layer, pair] = jnp.where(odd, up, down)
            even_ref[layer, pair] = jnp.where(odd, down, up)


def strip_tile(tiles):
    lane = lanes((8, 128))
    strip = jnp.zeros((8, 128), jnp.float32)
    for k, tile in enumerate(tiles):
        at = lane - STARTS[k]
        strip = jnp.where((at >= 4) & (at < 12), roll(tile, STARTS[k] + 4, 1), strip)
        strip = jnp.where((at >= 12) & (at < 20), roll(tile, STARTS[k] + 12 - 120, 1), strip)
    return strip


def side_messages(strip_of, layers, swapped):
    lane = lanes((8, 128))
    used = lane % SECOND < 2 * STRIP
    slot = (lane % SECOND % STRIP) // HALO
    for group in range(2):
        right = jnp.zeros((8, 128), jnp.float32)
        left = right
        for index in range(min(GROUPED, layers + 1 - GROUPED * group)):
            strip = strip_of(GROUPED * group + index)
            here = used & (slot == index)
            right = jnp.where(here, roll(strip, HALO * index - 16, 1), right)
            left = jnp.where(here, roll(strip, HALO * index - 4, 1), left)
        yield group, jnp.where(swapped, right, left), jnp.where(swapped, left, right)


def pack_strips(column_turn_ref, u_ref, geo_ref, own_ref, odd_ref, even_ref):
    layers = u_ref.shape[2]
    for layer in range(layers + 1):
        for t in range(2):
            at = slice(8 * t, 8 * t + 8)
            own_ref[layer, at] = strip_tile(
                [u_ref[k % 2, k // 2, layer, at] if layer < layers else geo_ref[k, at] for k in range(4)]
            )
    swapped = column_turn_ref[0] % 2 == 1

    def send(t, carry):
        at = pl.ds(pl.multiple_of(8 * t, 8), 8)
        for group, by_odd, by_even in side_messages(lambda layer: own_ref[layer, at], layers, swapped):
            odd_ref[group, at] = by_odd
            even_ref[group, at] = by_even
        return carry

    lax.fori_loop(0, 2, send, 0)


def pack_columns(
    row_turn_ref, column_turn_ref, own_ref, own_odd_ref, own_even_ref, by_odd_ref, by_even_ref,
    outer_ref, strip_ref, odd_ref, even_ref,
):
    layers = own_ref.shape[0] - 1
    low = rows((8, 128)) < HALO
    odd = row_turn_ref[0] % 2 == 1
    for layer in range(layers + 1):
        outer = []
        for pair in range(2):
            by_odd = by_odd_ref[layer, pair]
            by_even = by_even_ref[layer, pair]
            below = jnp.where(odd, by_even, by_odd)
            above = jnp.where(odd, by_odd, by_even)
            outer.append(jnp.where(low, above, roll(below, HALO, 0)))
            outer.append(jnp.where(low, roll(above, HALO, 0), below))
        for k in range(4):
            outer_ref[layer, k] = outer[k]
        strip_ref[layer, 0:16] = own_ref[layer]
        strip_ref[layer, 16:24] = strip_tile(outer)
    for group in range(2):
        odd_ref[group, 0:16] = own_odd_ref[group]
        even_ref[group, 0:16] = own_even_ref[group]
    swapped = column_turn_ref[0] % 2 == 1

    for group, by_odd, by_even in side_messages(lambda layer: strip_ref[layer, 16:24], layers, swapped):
        odd_ref[group, 16:24] = by_odd
        even_ref[group, 16:24] = by_even


def around_i(x):
    return roll(x, 1, 0) + roll(x, -1, 0)


def around_j(x):
    return roll(x, 1, 1) + roll(x, -1, 1)


def forces(cover, ground, row_start, total_x):
    row = rows(cover.shape)
    position = (jnp.where(row < 20, row, row - 24) + row_start).astype(jnp.float32)
    thickness = 1.0 + 2.0 * position / (total_x - 1)
    slope_x = (roll(ground, -1, 0) - roll(ground, 1, 0)) * 0.5
    slope_y = (roll(ground, -1, 1) - roll(ground, 1, 1)) * 0.5
    return -(cover * thickness * slope_x), -(cover * thickness * slope_y)


def difference(get, z, layers):
    if z == 0:
        return get(1)
    if z + 1 == layers:
        return -get(z - 1)
    return get(z + 1) - get(z - 1)


def viscosity(get_u, get_v, z, layers, cover):
    u, v = get_u(z), get_v(z)
    stretch_x = roll(u, -1, 0) - roll(u, 1, 0)
    stretch_y = roll(v, -1, 1) - roll(v, 1, 1)
    shear = (roll(u, -1, 1) - roll(u, 1, 1)) + (roll(v, -1, 0) - roll(v, 1, 0))
    rise_u = difference(get_u, z, layers)
    rise_v = difference(get_v, z, layers)
    strain = stretch_x * stretch_x + stretch_y * (stretch_y + stretch_x)
    strain = strain + 0.25 * (shear * shear + (rise_u * rise_u + rise_v * rise_v))
    return cover * jnp.exp(jnp.log(0.25 * strain + 0.1) * (-1.0 / 6.0))


def with_neighbours(get, z, layers):
    if z == 0:
        return get(0) + 0.5 * get(1)
    if z + 1 == layers:
        return get(z) + 0.5 * get(z - 1)
    return get(z) + 0.5 * (get(z - 1) + get(z + 1))


def apply(get, put, roots, scale, weight_i, weight_j, friction, empty, layers, kept=24):
    def kept_rows(x):
        return x[0:kept] if x.ndim else x

    def filtered(z):
        product = roots(z) * get(z)
        product = (product + weight_i * around_i(product))[0:kept]
        return product + kept_rows(weight_j) * around_j(product)

    done = {}
    for z in range(layers + 1):
        if z < layers:
            done[z] = filtered(z)
        if z > 0:
            at = z - 1
            total = with_neighbours(lambda y: done[y], at, layers)
            field = get(at)[0:kept]
            result = 4.0 * roots(at)[0:kept] * (scale(at)[0:kept] * field - total)
            put(at, result + (friction if at == 0 else empty)[0:kept] * field)


def products(field, image, second, layers, totals):
    totals = list(totals)
    for z in range(layers):
        for t in range(2):
            at = slice(8 * t, 8 * t + 8)
            r, a, b = field(z)[at], image(z)[at], second(z)[at]
            for i, (x, y) in enumerate(((r, r), (r, a), (a, a), (a, b))):
                totals[i] = totals[i] + x * y
    return totals


def main_part(
    row_place_ref, u_ref, geo_ref, outer_ref,
    residual_ref, image_ref, start_ref, table_ref,
    wide_ref, roots_ref, scale_ref, field_ref, next_ref, second_ref, *, total_x,
):
    layers = u_ref.shape[2]
    row_start = row_place_ref[0] * 16

    def geo(k):
        return jnp.concatenate([geo_ref[k], outer_ref[layers, k]], axis=0)

    mask = geo(0)
    bare = 1.0 - mask
    force = forces(mask, geo(1), row_start, total_x)
    lane8 = lanes((8, 128))
    inside = (lane8 >= HALO) & (lane8 < 128 - HALO)
    row8 = rows((8, 128))
    table_ref[...] = jnp.zeros((8, 128), jnp.float32)

    def sample(s, carry):
        friction = mask * jnp.concatenate([geo_ref[2 + s], outer_ref[layers, 2 + s]], axis=0) + bare
        for c in range(2):
            for z in range(layers):
                wide_ref[c, z, 0:16] = u_ref[s, c, z]
                wide_ref[c, z, 16:24] = outer_ref[z, 2 * c + s]
        for z in range(layers):
            roots_ref[z] = viscosity(
                lambda y: wide_ref[0, y], lambda y: wide_ref[1, y], z, layers, mask
            )
        for z in range(layers):
            centre = with_neighbours(lambda y: roots_ref[y], z, layers)
            along_i = around_i(centre)
            along_j = around_j(centre)
            both = centre + 0.03125 * around_j(along_i)
            for c in range(2):
                scale_ref[c, z] = both + MAIN_I[c] * along_i + MAIN_J[c] * along_j

        def component(c, carry):
            first = c == 0
            weight_i = jnp.where(first, MAIN_I[0], MAIN_I[1])
            weight_j = jnp.where(first, MAIN_J[0], MAIN_J[1])
            pull = jnp.where(first, force[0], force[1])
            shared = (
                lambda z: roots_ref[z], lambda z: scale_ref[c, z],
                weight_i, weight_j, friction, bare, layers,
            )

            def put_residual(z, value):
                residual = pull - value
                field_ref[z] = residual
                residual_ref[2 * c + s, z] = residual[0:16]

            def put_image(z, value):
                next_ref[z] = value
                image_ref[2 * c + s, z] = value[0:16]

            def put_second(z, value):
                second_ref[z] = value

            apply(lambda z: mask * wide_ref[c, z], put_residual, *shared)
            apply(lambda z: field_ref[z], put_image, *shared)
            apply(lambda z: next_ref[z], put_second, *shared, kept=16)
            totals = products(
                lambda z: field_ref[z], lambda z: next_ref[z], lambda z: second_ref[z], layers,
                [jnp.zeros((8, 128), jnp.float32)] * 4,
            )
            for g in range(4):
                line = jnp.sum(jnp.where(inside, totals[g], 0.0), axis=0, keepdims=True)
                table_ref[...] += jnp.where(row8 == 2 * g + s, line, 0.0)
            return carry

        return lax.fori_loop(0, 2, component, carry)

    lax.fori_loop(0, 2, sample, 0)
    for c in range(2):
        for z in range(layers):
            start_ref[c, z] = mask[0:16] * u_ref[0, c, z] + mask[0:16] * u_ref[1, c, z]


def strip_part(
    row_place_ref, column_turn_ref, strip_ref, by_odd_ref, by_even_ref, table_ref,
    residual_ref, image_ref, gram_ref,
    wide_ref, roots_ref, scale_ref, field_ref, next_ref, second_ref, *, total_x,
):
    layers = strip_ref.shape[0] - 1
    shape = (24, 128)
    lane = lanes(shape)
    used = lane % SECOND < 2 * STRIP
    place = lane % SECOND % STRIP
    number = jnp.where(used, 2 * (lane // SECOND) + lane % SECOND // STRIP, -1)
    low = lane < SECOND

    geo = None
    odd = column_turn_ref[0] % 2 == 1
    from_left = [jnp.where(odd, by_even_ref[g], by_odd_ref[g]) for g in range(2)]
    from_right = [jnp.where(odd, by_odd_ref[g], by_even_ref[g]) for g in range(2)]
    for layer in range(layers + 1):
        group, index = layer // GROUPED, layer % GROUPED
        strip = strip_ref[layer]
        strip = jnp.where(used & (place < 4), roll(from_left[group], -HALO * index, 1), strip)
        strip = jnp.where(used & (place >= 20), roll(from_right[group], 20 - HALO * index, 1), strip)
        if layer < layers:
            wide_ref[layer] = strip
        else:
            geo = strip

    def spread(to):
        result = jnp.zeros(shape, jnp.float32)
        for k in range(4):
            result = jnp.where(number == k, roll(geo, STARTS[k] - STARTS[to], 1), result)
        return result

    mask = spread(0)
    bare = 1.0 - mask
    friction = mask * jnp.where(low, roll(geo, -SECOND, 1), geo) + bare
    force_x, force_y = forces(mask, spread(1), row_place_ref[0] * 16, total_x)
    force = jnp.where(low, force_x, force_y)
    weight_i = jnp.where(low, MAIN_I[0], MAIN_I[1])
    weight_j = jnp.where(low, MAIN_J[0], MAIN_J[1])

    for z in range(layers):
        wide = wide_ref[z]
        slope_i = roll(wide, -1, 0) - roll(wide, 1, 0)
        slope_j = roll(wide, -1, 1) - roll(wide, 1, 1)
        rise = difference(lambda y: wide_ref[y], z, layers)
        rise = rise * rise
        stretch = jnp.where(low, slope_i, slope_j)
        shear = jnp.where(low, slope_j, slope_i)
        stretch_y = roll(stretch, SECOND, 1)
        shear = shear + roll(shear, SECOND, 1)
        strain = stretch * stretch + stretch_y * (stretch_y + stretch)
        strain = strain + 0.25 * (shear * shear + (rise + roll(rise, SECOND, 1)))
        roots_ref[z] = mask * jnp.exp(jnp.log(0.25 * strain + 0.1) * (-1.0 / 6.0))
    for z in range(layers):
        centre = with_neighbours(lambda y: roots_ref[y], z, layers)
        centre = centre + weight_i * around_i(centre)
        scale_ref[z] = centre + weight_j * around_j(centre)

    def put_residual(z, value):
        residual = force - value
        field_ref[z] = residual
        residual_ref[z] = residual[0:16]

    def put_image(z, value):
        next_ref[z] = value
        image_ref[z] = value[0:16]

    def put_second(z, value):
        second_ref[z] = value

    shared = (
        lambda z: roots_ref[z], lambda z: scale_ref[z], weight_i, weight_j, friction, bare, layers,
    )
    apply(lambda z: mask * wide_ref[z], put_residual, *shared)
    apply(lambda z: field_ref[z], put_image, *shared)
    apply(lambda z: next_ref[z], put_second, *shared, kept=16)
    totals = products(
        lambda z: field_ref[z], lambda z: next_ref[z], lambda z: second_ref[z], layers,
        [jnp.zeros((8, 128), jnp.float32)] * 4,
    )

    lane8 = lanes((8, 128))
    row8 = rows((8, 128))
    spot = lane8 % SECOND % STRIP
    edge = (lane8 % SECOND < 2 * STRIP) & (((spot >= 4) & (spot < 8)) | ((spot >= 16) & (spot < 20)))
    table = table_ref[...]
    for g in range(4):
        line = jnp.broadcast_to(jnp.sum(totals[g], axis=0, keepdims=True), (8, 128))
        for s in range(2):
            here = edge & (lane8 % SECOND // STRIP == s) & (row8 == 2 * g + s)
            table = table + jnp.where(here, line, 0.0)
    table = jnp.sum(table, axis=1, keepdims=True)
    line = jnp.sum(jnp.where(lane8 == row8, table, 0.0), axis=0, keepdims=True)
    gram_ref[...] = jnp.broadcast_to(line, gram_ref.shape)


def combine(
    gram_ref, residual_ref, image_ref, start_ref, side_residual_ref, side_image_ref, out_ref
):
    layers = start_ref.shape[1]
    shape = (8, 128)
    lane = lanes(shape)
    total = jnp.broadcast_to(jnp.sum(gram_ref[...], axis=0, keepdims=True), shape)
    ks, ms = [], []
    for s in range(2):
        rr, ra, aa, ab = (
            jnp.broadcast_to(total[:, q : q + 1], shape) for q in (s, 2 + s, 4 + s, 6 + s)
        )
        first = rr / ra
        norm_next = rr - 2.0 * first * ra + first * first * aa
        growth = 1.0 + norm_next / rr
        curve = growth * growth * ra - 2.0 * growth * first * aa + first * first * ab
        second = norm_next / curve
        ks.append(first + second * growth)
        ms.append(second * first)
    odd = lane % SECOND // STRIP == 1
    k_side = jnp.where(odd, ks[1], ks[0])
    m_side = jnp.where(odd, ms[1], ms[0])
    for z in range(layers):
        for t in range(2):
            at = slice(8 * t, 8 * t + 8)
            side = k_side * side_residual_ref[z, at] - m_side * side_image_ref[z, at]
            for c in range(2):
                step = ks[0] * residual_ref[2 * c, z, at] - ms[0] * image_ref[2 * c, z, at]
                step = step + ks[1] * residual_ref[2 * c + 1, z, at]
                step = step - ms[1] * image_ref[2 * c + 1, z, at]
                base = SECOND * c
                left = roll(side, -(base + 4), 1) + roll(side, -(base + STRIP + 4), 1)
                right = roll(side, 124 - base - 16, 1) + roll(side, 124 - base - STRIP - 16, 1)
                step = jnp.where(lane < HALO, left, step)
                step = jnp.where(lane >= 128 - HALO, right, step)
                out_ref[c, z, at] = start_ref[c, z, at] + step


def f32(*shape):
    return pltpu.VMEM(shape, jnp.float32)


def call(kernel, outs, ins, name, scratch=(), in_specs=None):
    specs = in_specs or [VMEM] * len(ins)
    ins = [
        pltpu.with_memory_space_constraint(x, pltpu.VMEM) if spec is VMEM else x
        for x, spec in zip(ins, specs)
    ]
    return pl.pallas_call(
        kernel,
        in_specs=specs,
        out_specs=[VMEM] * len(outs),
        out_shape=list(outs),
        scratch_shapes=list(scratch),
        name=name,
    )(*ins)


def swap_sides(by_odd, by_even, axis, other="ens"):
    count = lax.axis_size(axis)
    others = lax.axis_size(other) if other else 1

    def swap(message, first):
        pairs = []
        for o in range(others):
            for i in range((first + o) % 2, count - 1, 2):
                low, high = i * others + o, (i + 1) * others + o
                pairs += [(low, high), (high, low)]
        return lax.ppermute(message, (axis, other) if other else axis, pairs)

    return swap(by_odd, 1), swap(by_even, 0)


def body(u_prior, friction_rows, friction_table, bed_fixed, ice_mask):
    members, parts, layers, rows_x, rows_y = u_prior.shape
    total_x = rows_x * lax.axis_size("plane")
    row_place = lax.axis_index("plane").reshape(1)
    row_turn = row_place + lax.axis_index("ens")
    column_turn = (lax.axis_index("planey") + lax.axis_index("ens")).reshape(1)
    by_odd, by_even, geo, u_near = call(
        pack_rows,
        [
            f32(layers + 1, 2, 8, rows_y),
            f32(layers + 1, 2, 8, rows_y),
            f32(4, rows_x, rows_y),
            f32(*u_prior.shape),
        ],
        [row_turn, friction_rows, u_prior, friction_table, bed_fixed, ice_mask],
        "pack_rows",
        scratch=[
            pltpu.SMEM(friction_rows.shape, jnp.int32),
            pltpu.VMEM(friction_table.shape, jnp.float32),
            pltpu.VMEM((2, rows_x, rows_y), jnp.int32),
            pltpu.SemaphoreType.DMA((5,)),
        ],
        in_specs=[SMEM] + [ANY] * 5,
    )
    by_odd, by_even = swap_sides(by_odd, by_even, "plane")
    own = call(
        pack_strips,
        [f32(layers + 1, rows_x, 128), f32(2, rows_x, 128), f32(2, rows_x, 128)],
        [column_turn, u_near, geo],
        "pack_strips",
        in_specs=[SMEM, VMEM, VMEM],
    )
    outer, strip, side_odd, side_even = call(
        pack_columns,
        [f32(layers + 1, 4, 8, rows_y), f32(layers + 1, 24, 128), f32(2, 24, 128), f32(2, 24, 128)],
        [row_turn, column_turn, *own, by_odd, by_even],
        "pack_columns",
        in_specs=[SMEM, SMEM] + [VMEM] * 5,
    )
    side_odd, side_even = swap_sides(side_odd, side_even, "planey")
    residual, image, start, table = call(
        lambda *refs: main_part(*refs, total_x=total_x),
        [
            f32(4, layers, rows_x, 128),
            f32(4, layers, rows_x, 128),
            f32(2, layers, rows_x, 128),
            f32(8, 128),
        ],
        [row_place, u_near, geo, outer],
        "main_part",
        scratch=[
            pltpu.VMEM((2, layers, 24, 128), jnp.float32),
            pltpu.VMEM((layers, 24, 128), jnp.float32),
            pltpu.VMEM((2, layers, 24, 128), jnp.float32),
            pltpu.VMEM((layers, 24, 128), jnp.float32),
            pltpu.VMEM((layers, 24, 128), jnp.float32),
            pltpu.VMEM((layers, 16, 128), jnp.float32),
        ],
        in_specs=[SMEM] + [VMEM] * 3,
    )
    side_residual, side_image, gram = call(
        lambda *refs: strip_part(*refs, total_x=total_x),
        [
            f32(layers, rows_x, 128),
            f32(layers, rows_x, 128),
            f32(lax.axis_size("plane") * lax.axis_size("planey"), 128),
        ],
        [row_place, column_turn, strip, side_odd, side_even, table],
        "strip_part",
        scratch=[pltpu.VMEM((layers, 24, 128), jnp.float32)] * 5
        + [pltpu.VMEM((layers, 16, 128), jnp.float32)],
        in_specs=[SMEM, SMEM] + [VMEM] * 4,
    )
    gathered = lax.all_to_all(gram, ("plane", "planey"), 0, 0, tiled=True)
    (local_sum,) = call(
        combine, [f32(2, layers, rows_x, 128)], [gathered, residual, image, start, side_residual, side_image],
        "combine",

    )
    summed = lax.all_gather(local_sum, "ens").sum(axis=0)
    return summed / (members * lax.axis_size("ens"))


def solution(mesh):
    in_specs = (
        P(("group", "ens"), None, None, "plane", "planey"),
        P(("group", "ens")),
        P("group", "plane", "planey"),
        P("plane", "planey"),
        P("plane", "planey"),
    )
    out_specs = P("group", None, "plane", "planey")
    return jax.shard_map(body, mesh=mesh, in_specs=in_specs, out_specs=out_specs, check_vma=False)
```
